128 devices in a mesh: seq: 16 (over x_hi, y, core), head: 8 (over z, x_lo).
Axes of the slice: x: 4 (x_hi: 2, x_lo: 2; x = x_hi * 2 + x_lo), y: 4, z: 4, core: 2. Of those that a mesh axis runs over, the one named last changes fastest.
Arguments:
- mid: bfloat16 [4096, 3072], P('seq'), may hold values from -20 to 20
- second_in: bfloat16 [4096, 3072], P('seq'), may hold values from -20 to 20
- cotangent: bfloat16 [4096, 3072], P('seq'), may hold values from -6 to 6
- w_key: bfloat16 [3072, 1024], P(None, 'head'), may hold values from -0.109375 to 0.109375
- w_value: bfloat16 [3072, 1024], P(None, 'head'), may hold values from -0.109375 to 0.109375
- w_query: bfloat16 [2, 3072, 3072], P(None, None, 'head'), may hold values from -0.109375 to 0.109375
- w_out: bfloat16 [2, 3072, 3072], P(None, 'head'), may hold values from -0.109375 to 0.109375
- w_ret_out: bfloat16 [3072, 3072], P('head'), may hold values from -0.109375 to 0.109375
- ret_query: bfloat16 [4096, 3072], P('seq', 'head'), may hold values from -6 to 6
- ret_key: bfloat16 [4096, 3072], P('seq', 'head'), may hold values from -3 to 3
- ret_value: bfloat16 [4096, 3072], P('seq', 'head'), may hold values from -6 to 6
- gate: float32 [24, 4096], P('head', 'seq'), may hold values from 0 to 6
- decay_exp: int32 [24], P('head'), may hold values from 0 to 256
- mask_start: int32 [32], P('seq'), may hold values from 0 to 3968, as said below
Outputs:
- grad_mid: bfloat16 [4096, 3072], P('seq')
- grad_ret_query: bfloat16 [4096, 3072], P('seq', 'head')
- grad_ret_key: bfloat16 [4096, 3072], P('seq', 'head')
- grad_ret_value: bfloat16 [4096, 3072], P('seq', 'head')
- grad_w_key: float32 [3072, 1024], P(None, 'head')
- grad_w_value: float32 [3072, 1024], P(None, 'head')
The draws below stay inside these ranges and needn't reach their ends.
Inputs may be any that keep to these rules, and one draw needn't show every extreme that they name: `mask_start`: the entry of each block of 128 queries is at most the position of that block's first query.
All inputs are finite; a program needn't handle non-finite values.
Results may differ from the reference program's by a relative error of at most 0.025.
The reference program's roundings to bfloat16 on the way count: a program that leaves them out, or rounds other values in their place, can miss the bound.
Values may be sent and summed in bfloat16 or wider, within the bound.
A program may use at most 192 MiB of HBM per device.

```python
import math
import jax
import jax.numpy as jnp
from jax import lax

D = 3072
H = 24
KVH = 8
HR = 24
E = 128
LAYERS = 2
BLK = 128
RC = 128
TOK_DEV = 256
TOKENS = 4096


def rows_with_peaks(key):
    values = jnp.clip(jax.random.normal(key, (TOKENS, D), jnp.float32), -5.0, 5.0)
    return values.astype(jnp.bfloat16)


def draw_mid(key, part):
    return rows_with_peaks(key)


def draw_second_in(key, part):
    return rows_with_peaks(jax.random.fold_in(key, 11))


def draw_gate(key, part):
    chooser, rough_key, block_key = jax.random.split(key, 3)
    portion = 0.5
    lasting = jax.random.uniform(chooser, (HR, 1), jnp.float32) < portion
    rough = jax.random.uniform(rough_key, (HR, TOKENS), jnp.float32, 0.5, 2.0)
    blocks = jax.random.uniform(block_key, (HR, TOKENS // TOK_DEV), jnp.float32, 0.5, 2.0)
    rough = rough * jnp.repeat(blocks, TOK_DEV, axis=1)
    factor = jnp.where(lasting, 0.5 / TOKENS, 1.5)
    return (factor * rough).astype(jnp.float32)


def draw_mask_start(key, part):
    blocks = TOKENS // BLK
    firsts = jnp.arange(blocks, dtype=jnp.int32) * BLK
    drawn = jax.random.randint(key, (blocks,), 0, firsts + 1, dtype=jnp.int32)
    last_block = jnp.arange(blocks, dtype=jnp.int32) == blocks - 1
    return jnp.where(last_block, firsts, drawn).astype(jnp.int32)


def with_ends(result, stream_key, least, top_value):
    longest = result.shape.index(max(result.shape))
    spots = []
    for shift in (0, 1):
        where = [jax.random.randint(jax.random.fold_in(stream_key, axis), (), 0, length) for axis, length in enumerate(result.shape)]
        where[longest] = (where[longest] + shift) % result.shape[longest]
        spots.append(tuple(where))
    return result.at[spots[0]].set(least).at[spots[1]].set(top_value)


def steps_of(rng, dims, cuts, smallest, high):
    loudness = 1.0
    for position, parts in cuts:
        steps = jax.random.uniform(jax.random.fold_in(jax.random.fold_in(rng, 6), position), (parts,), jnp.float32, smallest / len(cuts), high / len(cuts))
        loudness = loudness * jnp.repeat(jnp.exp(steps), dims[position] // parts).reshape((-1,) + (1,) * (len(dims) - 1 - position))
    return loudness


def gaussian(rng, shape, spread, bound, shards=(), kind=jnp.bfloat16):
    factor_of = steps_of(rng, shape, shards, -0.22, 0.18) if shards else 1.0
    result = jax.random.normal(rng, shape, jnp.float32) * spread * factor_of
    return jnp.minimum(jnp.maximum(result, -bound), bound).astype(kind)


def setup_inputs(seed: int = 0) -> dict:
    streams_of = jax.random.split(jax.random.key(seed), 15)
    return {
        "mid": draw_mid(jax.random.fold_in(streams_of[14], 71), 0),
        "second_in": draw_second_in(jax.random.fold_in(streams_of[14], 71), 0),
        "cotangent": gaussian(streams_of[2], (TOKENS, D), 1.0, 6.0, ((0, 16),)),
        "w_key": gaussian(streams_of[3], (D, KVH * E), D ** -0.5, 0.109375, ((1, 8),)),
        "w_value": gaussian(streams_of[4], (D, KVH * E), D ** -0.5, 0.109375, ((1, 8),)),
        "w_query": gaussian(streams_of[5], (LAYERS, D, H * E), D ** -0.5, 0.109375, ((2, 8),)),
        "w_out": gaussian(streams_of[6], (LAYERS, H * E, D), (H * E) ** -0.5, 0.109375, ((1, 8),)),
        "w_ret_out": gaussian(streams_of[7], (HR * E, D), (HR * E) ** -0.5, 0.109375, ((0, 8),)),
        "ret_query": gaussian(streams_of[8], (TOKENS, HR * E), 1.0, 6.0, ((0, 16), (1, 8))),
        "ret_key": gaussian(streams_of[9], (TOKENS, HR * E), 0.5, 3.0, ((0, 16), (1, 8))),
        "ret_value": gaussian(streams_of[10], (TOKENS, HR * E), 1.0, 6.0, ((0, 16), (1, 8))),
        "gate": draw_gate(jax.random.fold_in(streams_of[14], 71), 0),
        "decay_exp": with_ends(jax.random.randint(streams_of[12], (HR,), 0, 257), jax.random.fold_in(streams_of[12], 1), 0, 256).astype(jnp.int32),
        "mask_start": draw_mask_start(jax.random.fold_in(streams_of[14], 71), 0),
    }


def contract_last(left, right):
    return lax.dot_general(left, right, (((1,), (1,)), ((), ())), preferred_element_type=jnp.float32)

def round_trip(value):
    return lax.optimization_barrier(value.astype(jnp.bfloat16)).astype(jnp.float32)

def attend_back(layer_in, w_query_l, w_out_l, upstream, keys, values, visible):
    length = layer_in.shape[0]
    kv_heads = keys.shape[1] // E
    factor = 1.0 / math.sqrt(E)
    queries = jnp.dot(layer_in, w_query_l, preferred_element_type=jnp.float32).astype(jnp.bfloat16)
    group = queries.shape[1] // keys.shape[1]
    grad_out = contract_last(upstream, w_out_l).astype(jnp.bfloat16)
    query_heads = queries.reshape(length, kv_heads, group, E).transpose(1, 2, 0, 3)
    grad_heads = grad_out.reshape(length, kv_heads, group, E).transpose(1, 2, 0, 3)
    key_heads = keys.reshape(length, kv_heads, E).transpose(1, 0, 2)
    value_heads = values.reshape(length, kv_heads, E).transpose(1, 0, 2)

    def one_group(items):
        query_now = items[0].astype(jnp.float32)
        grad_now = items[1].astype(jnp.float32)
        key_now = items[2].astype(jnp.float32)
        value_now = items[3].astype(jnp.float32)
        scores = jnp.einsum('gte,se->gts', query_now, key_now) * factor
        scores = jnp.where(visible, scores, -jnp.inf)
        top = lax.optimization_barrier(jnp.max(scores, axis=-1, keepdims=True))
        raised = jnp.exp(scores - top)
        probs = raised / lax.optimization_barrier(jnp.sum(raised, axis=-1, keepdims=True))
        rounded = round_trip(probs)
        outputs = round_trip(jnp.einsum('gts,se->gte', rounded, value_now))
        delta = lax.optimization_barrier(jnp.sum(grad_now * outputs, axis=-1, keepdims=True))
        dprobs = jnp.einsum('gte,se->gts', grad_now, value_now)
        dscores = round_trip(probs * (dprobs - delta) * factor)
        query_grad = jnp.einsum('gts,se->gte', dscores, key_now).astype(jnp.bfloat16)
        key_part = jnp.einsum('gts,gte->se', dscores, query_now)
        value_part = jnp.einsum('gts,gte->se', rounded, grad_now)
        return (query_grad, key_part, value_part)
    query_grads, key_parts, value_parts = lax.map(one_group, (query_heads, grad_heads, key_heads, value_heads))
    query_grad = query_grads.transpose(2, 0, 1, 3).reshape(length, -1)
    key_part = key_parts.transpose(1, 0, 2).reshape(length, -1)
    value_part = value_parts.transpose(1, 0, 2).reshape(length, -1)
    return (contract_last(query_grad, w_query_l), key_part, value_part)

def retention_states(ret_key, ret_value, gate, decay_exp):
    length, width = ret_key.shape
    heads = gate.shape[0]
    size = width // heads
    count = length // RC
    key_blocks = ret_key.reshape(count, RC, heads, size).astype(jnp.float32)
    value_blocks = ret_value.reshape(count, RC, heads, size).astype(jnp.float32)
    rate = jnp.exp2(-decay_exp.astype(jnp.float32) / 64.0)
    accum = jnp.cumsum((-rate[:, None] * gate).reshape(heads, count, RC), axis=2)
    ends = accum[:, :, -1]
    shrink = jnp.transpose(jnp.exp(ends[:, :, None] - accum), (1, 2, 0))[..., None]
    own_state = jnp.einsum('csha,cshb->hcab', round_trip(shrink * key_blocks), value_blocks)
    return (accum, ends, shrink, own_state)

def grad_states(ret_query, grad_o, accum):
    heads, count, block = accum.shape
    size = ret_query.shape[1] // heads
    query_blocks = ret_query.reshape(count, block, heads, size).astype(jnp.float32)
    grad_blocks = grad_o.reshape(count, block, heads, size).astype(jnp.float32)
    grow = jnp.transpose(jnp.exp(accum), (1, 2, 0))[..., None]
    own_grad = jnp.einsum('ctha,cthb->hcab', round_trip(grow * query_blocks), grad_blocks) / E
    return (grow, own_grad)

def retention_grads(ret_query, ret_key, ret_value, grad_o, accum, shrink, grow, entering, after):
    length, width = ret_query.shape
    heads, count, block = accum.shape
    size = width // heads
    shape4 = (count, block, heads, size)
    query_blocks = ret_query.reshape(shape4).astype(jnp.float32)
    key_blocks = ret_key.reshape(shape4).astype(jnp.float32)
    value_blocks = ret_value.reshape(shape4).astype(jnp.float32)
    grad_blocks = grad_o.reshape(shape4).astype(jnp.float32)
    lower = jnp.arange(block)[:, None] >= jnp.arange(block)[None, :]
    diff = accum[:, :, :, None] - accum[:, :, None, :]
    weights = jnp.where(lower, jnp.exp(jnp.where(lower, diff, 0.0)), 0.0)
    first = round_trip(weights * jnp.einsum('ctha,csha->hcts', grad_blocks, value_blocks))
    second = round_trip(weights * jnp.einsum('ctha,csha->hcts', query_blocks, key_blocks))
    inner_query = jnp.einsum('hcts,csha->ctha', first, key_blocks)
    inner_key = jnp.einsum('hcts,ctha->csha', first, query_blocks)
    inner_value = jnp.einsum('hcts,ctha->csha', second, grad_blocks)
    highest = lax.Precision.HIGHEST
    carried_query = jnp.einsum('cthb,hcab->ctha', grad_blocks, entering, precision=highest)
    carried_key = jnp.einsum('cshb,hcab->csha', value_blocks, after, precision=highest)
    carried_value = jnp.einsum('csha,hcab->cshb', key_blocks, after, precision=highest)
    grad_query = ((inner_query + grow * carried_query) / E).astype(jnp.bfloat16).reshape(length, width)
    grad_key = (inner_key / E + shrink * carried_key).astype(jnp.bfloat16).reshape(length, width)
    grad_value = (inner_value / E + shrink * carried_value).astype(jnp.bfloat16).reshape(length, width)
    return (grad_query, grad_key, grad_value)

def reference(mid, second_in, cotangent, w_key, w_value, w_query, w_out, w_ret_out, ret_query, ret_key, ret_value, gate, decay_exp, mask_start):
    keys = jnp.dot(mid, w_key, preferred_element_type=jnp.float32).astype(jnp.bfloat16)
    values = jnp.dot(mid, w_value, preferred_element_type=jnp.float32).astype(jnp.bfloat16)
    positions = jnp.arange(TOKENS, dtype=jnp.int32)
    first_seen = jnp.repeat(mask_start, BLK)
    visible = (positions[None, :] >= first_seen[:, None]) & (positions[None, :] <= positions[:, None])
    upper_in, upper_key, upper_value = attend_back(second_in, w_query[1], w_out[1], cotangent, keys, values, visible)
    upstream = (cotangent.astype(jnp.float32) + upper_in).astype(jnp.bfloat16)
    lower_in, lower_key, lower_value = attend_back(mid, w_query[0], w_out[0], upstream, keys, values, visible)
    key_grad = (upper_key + lower_key).astype(jnp.bfloat16)
    value_grad = (upper_value + lower_value).astype(jnp.bfloat16)
    grad_mid = (upstream.astype(jnp.float32) + lower_in + contract_last(key_grad, w_key) + contract_last(value_grad, w_value)).astype(jnp.bfloat16)
    tokens_dims = (((0,), (0,)), ((), ()))
    grad_w_key = lax.dot_general(mid, key_grad, tokens_dims, preferred_element_type=jnp.float32)
    grad_w_value = lax.dot_general(mid, value_grad, tokens_dims, preferred_element_type=jnp.float32)
    grad_o = contract_last(grad_mid, w_ret_out).astype(jnp.bfloat16)
    accum, ends, shrink, own_state = retention_states(ret_key, ret_value, gate, decay_exp)
    grow, own_grad = grad_states(ret_query, grad_o, accum)
    decays = jnp.exp(ends)
    zeros = jnp.zeros((gate.shape[0], E, E), jnp.float32)

    def forward(state, items):
        return (items[0][:, None, None] * state + items[1], state)

    def backward(state, items):
        return (items[1] + items[0][:, None, None] * state, state)
    unused_state, entering = lax.scan(forward, zeros, (decays.T, jnp.moveaxis(own_state, 1, 0)))
    unused_grad, after = lax.scan(backward, zeros, (decays.T, jnp.moveaxis(own_grad, 1, 0)), reverse=True)
    entering = jnp.moveaxis(entering, 0, 1)
    after = jnp.moveaxis(after, 0, 1)
    grad_query, grad_key, grad_value = retention_grads(ret_query, ret_key, ret_value, grad_o, accum, shrink, grow, entering, after)
    return (grad_mid, grad_query, grad_key, grad_value, grad_w_key, grad_w_value)
```

```python
import functools
import math

import jax
import jax.numpy as jnp
from jax import lax
from jax.experimental import pallas as pl
from jax.experimental.pallas import tpu as pltpu
from jax.sharding import Mesh
from jax.sharding import PartitionSpec as P

E = 128
BLK = 128
RC = 128
SEQ = ("xh", "y", "core")
HEAD = ("z", "xl")

MESH = pl.DeviceIdType.MESH
BF16 = jnp.bfloat16
F32 = jnp.float32


class Wire:
    def __init__(self, send, recv):
        self.send, self.recv, self.sent, self.used = send, recv, [], 0

    def put(self, src, dst, to):
        k = self.used
        self.used += 1
        copy = pltpu.make_async_remote_copy(
            src_ref=src,
            dst_ref=dst,
            send_sem=self.send.at[k],
            recv_sem=self.recv.at[k],
            device_id=to,
            device_id_type=MESH,
        )
        copy.start()
        self.sent.append(copy)
        return (k, to)

    def got(self, ticket, landed):
        k, to = ticket
        pltpu.make_async_remote_copy(
            src_ref=landed,
            dst_ref=landed,
            send_sem=self.send.at[k],
            recv_sem=self.recv.at[k],
            device_id=to,
            device_id_type=MESH,
        ).wait_recv()

    def drain(self):
        for copy in self.sent:
            copy.wait_send()


def meet(peers):
    barrier = pltpu.get_barrier_semaphore()
    for to in peers:
        pl.semaphore_signal(barrier, inc=1, device_id=to, device_id_type=MESH)
    pl.semaphore_wait(barrier, len(peers))


def near(axis):
    at = lax.axis_index(axis)
    return at, lax.rem(at + 1, 4), lax.rem(at + 3, 4), lax.rem(at + 2, 4)


def seq_peers():
    y, yp, ym, y2 = near("y")
    return [
        {"xh": 1 - lax.axis_index("xh")},
        {"y": yp},
        {"y": ym},
        {"core": 1 - lax.axis_index("core")},
    ]


def head_peers():
    z, zp, zm, z2 = near("z")
    return [{"xl": 1 - lax.axis_index("xl")}, {"z": zp}, {"z": zm}]


def by_rows(ref, rows):
    step = math.gcd(rows, rows // 2)
    def at(slot, first, count):
        return ref.at[pl.ds(pl.multiple_of(slot * rows + first, step), count)]

    return at


def by_columns(ref, width):
    def at(slot, first, count):
        return ref.at[pl.ds(first, count), pl.ds(pl.multiple_of(slot * width, 128), width)]

    return at


def add_to(total, part):
    total[...] = (total[...].astype(F32) + part[...].astype(F32)).astype(total.dtype)


def together(*runs):
    runs = list(runs)
    while runs:
        for run in list(runs):
            try:
                next(run)
            except StopIteration:
                runs.remove(run)
        yield


def finish(run):
    for _ in run:
        pass


def gather_seq(wire, at, rows):
    xh, c = lax.axis_index("xh"), lax.axis_index("core")
    y, yp, ym, y2 = near("y")
    xo, co = 1 - xh, 1 - c
    half = rows // 2
    whole, low, high = (0, rows), (0, half), (half, half)
    across, up, down, beside = {"xh": xo}, {"y": yp}, {"y": ym}, {"core": co}

    def slot(a, b, d):
        return a * 8 + b * 2 + d

    def pass_on(s, part, to):
        return wire.put(at(s, *part), at(s, *part), to)

    side = []
    own, far = slot(xh, y, c), slot(xo, y, c)
    t_x = pass_on(own, whole, across)
    ups, downs = [pass_on(own, whole, up)], [pass_on(own, whole, down)]
    side.append((pass_on(own, whole, beside), slot(xh, y, co)))
    yield
    wire.got(t_x, at(far, *whole))
    ups.append(pass_on(far, whole, up))
    downs.append(pass_on(far, whole, down))
    side.append((pass_on(far, whole, beside), slot(xo, y, co)))
    yield
    last = []
    for k, q in enumerate((xh, xo)):
        wire.got(ups[k], at(slot(q, ym, c), *whole))
        a = pass_on(slot(q, ym, c), low, up)
        side.append((pass_on(slot(q, ym, c), whole, beside), slot(q, ym, co)))
        wire.got(downs[k], at(slot(q, yp, c), *whole))
        b = pass_on(slot(q, yp, c), high, down)
        side.append((pass_on(slot(q, yp, c), whole, beside), slot(q, yp, co)))
        last.append((a, b))
        yield
    for k, q in enumerate((xh, xo)):
        wire.got(last[k][0], at(slot(q, y2, c), *low))
        wire.got(last[k][1], at(slot(q, y2, c), *high))
        side.append((pass_on(slot(q, y2, c), whole, beside), slot(q, y2, co)))
        yield
    for ticket, s in side:
        wire.got(ticket, at(s, *whole))


def ring_scatter(wire, at, slot, axis, first, count, land, before=None):
    r, rp, rm, r2 = near(axis)
    up, down = {axis: rp}, {axis: rm}
    half = count // 2
    wait = before or (lambda j: None)
    low, high = land.at[pl.ds(0, half)], land.at[pl.ds(half, half)]
    from_up, from_down = land.at[pl.ds(count, count)], land.at[pl.ds(2 * count, count)]
    wait(2)
    a = wire.put(at(slot(r2), first, half), low, up)
    b = wire.put(at(slot(r2), first + half, half), high, down)
    yield
    wait(1)
    wire.got(a, low)
    add_to(at(slot(rp), first, half), low)
    u = wire.put(at(slot(rp), first, count), from_down, up)
    wait(3)
    wire.got(b, high)
    add_to(at(slot(rm), first + half, half), high)
    d = wire.put(at(slot(rm), first, count), from_up, down)
    yield
    wait(0)
    wire.got(u, from_down)
    add_to(at(slot(r), first, count), from_down)
    wire.got(d, from_up)
    add_to(at(slot(r), first, count), from_up)


def scatter_seq(wire, at, rows, land):
    xh, c = lax.axis_index("xh"), lax.axis_index("core")
    y, yp, ym, y2 = near("y")
    xo, co = 1 - xh, 1 - c

    def slot(a, b, d):
        return a * 8 + b * 2 + d

    def block(k, count=1):
        return land.at[pl.ds(k * rows, count * rows)]

    places = {0: y, 1: yp, 2: y2, 3: ym}
    side = {}
    for n, q in enumerate((xo, xh)):
        for m, j in enumerate((2, 1, 3, 0)):
            dst = block(4 * n + m)
            side[n, j] = (wire.put(at(slot(q, places[j], co), 0, rows), dst, {"core": co}), dst)

    def before(n, q):
        def wait(j):
            ticket, dst = side[n, j]
            wire.got(ticket, dst)
            add_to(at(slot(q, places[j], c), 0, rows), dst)

        return wait

    def ring(n, q):
        return ring_scatter(
            wire, at, lambda j: slot(q, j, c), "y", 0, rows, block(8 + 3 * n, 3), before(n, q)
        )

    sent = []

    def far():
        yield from ring(0, xo)
        sent.append(wire.put(at(slot(xo, y, c), 0, rows), block(14), {"xh": xo}))

    yield from together(far(), ring(1, xh))
    wire.got(sent[0], block(14))
    return block(14)


def scatter_head(wire, at, rows, land):
    xl = lax.axis_index("xl")
    z, zp, zm, z2 = near("z")
    xo = 1 - xl
    half = rows // 2

    def slot(j, q):
        return j * 2 + q

    def block(k, count=1):
        return land.at[pl.ds(k * half, count * half)]

    places = {0: z, 1: zp, 2: z2, 3: zm}
    side = {}
    for m, j in enumerate((2, 1, 3, 0)):
        side[j] = (wire.put(at(slot(places[j], xo), 0, half), block(m), {"xl": xo}), block(m))

    def wait(j):
        ticket, dst = side[j]
        wire.got(ticket, dst)
        add_to(at(slot(places[j], xl), 0, half), dst)

    sent = []

    def far():
        yield from ring_scatter(
            wire, at, lambda j: slot(j, xo), "z", half, half, block(4, 3)
        )
        sent.append(wire.put(at(slot(z, xo), half, half), block(13), {"xl": xo}))

    yield from together(
        far(),
        ring_scatter(wire, at, lambda j: slot(j, xl), "z", half, half, block(7, 3)),
        ring_scatter(wire, at, lambda j: slot(j, xl), "z", 0, half, block(10, 3), wait),
    )
    wire.got(sent[0], block(13))
    add_to(at(slot(z, xl), half, half), block(13))


def gather_head(wire, at, rows):
    xl = lax.axis_index("xl")
    z, zp, zm, z2 = near("z")
    xo = 1 - xl
    half = rows // 2
    up, down, across = {"z": zp}, {"z": zm}, {"xl": xo}

    def slot(j, q):
        return j * 2 + q

    def pass_on(s, first, count, to):
        return wire.put(at(s, first, count), at(s, first, count), to)

    def ring(q, first, each=None):
        h = half // 2
        tell = each or (lambda j: None)
        a = pass_on(slot(z, q), first, half, up)
        b = pass_on(slot(z, q), first, half, down)
        tell(z)
        yield
        wire.got(a, at(slot(zm, q), first, half))
        c = pass_on(slot(zm, q), first, h, up)
        tell(zm)
        wire.got(b, at(slot(zp, q), first, half))
        d = pass_on(slot(zp, q), first + h, h, down)
        tell(zp)
        yield
        wire.got(c, at(slot(z2, q), first, h))
        wire.got(d, at(slot(z2, q), first + h, h))
        tell(z2)

    side = []

    def tell(j):
        side.append((pass_on(slot(j, xl), 0, half, across), slot(j, xo)))

    t_x = pass_on(slot(z, xl), half, half, across)

    def far():
        wire.got(t_x, at(slot(z, xo), half, half))
        yield from ring(xo, half)

    yield from together(ring(xl, 0, tell), ring(xl, half), far())
    for ticket, s in side:
        wire.got(ticket, at(s, 0, half))


ANY = pl.BlockSpec(memory_space=pl.ANY)
VMEM = pl.BlockSpec(memory_space=pltpu.VMEM)


def wires(count):
    return [pltpu.SemaphoreType.DMA((count,)), pltpu.SemaphoreType.DMA((count,))]


def params(number):
    return pltpu.CompilerParams(collective_id=number, has_side_effects=True)


def bring(*pairs, sem):
    copies = [pltpu.make_async_copy(s, d, sem.at[k]) for k, (s, d) in enumerate(pairs)]
    for copy in copies:
        copy.start()
    return copies


def seq_index():
    return lax.axis_index("xh") * 8 + lax.axis_index("y") * 2 + lax.axis_index("core")


def head_index():
    return lax.axis_index("z") * 2 + lax.axis_index("xl")


def seq_gather_kernel(own, out, local, send, recv):
    rows = own.shape[0]
    at = by_rows(out, rows)
    (copy,) = bring((own, at(seq_index(), 0, rows)), sem=local)
    meet(seq_peers())
    copy.wait()
    wire = Wire(send, recv)
    finish(gather_seq(wire, at, rows))
    wire.drain()


def seq_gather(own, number):
    rows, width = own.shape
    return pl.pallas_call(
        seq_gather_kernel,
        out_shape=jax.ShapeDtypeStruct((16 * rows, width), own.dtype),
        in_specs=[ANY],
        out_specs=VMEM,
        scratch_shapes=[pltpu.SemaphoreType.DMA((1,)), *wires(20)],
        compiler_params=params(number),
    )(own)


def total_into(out_at, acc_at, residual, rows, width):
    me = head_index()
    own = acc_at(me, 0, rows)
    kept = residual.at[pl.ds(0, rows), pl.ds(pl.multiple_of(me * width, 128), width)]
    out_at(me, 0, rows)[...] = (kept[...].astype(F32) + own[...].astype(F32)).astype(BF16)


def head_run(wire, acc, land, residual, out):
    rows, columns = acc.shape
    width = columns // 8
    yield from scatter_head(wire, by_columns(acc, width), rows, land)
    total_into(by_columns(out, width), by_columns(acc, width), residual, rows, width)
    yield from gather_head(wire, by_columns(out, width), rows)


def upstream_kernel(
    part, residual, state, decay, out, states, decays, acc, land, local, send, recv
):
    s_rows, d_rows = state.shape[0], decay.shape[0]
    s_at, d_at = by_rows(states, s_rows), by_rows(decays, d_rows)
    me = seq_index()
    copies = bring(
        (part, acc), (state, s_at(me, 0, s_rows)), (decay, d_at(me, 0, d_rows)), sem=local
    )
    meet(seq_peers() + head_peers())
    for copy in copies:
        copy.wait()
    wire = Wire(send, recv)
    finish(
        together(
            head_run(wire, acc, land, residual, out),
            gather_seq(wire, s_at, s_rows),
            gather_seq(wire, d_at, d_rows),
        )
    )
    wire.drain()


def upstream_of(part, residual, state, decay, number):
    rows, columns = part.shape
    return pl.pallas_call(
        upstream_kernel,
        out_shape=(
            jax.ShapeDtypeStruct(part.shape, BF16),
            jax.ShapeDtypeStruct((16 * state.shape[0], state.shape[1]), BF16),
            jax.ShapeDtypeStruct((16 * decay.shape[0], decay.shape[1]), F32),
        ),
        in_specs=[ANY, VMEM, ANY, ANY],
        out_specs=(VMEM, VMEM, VMEM),
        scratch_shapes=[
            pltpu.VMEM(part.shape, BF16),
            pltpu.VMEM((7 * rows, columns // 8), BF16),
            pltpu.SemaphoreType.DMA((3,)),
            *wires(90),
        ],
        compiler_params=params(number),
    )(part, residual, state, decay)


def seq_run(wire, acc, land, out_own):
    rows = acc.shape[0] // 16
    at = by_rows(acc, rows)
    rest = yield from scatter_seq(wire, at, rows, land)
    own = at(seq_index(), 0, rows)
    out_own[...] = (own[...].astype(F32) + rest[...].astype(F32)).astype(BF16)


def seq_scatter_kernel(part, out, acc, land, local, send, recv):
    (copy,) = bring((part, acc), sem=local)
    meet(seq_peers())
    copy.wait()
    wire = Wire(send, recv)
    finish(seq_run(wire, acc, land, out))
    wire.drain()


def seq_scatter(part, number):
    rows, width = part.shape[0] // 16, part.shape[1]
    return pl.pallas_call(
        seq_scatter_kernel,
        out_shape=jax.ShapeDtypeStruct((rows, width), BF16),
        in_specs=[ANY],
        out_specs=VMEM,
        scratch_shapes=[
            pltpu.VMEM(part.shape, BF16),
            pltpu.VMEM((15 * rows, width), BF16),
            pltpu.SemaphoreType.DMA((1,)),
            *wires(30),
        ],
        compiler_params=params(number),
    )(part)


def mid_kernel(part, residual, weight, out, weights, acc, land, w_acc, w_land, local, send, recv):
    w_rows = weight.shape[0] // 16
    w_at = by_rows(weights, w_rows)
    copies = bring((part, acc), (weight, w_acc), sem=local)
    meet(seq_peers() + head_peers())
    for copy in copies:
        copy.wait()
    wire = Wire(send, recv)

    def summed():
        yield from seq_run(wire, w_acc, w_land, w_at(seq_index(), 0, w_rows))
        yield from gather_seq(wire, w_at, w_rows)

    finish(together(head_run(wire, acc, land, residual, out), summed()))
    wire.drain()


def mid_of(part, residual, weight, number):
    rows, columns = part.shape
    w_rows = weight.shape[0] // 16
    return pl.pallas_call(
        mid_kernel,
        out_shape=(
            jax.ShapeDtypeStruct(part.shape, BF16),
            jax.ShapeDtypeStruct(weight.shape, BF16),
        ),
        in_specs=[ANY, VMEM, ANY],
        out_specs=(VMEM, VMEM),
        scratch_shapes=[
            pltpu.VMEM(part.shape, BF16),
            pltpu.VMEM((7 * rows, columns // 8), BF16),
            pltpu.VMEM(weight.shape, BF16),
            pltpu.VMEM((15 * w_rows, weight.shape[1]), BF16),
            pltpu.SemaphoreType.DMA((2,)),
            *wires(100),
        ],
        compiler_params=params(number),
    )(part, residual, weight)


def contract_last(left, right):
    return lax.dot_general(
        left, right, (((1,), (1,)), ((), ())), preferred_element_type=jnp.float32
    )


def attend_back(layer_in, w_query_l, w_out_l, upstream, keys, values, visible):
    row_count = layer_in.shape[0]
    key_count = keys.shape[0]
    kv_heads = keys.shape[1] // E
    factor = 1.0 / math.sqrt(E)
    queries = jnp.dot(layer_in, w_query_l, preferred_element_type=jnp.float32).astype(jnp.bfloat16)
    group = queries.shape[1] // keys.shape[1]
    grad_out = contract_last(upstream, w_out_l).astype(jnp.bfloat16)
    query_heads = queries.reshape(row_count, kv_heads, group, E)
    grad_heads = grad_out.reshape(row_count, kv_heads, group, E)
    key_heads = keys.reshape(key_count, kv_heads, E)
    value_heads = values.reshape(key_count, kv_heads, E)
    scores = (
        jnp.einsum("tkge,ske->kgts", query_heads, key_heads, preferred_element_type=jnp.float32)
        * factor
    )
    scores = jnp.where(visible, scores, -jnp.inf)
    top = jnp.max(scores, axis=-1, keepdims=True)
    raised = jnp.exp(scores - top)
    probs = raised / jnp.sum(raised, axis=-1, keepdims=True)
    rounded = probs.astype(jnp.bfloat16)
    outputs = jnp.einsum(
        "kgts,ske->tkge", rounded, value_heads, preferred_element_type=jnp.float32
    ).astype(jnp.bfloat16)
    delta = jnp.sum(grad_heads.astype(jnp.float32) * outputs.astype(jnp.float32), axis=-1)
    delta = jnp.transpose(delta, (1, 2, 0))[..., None]
    dprobs = jnp.einsum(
        "tkge,ske->kgts", grad_heads, value_heads, preferred_element_type=jnp.float32
    )
    dscores = (probs * (dprobs - delta) * factor).astype(jnp.bfloat16)
    query_grad = jnp.einsum(
        "kgts,ske->tkge", dscores, key_heads, preferred_element_type=jnp.float32
    )
    query_grad = query_grad.astype(jnp.bfloat16).reshape(row_count, -1)
    key_part = jnp.einsum(
        "kgts,tkge->ske", dscores, query_heads, preferred_element_type=jnp.float32
    ).reshape(key_count, -1)
    value_part = jnp.einsum(
        "kgts,tkge->ske", rounded, grad_heads, preferred_element_type=jnp.float32
    ).reshape(key_count, -1)
    return (contract_last(query_grad, w_query_l), key_part, value_part)


def retention_states(ret_key, ret_value, gate, decay_exp):
    length, width = ret_key.shape
    heads = gate.shape[0]
    size = width // heads
    count = length // RC
    key_blocks = ret_key.reshape(count, RC, heads, size)
    value_blocks = ret_value.reshape(count, RC, heads, size)
    rate = jnp.exp2(-decay_exp.astype(jnp.float32) / 64.0)
    accum = jnp.cumsum((-rate[:, None] * gate).reshape(heads, count, RC), axis=2)
    ends = accum[:, :, -1]
    shrink = jnp.transpose(jnp.exp(ends[:, :, None] - accum), (1, 2, 0))[..., None]
    weighted = (shrink * key_blocks).astype(jnp.bfloat16)
    own_state = jnp.einsum(
        "csha,cshb->hcab", weighted, value_blocks, preferred_element_type=jnp.float32
    )
    return (accum, ends, shrink, own_state)


def grad_states(ret_query, grad_o, accum):
    heads, count, block = accum.shape
    size = ret_query.shape[1] // heads
    query_blocks = ret_query.reshape(count, block, heads, size)
    grad_blocks = grad_o.reshape(count, block, heads, size)
    grow = jnp.transpose(jnp.exp(accum), (1, 2, 0))[..., None]
    weighted = (grow * query_blocks).astype(jnp.bfloat16)
    own_grad = (
        jnp.einsum("ctha,cthb->hcab", weighted, grad_blocks, preferred_element_type=jnp.float32) / E
    )
    return (grow, own_grad)


def retention_grads(ret_query, ret_key, ret_value, grad_o, accum, shrink, grow, entering, after):
    length, width = ret_query.shape
    heads, count, block = accum.shape
    size = width // heads
    shape4 = (count, block, heads, size)
    query_blocks = ret_query.reshape(shape4)
    key_blocks = ret_key.reshape(shape4)
    value_blocks = ret_value.reshape(shape4)
    grad_blocks = grad_o.reshape(shape4)
    lower = jnp.arange(block)[:, None] >= jnp.arange(block)[None, :]
    diff = accum[:, :, :, None] - accum[:, :, None, :]
    weights = jnp.where(lower, jnp.exp(jnp.where(lower, diff, 0.0)), 0.0)
    first = (
        weights
        * jnp.einsum(
            "ctha,csha->hcts", grad_blocks, value_blocks, preferred_element_type=jnp.float32
        )
    ).astype(jnp.bfloat16)
    second = (
        weights
        * jnp.einsum(
            "ctha,csha->hcts", query_blocks, key_blocks, preferred_element_type=jnp.float32
        )
    ).astype(jnp.bfloat16)
    inner_query = jnp.einsum(
        "hcts,csha->ctha", first, key_blocks, preferred_element_type=jnp.float32
    )
    inner_key = jnp.einsum(
        "hcts,ctha->csha", first, query_blocks, preferred_element_type=jnp.float32
    )
    inner_value = jnp.einsum(
        "hcts,ctha->csha", second, grad_blocks, preferred_element_type=jnp.float32
    )
    carried_query = jnp.einsum("cthb,hcab->ctha", grad_blocks.astype(jnp.float32), entering)
    carried_key = jnp.einsum("cshb,hcab->csha", value_blocks.astype(jnp.float32), after)
    carried_value = jnp.einsum("csha,hcab->cshb", key_blocks.astype(jnp.float32), after)
    grad_query = (
        ((inner_query + grow * carried_query) / E).astype(jnp.bfloat16).reshape(length, width)
    )
    grad_key = (inner_key / E + shrink * carried_key).astype(jnp.bfloat16).reshape(length, width)
    grad_value = (
        (inner_value / E + shrink * carried_value).astype(jnp.bfloat16).reshape(length, width)
    )
    return (grad_query, grad_key, grad_value)


def local(
    mid,
    second_in,
    cotangent,
    w_key,
    w_value,
    w_query,
    w_out,
    w_ret_out,
    ret_query,
    ret_key,
    ret_value,
    gate,
    decay_exp,
    mask_start,
):
    row_count = mid.shape[0]
    accum, ends, shrink, own_state = retention_states(ret_key, ret_value, gate, decay_exp)
    decay_rows = jnp.exp(ends)
    count = decay_rows.shape[1]
    device_state = jnp.zeros_like(own_state[:, 0])
    for block in range(count):
        device_state = decay_rows[:, block, None, None] * device_state + own_state[:, block]
    device_log = jnp.sum(ends, axis=1)
    decay_tile = jnp.broadcast_to(jnp.pad(device_log, (0, 13))[:, None], (16, 128))
    keys_own = jnp.dot(mid, w_key, preferred_element_type=jnp.float32).astype(jnp.bfloat16)
    values_own = jnp.dot(mid, w_value, preferred_element_type=jnp.float32).astype(jnp.bfloat16)
    everything = seq_gather(jnp.concatenate((keys_own, values_own), axis=1), 0)
    all_keys, all_values = everything[:, :E], everything[:, E:]
    key_count = all_keys.shape[0]
    positions = lax.axis_index(SEQ) * row_count + jnp.arange(row_count, dtype=jnp.int32)
    first_seen = jnp.repeat(mask_start, BLK)
    key_positions = jnp.arange(key_count, dtype=jnp.int32)
    visible = (key_positions[None, :] >= first_seen[:, None]) & (
        key_positions[None, :] <= positions[:, None]
    )
    upper_in, upper_key, upper_value = attend_back(
        second_in, w_query[1], w_out[1], cotangent, all_keys, all_values, visible
    )
    upstream, states, logs = upstream_of(
        upper_in.astype(BF16), cotangent, device_state.reshape(-1, E).astype(BF16), decay_tile, 1
    )
    lower_in, lower_key, lower_value = attend_back(
        mid, w_query[0], w_out[0], upstream, all_keys, all_values, visible
    )
    kv_part = jnp.concatenate((upper_key + lower_key, upper_value + lower_value), axis=1)
    kv_grad = seq_scatter(kv_part.astype(BF16), 2)
    key_grad, value_grad = kv_grad[:, :E], kv_grad[:, E:]
    mid_part = lower_in + contract_last(key_grad, w_key) + contract_last(value_grad, w_value)
    tokens_dims = (((0,), (0,)), ((), ()))
    weight_part = lax.dot_general(mid, kv_grad, tokens_dims, preferred_element_type=jnp.float32)
    grad_mid, weight_sum = mid_of(mid_part.astype(BF16), upstream, weight_part.astype(BF16), 3)
    grad_w_key = weight_sum[:, :E].astype(F32)
    grad_w_value = weight_sum[:, E:].astype(F32)
    grad_o = contract_last(grad_mid, w_ret_out).astype(jnp.bfloat16)
    grow, own_grad = grad_states(ret_query, grad_o, accum)
    device_grad = jnp.zeros_like(device_state)
    for block in reversed(range(count)):
        device_grad = own_grad[:, block] + decay_rows[:, block, None, None] * device_grad
    grads = seq_gather(device_grad.reshape(-1, E).astype(BF16), 4)
    heads = gate.shape[0]
    logs = logs.reshape(16, 16, 128)[:, :heads, 0]
    reach = jnp.cumsum(logs, axis=0)
    here = lax.axis_index(SEQ)
    index = jnp.arange(16)[:, None]
    own_reach = lax.dynamic_slice_in_dim(reach, here, 1, 0)
    own_log = lax.dynamic_slice_in_dim(logs, here, 1, 0)
    toward = jnp.exp(jnp.where(index < here, own_reach - own_log - reach, 0.0))
    toward = jnp.where(index < here, toward, 0.0)
    since = jnp.exp(jnp.where(index > here, reach - logs - own_reach, 0.0))
    since = jnp.where(index > here, since, 0.0)
    states = states.reshape(16, heads, E, E).astype(F32)
    grads = grads.reshape(16, heads, E, E).astype(F32)
    incoming = jnp.sum(toward[:, :, None, None] * states, axis=0)
    outgoing = jnp.sum(since[:, :, None, None] * grads, axis=0)
    entering_list = []
    state_now = incoming
    for block in range(count):
        entering_list.append(state_now)
        state_now = decay_rows[:, block, None, None] * state_now + own_state[:, block]
    after_list = [state_now] * count
    state_now = outgoing
    for block in reversed(range(count)):
        after_list[block] = state_now
        state_now = own_grad[:, block] + decay_rows[:, block, None, None] * state_now
    entering = jnp.stack(entering_list, axis=1)
    after = jnp.stack(after_list, axis=1)
    grad_query, grad_key, grad_value = retention_grads(
        ret_query, ret_key, ret_value, grad_o, accum, shrink, grow, entering, after
    )
    return (grad_mid, grad_query, grad_key, grad_value, grad_w_key, grad_w_value)


def solution(mesh):
    torus = Mesh(mesh.devices.reshape(2, 4, 2, 4, 2), ("xh", "y", "core", "z", "xl"))
    in_specs = (
        P(SEQ, None),
        P(SEQ, None),
        P(SEQ, None),
        P(None, HEAD),
        P(None, HEAD),
        P(None, None, HEAD),
        P(None, HEAD, None),
        P(HEAD, None),
        P(SEQ, HEAD),
        P(SEQ, HEAD),
        P(SEQ, HEAD),
        P(HEAD, SEQ),
        P(HEAD),
        P(SEQ),
    )
    out_specs = (
        P(SEQ, None),
        P(SEQ, HEAD),
        P(SEQ, HEAD),
        P(SEQ, HEAD),
        P(None, HEAD),
        P(None, HEAD),
    )
    return jax.shard_map(local, mesh=torus, in_specs=in_specs, out_specs=out_specs, check_vma=False)
```

```python
import functools
import math

import jax
import jax.numpy as jnp
from jax import lax
from jax.experimental import pallas as pl
from jax.experimental.pallas import tpu as pltpu
from jax.sharding import Mesh
from jax.sharding import PartitionSpec as P

E = 128
BLK = 128
RC = 128
SEQ = ("xh", "y", "core")
HEAD = ("z", "xl")

MESH = pl.DeviceIdType.MESH
BF16 = jnp.bfloat16
F32 = jnp.float32


class Wire:
    def __init__(self, send, recv):
        self.send, self.recv, self.sent, self.used = send, recv, [], 0

    def put(self, src, dst, to):
        k = self.used
        self.used += 1
        copy = pltpu.make_async_remote_copy(
            src_ref=src,
            dst_ref=dst,
            send_sem=self.send.at[k],
            recv_sem=self.recv.at[k],
            device_id=to,
            device_id_type=MESH,
        )
        copy.start()
        self.sent.append(copy)
        return (k, to)

    def got(self, ticket, landed):
        k, to = ticket
        pltpu.make_async_remote_copy(
            src_ref=landed,
            dst_ref=landed,
            send_sem=self.send.at[k],
            recv_sem=self.recv.at[k],
            device_id=to,
            device_id_type=MESH,
        ).wait_recv()

    def drain(self):
        for copy in self.sent:
            copy.wait_send()


def meet(peers):
    barrier = pltpu.get_barrier_semaphore()
    for to in peers:
        pl.semaphore_signal(barrier, inc=1, device_id=to, device_id_type=MESH)
    pl.semaphore_wait(barrier, len(peers))


def near(axis):
    at = lax.axis_index(axis)
    return at, lax.rem(at + 1, 4), lax.rem(at + 3, 4), lax.rem(at + 2, 4)


def seq_peers():
    y, yp, ym, y2 = near("y")
    return [
        {"xh": 1 - lax.axis_index("xh")},
        {"y": yp},
        {"y": ym},
        {"core": 1 - lax.axis_index("core")},
    ]


def head_peers():
    z, zp, zm, z2 = near("z")
    return [{"xl": 1 - lax.axis_index("xl")}, {"z": zp}, {"z": zm}]


def by_rows(ref, rows, parts=2):
    step = rows // parts

    def at(slot, first, count):
        return ref.at[pl.ds(pl.multiple_of(slot * rows + first, step), count)]

    return at


def by_columns(ref, width):
    def at(slot, first, count):
        return ref.at[pl.ds(first, count), pl.ds(pl.multiple_of(slot * width, 128), width)]

    return at


def add_to(total, part):
    total[...] = (total[...].astype(F32) + part[...].astype(F32)).astype(total.dtype)


def together(*runs):
    runs = list(runs)
    while runs:
        for run in list(runs):
            try:
                next(run)
            except StopIteration:
                runs.remove(run)
        yield


def finish(run):
    for _ in run:
        pass


def gather_seq(wire, at, rows):
    xh, c = lax.axis_index("xh"), lax.axis_index("core")
    y, yp, ym, y2 = near("y")
    xo, co = 1 - xh, 1 - c
    half = rows // 2
    whole, low, high = (0, rows), (0, half), (half, half)
    across, up, down, beside = {"xh": xo}, {"y": yp}, {"y": ym}, {"core": co}

    def slot(a, b, d):
        return a * 8 + b * 2 + d

    def pass_on(s, part, to):
        return wire.put(at(s, *part), at(s, *part), to)

    side = []
    own, far = slot(xh, y, c), slot(xo, y, c)
    t_x = pass_on(own, whole, across)
    ups, downs = [pass_on(own, whole, up)], [pass_on(own, whole, down)]
    side.append((pass_on(own, whole, beside), slot(xh, y, co)))
    yield
    wire.got(t_x, at(far, *whole))
    ups.append(pass_on(far, whole, up))
    downs.append(pass_on(far, whole, down))
    side.append((pass_on(far, whole, beside), slot(xo, y, co)))
    yield
    last = []
    for k, q in enumerate((xh, xo)):
        wire.got(ups[k], at(slot(q, ym, c), *whole))
        a = pass_on(slot(q, ym, c), low, up)
        side.append((pass_on(slot(q, ym, c), whole, beside), slot(q, ym, co)))
        wire.got(downs[k], at(slot(q, yp, c), *whole))
        b = pass_on(slot(q, yp, c), high, down)
        side.append((pass_on(slot(q, yp, c), whole, beside), slot(q, yp, co)))
        last.append((a, b))
        yield
    for k, q in enumerate((xh, xo)):
        wire.got(last[k][0], at(slot(q, y2, c), *low))
        wire.got(last[k][1], at(slot(q, y2, c), *high))
        side.append((pass_on(slot(q, y2, c), whole, beside), slot(q, y2, co)))
        yield
    for ticket, s in side:
        wire.got(ticket, at(s, *whole))


def ring_scatter(wire, at, slot, axis, first, count, land, before=None):
    r, rp, rm, r2 = near(axis)
    up, down = {axis: rp}, {axis: rm}
    half = count // 2
    wait = before or (lambda j: None)
    low, high = land.at[pl.ds(0, half)], land.at[pl.ds(half, half)]
    from_up, from_down = land.at[pl.ds(count, count)], land.at[pl.ds(2 * count, count)]
    wait(2)
    a = wire.put(at(slot(r2), first, half), low, up)
    b = wire.put(at(slot(r2), first + half, half), high, down)
    yield
    wait(1)
    wire.got(a, low)
    add_to(at(slot(rp), first, half), low)
    u = wire.put(at(slot(rp), first, count), from_down, up)
    wait(3)
    wire.got(b, high)
    add_to(at(slot(rm), first + half, half), high)
    d = wire.put(at(slot(rm), first, count), from_up, down)
    yield
    wait(0)
    wire.got(u, from_down)
    add_to(at(slot(r), first, count), from_down)
    wire.got(d, from_up)
    add_to(at(slot(r), first, count), from_up)


def scatter_seq(wire, at, rows, land):
    xh, c = lax.axis_index("xh"), lax.axis_index("core")
    y, yp, ym, y2 = near("y")
    xo, co = 1 - xh, 1 - c

    def slot(a, b, d):
        return a * 8 + b * 2 + d

    def block(k, count=1):
        return land.at[pl.ds(k * rows, count * rows)]

    places = {0: y, 1: yp, 2: y2, 3: ym}
    side = {}
    for n, q in enumerate((xo, xh)):
        for m, j in enumerate((2, 1, 3, 0)):
            dst = block(4 * n + m)
            side[n, j] = (wire.put(at(slot(q, places[j], co), 0, rows), dst, {"core": co}), dst)

    def before(n, q):
        def wait(j):
            ticket, dst = side[n, j]
            wire.got(ticket, dst)
            add_to(at(slot(q, places[j], c), 0, rows), dst)

        return wait

    def ring(n, q):
        return ring_scatter(
            wire, at, lambda j: slot(q, j, c), "y", 0, rows, block(8 + 3 * n, 3), before(n, q)
        )

    sent = []

    def far():
        yield from ring(0, xo)
        sent.append(wire.put(at(slot(xo, y, c), 0, rows), block(14), {"xh": xo}))

    yield from together(far(), ring(1, xh))
    wire.got(sent[0], block(14))
    return block(14)


def scatter_head(wire, at, rows, land):
    xl = lax.axis_index("xl")
    z, zp, zm, z2 = near("z")
    xo = 1 - xl
    half = rows // 2

    def slot(j, q):
        return j * 2 + q

    def block(k, count=1):
        return land.at[pl.ds(k * half, count * half)]

    places = {0: z, 1: zp, 2: z2, 3: zm}
    side = {}
    for m, j in enumerate((2, 1, 3, 0)):
        side[j] = (wire.put(at(slot(places[j], xo), 0, half), block(m), {"xl": xo}), block(m))

    def wait(j):
        ticket, dst = side[j]
        wire.got(ticket, dst)
        add_to(at(slot(places[j], xl), 0, half), dst)

    sent = []

    def far():
        yield from ring_scatter(
            wire, at, lambda j: slot(j, xo), "z", half, half, block(4, 3)
        )
        sent.append(wire.put(at(slot(z, xo), half, half), block(13), {"xl": xo}))

    yield from together(
        far(),
        ring_scatter(wire, at, lambda j: slot(j, xl), "z", half, half, block(7, 3)),
        ring_scatter(wire, at, lambda j: slot(j, xl), "z", 0, half, block(10, 3), wait),
    )
    wire.got(sent[0], block(13))
    add_to(at(slot(z, xl), half, half), block(13))


def gather_head(wire, at, rows):
    xl = lax.axis_index("xl")
    z, zp, zm, z2 = near("z")
    xo = 1 - xl
    half = rows // 2
    up, down, across = {"z": zp}, {"z": zm}, {"xl": xo}

    def slot(j, q):
        return j * 2 + q

    def pass_on(s, first, count, to):
        return wire.put(at(s, first, count), at(s, first, count), to)

    def ring(q, first, each=None):
        h = half // 2
        tell = each or (lambda j: None)
        a = pass_on(slot(z, q), first, half, up)
        b = pass_on(slot(z, q), first, half, down)
        tell(z)
        yield
        wire.got(a, at(slot(zm, q), first, half))
        c = pass_on(slot(zm, q), first, h, up)
        tell(zm)
        wire.got(b, at(slot(zp, q), first, half))
        d = pass_on(slot(zp, q), first + h, h, down)
        tell(zp)
        yield
        wire.got(c, at(slot(z2, q), first, h))
        wire.got(d, at(slot(z2, q), first + h, h))
        tell(z2)

    side = []

    def tell(j):
        side.append((pass_on(slot(j, xl), 0, half, across), slot(j, xo)))

    t_x = pass_on(slot(z, xl), half, half, across)

    def far():
        wire.got(t_x, at(slot(z, xo), half, half))
        yield from ring(xo, half)

    yield from together(ring(xl, 0, tell), ring(xl, half), far())
    for ticket, s in side:
        wire.got(ticket, at(s, 0, half))


ANY = pl.BlockSpec(memory_space=pl.ANY)
VMEM = pl.BlockSpec(memory_space=pltpu.VMEM)


def wires(count):
    return [pltpu.SemaphoreType.DMA((count,)), pltpu.SemaphoreType.DMA((count,))]


def params(number):
    return pltpu.CompilerParams(collective_id=number, has_side_effects=True)


def bring(*pairs, sem):
    copies = [pltpu.make_async_copy(s, d, sem.at[k]) for k, (s, d) in enumerate(pairs)]
    for copy in copies:
        copy.start()
    return copies


def seq_index():
    return lax.axis_index("xh") * 8 + lax.axis_index("y") * 2 + lax.axis_index("core")


def head_index():
    return lax.axis_index("z") * 2 + lax.axis_index("xl")


def total_into(out_at, acc_at, residual, rows, width):
    me = head_index()
    own = acc_at(me, 0, rows)
    kept = residual.at[pl.ds(0, rows), pl.ds(pl.multiple_of(me * width, 128), width)]
    out_at(me, 0, rows)[...] = (kept[...].astype(F32) + own[...].astype(F32)).astype(BF16)


def head_run(wire, acc, land, residual, out):
    rows, columns = acc.shape
    width = columns // 8
    yield from scatter_head(wire, by_columns(acc, width), rows, land)
    total_into(by_columns(out, width), by_columns(acc, width), residual, rows, width)
    yield from gather_head(wire, by_columns(out, width), rows)


def upstream_kernel(
    part, residual, state, decay, out, states, decays, acc, land, local, send, recv
):
    s_rows, d_rows = state.shape[0], decay.shape[0]
    s_at, d_at = by_rows(states, s_rows), by_rows(decays, d_rows)
    me = seq_index()
    copies = bring(
        (part, acc), (state, s_at(me, 0, s_rows)), (decay, d_at(me, 0, d_rows)), sem=local
    )
    meet(seq_peers() + head_peers())
    for copy in copies:
        copy.wait()
    wire = Wire(send, recv)
    finish(
        together(
            head_run(wire, acc, land, residual, out),
            gather_seq(wire, s_at, s_rows),
            gather_seq(wire, d_at, d_rows),
        )
    )
    wire.drain()


def upstream_of(part, residual, state, decay, number):
    rows, columns = part.shape
    return pl.pallas_call(
        upstream_kernel,
        out_shape=(
            jax.ShapeDtypeStruct(part.shape, BF16),
            jax.ShapeDtypeStruct((16 * state.shape[0], state.shape[1]), BF16),
            jax.ShapeDtypeStruct((16 * decay.shape[0], decay.shape[1]), F32),
        ),
        in_specs=[ANY, VMEM, ANY, ANY],
        out_specs=(VMEM, VMEM, VMEM),
        scratch_shapes=[
            pltpu.VMEM(part.shape, BF16),
            pltpu.VMEM((7 * rows, columns // 8), BF16),
            pltpu.SemaphoreType.DMA((3,)),
            *wires(90),
        ],
        compiler_params=params(number),
    )(part, residual, state, decay)


def dot_last(a, b):
    return lax.dot_general(a, b, (((1,), (1,)), ((), ())), preferred_element_type=F32)


def dot(a, b):
    return jnp.dot(a, b, preferred_element_type=F32)


def folded(value, op):
    parts = [value[:, k : k + 128] for k in range(0, value.shape[1], 128)]
    while len(parts) > 1:
        parts = [op(a, b) for a, b in zip(parts[::2], parts[1::2])]
    return parts[0]


CHUNK = 512


def fill_bias(bias, firsts, position, rows, length):
    row = lax.broadcasted_iota(jnp.int32, (rows, CHUNK), 0)
    low = jnp.where(row < BLK, firsts[0], firsts[1])
    high = row + position
    for k in range(0, length, CHUNK):
        column = lax.broadcasted_iota(jnp.int32, (rows, CHUNK), 1) + k
        seen = (column >= low) & (column <= high)
        bias[:, k : k + CHUNK] = jnp.where(seen, 0.0, -jnp.inf)


def one_head(q, g, kv, bias, raised, rounded, total, first):
    length = kv.shape[0]
    rows = q.shape[0]
    factor = 1.0 / math.sqrt(E)
    chunks = [slice(k, k + CHUNK) for k in range(0, length, CHUNK)]
    top = None
    for k in chunks:
        scores = dot_last(q, kv[k, :E]) + bias[:, k]
        raised[:, k] = scores
        most = folded(scores, jnp.maximum)
        top = most if top is None else jnp.maximum(top, most)
    top = jnp.max(top, axis=1, keepdims=True)
    whole = None
    for k in chunks:
        power = jnp.exp2((raised[:, k] - top) * (factor * math.log2(math.e)))
        raised[:, k] = power
        part = folded(power, jnp.add)
        whole = part if whole is None else whole + part
    inverse = 1.0 / jnp.sum(whole, axis=1, keepdims=True)
    outputs = jnp.zeros((rows, E), F32)
    for k in chunks:
        near_probs = (raised[:, k] * inverse).astype(BF16)
        rounded[:, k] = near_probs
        outputs = outputs + dot(near_probs, kv[k, E:])
    outputs = outputs.astype(BF16).astype(F32)
    delta = jnp.sum(g.astype(F32) * outputs, axis=1, keepdims=True)
    scaled = inverse * factor
    q_t = q.astype(F32).T.astype(BF16)
    g_t = g.astype(F32).T.astype(BF16)
    query_grad = jnp.zeros((rows, E), F32)
    for k in chunks:
        dprobs = dot_last(g, kv[k, E:])
        dscores = ((raised[:, k] * scaled) * (dprobs - delta)).astype(BF16)
        query_grad = query_grad + dot(dscores, kv[k, :E])
        total[:E, k] = total[:E, k] + dot(q_t, dscores)
        total[E:, k] = total[E:, k] + dot(g_t, rounded[:, k])
    return query_grad.astype(BF16)


def attend_kernel(firsts, q, g, kv, before, q_grad, after, bias, raised, rounded):
    rows, length = q.shape[0], kv.shape[0]
    fill_bias(bias, firsts, seq_index() * rows, rows, length)
    if before is None:
        after[...] = jnp.zeros_like(after)
    else:
        after[...] = before[...]

    def head(h, _):
        at = pl.ds(pl.multiple_of(h * E, E), E)
        q_grad[:, at] = one_head(q[:, at], g[:, at], kv, bias, raised, rounded, after, h)
        return 0

    lax.fori_loop(0, q.shape[1] // E, head, 0)


def attend(queries, grad_out, kv, firsts, before, final):
    rows, width = queries.shape
    length = kv.shape[0]
    kept = BF16 if final else F32
    operands = [firsts, queries, grad_out, kv]
    specs = [pl.BlockSpec(memory_space=pltpu.SMEM), VMEM, VMEM, VMEM]
    if before is not None:
        operands.append(before)
        specs.append(VMEM)

    def kernel(*refs):
        ins, rest = list(refs[: len(operands)]), refs[len(operands) :]
        if before is None:
            ins.append(None)
        q_grad, after, total, bias, raised, rounded = rest
        attend_kernel(*ins, q_grad, total, bias, raised, rounded)
        after[...] = total[...].astype(kept)

    return pl.pallas_call(
        kernel,
        out_shape=(
            jax.ShapeDtypeStruct((rows, width), BF16),
            jax.ShapeDtypeStruct((2 * E, length), kept),
        ),
        in_specs=specs,
        out_specs=(VMEM, VMEM),
        scratch_shapes=[
            pltpu.VMEM((2 * E, length), F32),
            pltpu.VMEM((rows, length), F32),
            pltpu.VMEM((rows, length), F32),
            pltpu.VMEM((rows, length), BF16),
        ],
        compiler_params=pltpu.CompilerParams(vmem_limit_bytes=56 * 1024 * 1024),
    )(*operands)


def weave(run, work, steps):
    work = list(work)
    each = -(-len(work) // steps)
    for _ in run:
        for item in work[:each]:
            item()
        work = work[each:]
    for item in work:
        item()


def flipped(value):
    return value.astype(F32).T


def log_decays(logs):
    t = lax.broadcasted_iota(jnp.int32, (RC, RC), 0)
    s = lax.broadcasted_iota(jnp.int32, (RC, RC), 1)
    upto = jnp.where(t <= s, 1.0, 0.0)
    rows, columns = [], []
    for c in range(logs.shape[1] // RC):
        part = jnp.dot(
            logs[:, c * RC : (c + 1) * RC],
            upto,
            precision=lax.Precision.HIGHEST,
            preferred_element_type=F32,
        )
        rows.append(part)
        tall = jnp.concatenate((part, jnp.zeros((RC - part.shape[0], RC), F32)), axis=0)
        columns.append(tall.T)
    return rows, columns


def spread(peers):
    z, xl = lax.axis_index("z"), lax.axis_index("xl")
    places = []
    for k in range(1, 8):
        to = (lax.rem(z + k // 2, 4), lax.rem(xl + k, 2))
        came = (lax.rem(z + 4 - k // 2, 4), lax.rem(xl + k, 2))
        places.append((to, came))
    return places


def open_kernel(
    mid_in, second_in, cot_in, wk_in, wv_in, wq_in, wo_in, ret_key, ret_value, logs,
    kv, q1, g1, q0, mid_t, slices, first_state, state, decay,
    mid, second, cot, wkv, wq1, wo1, wq0, flip, kept, local, sent, send, recv,
):
    rows = mid.shape[0]
    share = wkv.shape[0] // 8
    me = head_index()
    copies = bring(
        (mid_in, mid),
        (wk_in, wkv.at[:, pl.ds(0, E)]),
        (wv_in, wkv.at[:, pl.ds(E, E)]),
        (second_in, second),
        (wq_in.at[1], wq1),
        (cot_in, cot),
        (wo_in.at[1], wo1),
        (wq_in.at[0], wq0),
        sem=local,
    )
    places = spread(7)
    meet(seq_peers() + [{"z": a, "xl": b} for (a, b), _ in places])
    for copy in copies[:3]:
        copy.wait()
    wire = Wire(send, recv)
    at = by_rows(kv, rows)
    at(seq_index(), 0, rows)[...] = dot(mid[...], wkv[...]).astype(BF16)
    own = pltpu.make_async_copy(
        wkv.at[pl.ds(pl.multiple_of(me * share, share), share)], kept.at[me], sent.at[0]
    )
    own.start()

    def exchange():
        tickets = []
        for (a, b), (ca, cb) in places:
            src = wkv.at[pl.ds(pl.multiple_of((a * 2 + b) * share, share), share)]
            tickets.append((wire.put(src, kept.at[me], {"z": a, "xl": b}), ca * 2 + cb))
        yield
        yield
        yield
        yield
        yield
        for ticket, slot in tickets:
            wire.got(ticket, kept.at[slot])

    work = []

    def product(out, left, right, how, number):
        def first():
            copies[number].wait()
            if number != 7:
                copies[number - 1].wait()
            out[:, : 2 * E] = how(left, right, 0, 2 * E).astype(BF16)

        def rest():
            out[:, 2 * E :] = how(left, right, 2 * E, E).astype(BF16)

        work.extend((first, rest))

    def straight(left, right, at, count):
        return dot(left[...], right[:, at : at + count])

    def across(left, right, at, count):
        return dot_last(left[...], right[at : at + count])

    product(q1, second, wq1, straight, 4)
    product(g1, cot, wo1, across, 6)
    product(q0, mid, wq0, straight, 7)

    def states():
        arow, acol = log_decays(logs[...])
        total = arow[0][:, RC - 1 :] + arow[1][:, RC - 1 :]
        decay[:8] = jnp.broadcast_to(total, (8, 128))
        decay[8:] = jnp.zeros((8, 128), F32)
        for r in range(ret_key.shape[1] // E):
            cols = slice(r * E, (r + 1) * E)
            made = []
            for c in range(2):
                span = slice(c * RC, (c + 1) * RC)
                shrink = jnp.exp(arow[c][r : r + 1, RC - 1 :] - acol[c][:, r : r + 1])
                scaled = (shrink * ret_key[span, cols].astype(F32)).astype(BF16)
                made.append(dot(flipped(scaled).astype(BF16), ret_value[span, cols]))
            first_state[cols] = made[0]
            last = jnp.exp(arow[1][r : r + 1, RC - 1 :])
            state[cols] = (last * made[0] + made[1]).astype(BF16)

    work.append(states)

    def turn(k):
        def go():
            for j in range(k, k + 512, 128):
                flip[j : j + 128] = flipped(mid[:, j : j + 128]).astype(BF16)

        return go

    work.extend(turn(k) for k in range(0, mid.shape[1], 512))
    weave(together(gather_seq(wire, at, rows), exchange()), work, 6)
    own.wait()
    outs = [
        pltpu.make_async_copy(flip, mid_t, sent.at[1]),
        pltpu.make_async_copy(kept, slices, sent.at[2]),
    ]
    for copy in outs:
        copy.start()
    wire.drain()
    for copy in outs:
        copy.wait()


def open_stage(mid, second_in, cot, w_key, w_value, w_query, w_out, ret_key, ret_value, logs, number):
    rows, depth = mid.shape
    wide = w_query.shape[2]
    shape = jax.ShapeDtypeStruct
    return pl.pallas_call(
        open_kernel,
        out_shape=(
            shape((16 * rows, 2 * E), BF16),
            shape((rows, wide), BF16),
            shape((rows, wide), BF16),
            shape((rows, wide), BF16),
            shape((depth, rows), BF16),
            shape((8, depth // 8, 2 * E), BF16),
            shape((wide, E), F32),
            shape((wide, E), BF16),
            shape((16, 128), F32),
        ),
        in_specs=[ANY] * 7 + [VMEM] * 3,
        out_specs=(VMEM, VMEM, VMEM, VMEM, ANY, ANY, VMEM, VMEM, VMEM),
        scratch_shapes=[
            pltpu.VMEM((rows, depth), BF16),
            pltpu.VMEM((rows, depth), BF16),
            pltpu.VMEM((rows, depth), BF16),
            pltpu.VMEM((depth, 2 * E), BF16),
            pltpu.VMEM((depth, wide), BF16),
            pltpu.VMEM((wide, depth), BF16),
            pltpu.VMEM((depth, wide), BF16),
            pltpu.VMEM((depth, rows), BF16),
            pltpu.VMEM((8, depth // 8, 2 * E), BF16),
            pltpu.SemaphoreType.DMA((8,)),
            pltpu.SemaphoreType.DMA((3,)),
            *wires(30),
        ],
        compiler_params=params(number),
    )(mid, second_in, cot, w_key, w_value, w_query, w_out, ret_key, ret_value, logs)


def close_kernel(
    part_in, res_in, dkv_in, slices_in, mid_t_in, w_ret_in, states_in,
    rq, rk, rv, logs, decays, first_state,
    grad_mid, gq, gk, gv, gwk, gwv,
    acc_m, land_m, acc_k, land_k, kv_all, w_acc, w_land, w_sum, grads,
    residual, slices, mid_t, w_ret, states, local, send, recv,
):
    rows, depth = acc_m.shape
    share = depth // 8
    heads = rq.shape[1] // E
    me, here = head_index(), seq_index()
    copies = bring(
        (dkv_in, acc_k),
        (part_in, acc_m),
        (mid_t_in, mid_t),
        (slices_in, slices),
        (res_in, residual),
        (w_ret_in, w_ret),
        (states_in, states),
        sem=local,
    )
    meet(seq_peers() + head_peers())
    copies[0].wait()
    copies[1].wait()
    wire = Wire(send, recv)
    kv_at = by_rows(kv_all, rows, 4)
    w_rows = depth // 16
    w_at = by_rows(w_sum, w_rows)
    s_rows = heads * E
    s_at = by_rows(grads, s_rows)
    arow, acol = log_decays(logs[...])
    t = lax.broadcasted_iota(jnp.int32, (RC, RC), 0)
    s = lax.broadcasted_iota(jnp.int32, (RC, RC), 1)
    pieces = [(r, c) for r in range(heads) for c in range(2)]
    where = {(r, c): (slice(c * RC, (c + 1) * RC), slice(r * E, (r + 1) * E)) for r, c in pieces}
    weights, second, turned, entering, after = {}, {}, {}, {}, {}

    def end(r, c):
        return arow[c][r : r + 1, RC - 1 :]

    def prepare(r, c):
        a_t, a_s = acol[c][:, r : r + 1], arow[c][r : r + 1]
        lower = t >= s
        weights[r, c] = jnp.where(lower, jnp.exp(jnp.where(lower, a_t - a_s, 0.0)), 0.0)
        q, k = rq[where[r, c]], rk[where[r, c]]
        both = (weights[r, c] * dot_last(q, k)).astype(BF16)
        second[r, c] = flipped(both).astype(BF16)
        grown = (jnp.exp(a_t) * q.astype(F32)).astype(BF16)
        turned[r, c] = flipped(grown).astype(BF16)

    def arriving(r):
        cols = where[r, 0][1]
        now = jnp.zeros((E, E), F32)
        for k in range(15):
            mine = states[k * s_rows + r * E : k * s_rows + (r + 1) * E].astype(F32)
            new = jnp.exp(decays[k * 16 + r : k * 16 + r + 1]) * now + mine
            now = jnp.where(k < here, new, now)
        entering[r, 0] = now.astype(BF16)
        entering[r, 1] = (jnp.exp(end(r, 0)) * now + first_state[cols]).astype(BF16)

    def early():
        copies[6].wait()

    work = [early]
    for r in range(heads):
        work.append(lambda r=r: arriving(r))
    for r, c in pieces:
        work.append(lambda r=r, c=c: prepare(r, c))

    def keys():
        at = by_columns(acc_k, rows)
        rest = yield from scatter_seq(wire, at, rows, land_k)
        own = at(here, 0, rows)
        total = own[...].astype(F32) + rest[...].astype(F32)
        kv_at(me, 0, rows)[...] = total.T.astype(BF16)

    m_at = by_columns(acc_m, share)
    weave(together(keys(), scatter_head(wire, m_at, rows, land_m)), work, 3)
    own_kv = kv_at(me, 0, rows)
    gather_kv = gather_head(wire, kv_at, rows)
    next(gather_kv)
    copies[2].wait()
    w_acc[...] = dot(mid_t[...], own_kv[...]).astype(BF16)

    def sums():
        at = by_rows(w_acc, w_rows)
        rest = yield from scatter_seq(wire, at, w_rows, w_land)
        w_at(here, 0, w_rows)[...] = (
            at(here, 0, w_rows)[...].astype(F32) + rest[...].astype(F32)
        ).astype(BF16)
        yield
        yield from gather_seq(wire, w_at, w_rows)

    shared = sums()
    next(shared)
    finish(gather_kv)
    copies[3].wait()
    copies[4].wait()
    total = m_at(me, 0, rows)[...].astype(F32)
    total = total + residual[:, pl.ds(pl.multiple_of(me * share, 128), share)].astype(F32)
    for h in range(8):
        total = total + dot_last(kv_at(h, 0, rows)[...], slices[h])
    out_at = by_columns(grad_mid, share)
    out_at(me, 0, rows)[...] = total.astype(BF16)

    def beside(run):
        for _ in run:
            next(shared, None)

    beside(gather_head(wire, out_at, rows))
    copies[5].wait()
    grad_o = dot_last(grad_mid[...], w_ret[...]).astype(BF16)
    own_grad = {}
    for r, c in pieces:
        span, cols = where[r, c]
        own_grad[r, c] = dot(turned[r, c], grad_o[span, cols]) * (1.0 / E)
    for r in range(heads):
        made = own_grad[r, 0] + jnp.exp(end(r, 0)) * own_grad[r, 1]
        grads[pl.ds(pl.multiple_of(here * s_rows + r * E, E), E)] = made.astype(BF16)
    back = gather_seq(wire, s_at, s_rows)
    next(back)
    inner = {}

    def inside(r, c):
        span, cols = where[r, c]
        g, q, k, v = grad_o[span, cols], rq[span, cols], rk[span, cols], rv[span, cols]
        first = (weights[r, c] * dot_last(g, v)).astype(BF16)
        grow = jnp.exp(acol[c][:, r : r + 1])
        carried = grow * dot_last(g, entering[r, c])
        gq[span, cols] = ((dot(first, k) + carried) * (1.0 / E)).astype(BF16)
        inner[r, c] = (
            dot(flipped(first).astype(BF16), q) * (1.0 / E),
            dot(second[r, c], g) * (1.0 / E),
        )

    work = [lambda r=r, c=c: inside(r, c) for r, c in pieces]

    def both():
        for _ in back:
            next(shared, None)
            yield

    weave(both(), work, 5)
    for r in range(heads):
        now = jnp.zeros((E, E), F32)
        for k in range(15, 0, -1):
            mine = grads[k * s_rows + r * E : k * s_rows + (r + 1) * E].astype(F32)
            new = mine + jnp.exp(decays[k * 16 + r : k * 16 + r + 1]) * now
            now = jnp.where(k > here, new, now)
        after[r, 1] = now.astype(BF16)
        after[r, 0] = (own_grad[r, 1] + jnp.exp(end(r, 1)) * now).astype(BF16)
    for r, c in pieces:
        span, cols = where[r, c]
        shrink = jnp.exp(end(r, c) - acol[c][:, r : r + 1])
        gk[span, cols] = (
            inner[r, c][0] + shrink * dot_last(rv[span, cols], after[r, c])
        ).astype(BF16)
        gv[span, cols] = (inner[r, c][1] + shrink * dot(rk[span, cols], after[r, c])).astype(BF16)
    finish(shared)
    gwk[...] = w_sum[:, :E].astype(F32)
    gwv[...] = w_sum[:, E:].astype(F32)
    wire.drain()


def close_stage(
    part, residual, dkv, slices, mid_t, w_ret, states, rq, rk, rv, logs, decays, first_state, number
):
    rows, depth = part.shape
    width = rq.shape[1]
    shape = jax.ShapeDtypeStruct
    return pl.pallas_call(
        close_kernel,
        out_shape=(
            shape((rows, depth), BF16),
            shape((rows, width), BF16),
            shape((rows, width), BF16),
            shape((rows, width), BF16),
            shape((depth, E), F32),
            shape((depth, E), F32),
        ),
        in_specs=[ANY] * 7 + [VMEM] * 6,
        out_specs=(VMEM,) * 6,
        scratch_shapes=[
            pltpu.VMEM(part.shape, BF16),
            pltpu.VMEM((7 * rows, depth // 8), BF16),
            pltpu.VMEM(dkv.shape, BF16),
            pltpu.VMEM((15 * rows, dkv.shape[1] // 16), BF16),
            pltpu.VMEM((8 * rows, 2 * E), BF16),
            pltpu.VMEM((depth, 2 * E), BF16),
            pltpu.VMEM((15 * depth // 16, 2 * E), BF16),
            pltpu.VMEM((depth, 2 * E), BF16),
            pltpu.VMEM(states.shape, BF16),
            pltpu.VMEM(residual.shape, BF16),
            pltpu.VMEM(slices.shape, BF16),
            pltpu.VMEM(mid_t.shape, BF16),
            pltpu.VMEM(w_ret.shape, BF16),
            pltpu.VMEM(states.shape, BF16),
            pltpu.SemaphoreType.DMA((7,)),
            *wires(180),
        ],
        compiler_params=params(number),
    )(part, residual, dkv, slices, mid_t, w_ret, states, rq, rk, rv, logs, decays, first_state)


def contract_last(left, right):
    return lax.dot_general(
        left, right, (((1,), (1,)), ((), ())), preferred_element_type=jnp.float32
    )


def local(
    mid,
    second_in,
    cotangent,
    w_key,
    w_value,
    w_query,
    w_out,
    w_ret_out,
    ret_query,
    ret_key,
    ret_value,
    gate,
    decay_exp,
    mask_start,
):
    rate = jnp.exp2(-decay_exp.astype(F32) / 64.0)
    logs = jnp.pad(-rate[:, None] * gate, ((0, 8 - gate.shape[0]), (0, 0)))
    kv, q1, g1, q0, mid_t, slices, first_state, state, decay = open_stage(
        mid, second_in, cotangent, w_key, w_value, w_query, w_out, ret_key, ret_value, logs, 0
    )
    upper_grad, upper_kv = attend(q1, g1, kv, mask_start, None, False)
    upper_in = contract_last(upper_grad, w_query[1])
    upstream, states, decays = upstream_of(upper_in.astype(BF16), cotangent, state, decay, 1)
    g0 = contract_last(upstream, w_out[0]).astype(BF16)
    lower_grad, kv_part = attend(q0, g0, kv, mask_start, upper_kv, True)
    lower_in = contract_last(lower_grad, w_query[0])
    return close_stage(
        lower_in.astype(BF16),
        upstream,
        kv_part,
        slices,
        mid_t,
        w_ret_out,
        states,
        ret_query,
        ret_key,
        ret_value,
        logs,
        decays,
        first_state,
        2,
    )


def solution(mesh):
    torus = Mesh(mesh.devices.reshape(2, 4, 2, 4, 2), ("xh", "y", "core", "z", "xl"))
    in_specs = (
        P(SEQ, None),
        P(SEQ, None),
        P(SEQ, None),
        P(None, HEAD),
        P(None, HEAD),
        P(None, None, HEAD),
        P(None, HEAD, None),
        P(HEAD, None),
        P(SEQ, HEAD),
        P(SEQ, HEAD),
        P(SEQ, HEAD),
        P(HEAD, SEQ),
        P(HEAD),
        P(SEQ),
    )
    out_specs = (
        P(SEQ, None),
        P(SEQ, HEAD),
        P(SEQ, HEAD),
        P(SEQ, HEAD),
        P(None, HEAD),
        P(None, HEAD),
    )
    return jax.shard_map(local, mesh=torus, in_specs=in_specs, out_specs=out_specs, check_vma=False)
```

```python
import functools
import math

import jax
import jax.numpy as jnp
from jax import lax
from jax.experimental import pallas as pl
from jax.experimental.pallas import tpu as pltpu
from jax.sharding import Mesh
from jax.sharding import PartitionSpec as P

E = 128
BLK = 128
RC = 128
SEQ = ("xh", "y", "core")
HEAD = ("z", "xl")

MESH = pl.DeviceIdType.MESH
BF16 = jnp.bfloat16
F32 = jnp.float32


class Wire:
    def __init__(self, send, recv):
        self.send, self.recv, self.sent, self.used = send, recv, [], 0
        self.work, self.pace = [], 1

    def idle(self, count):
        for item in self.work[:count]:
            item()
        self.work = self.work[count:]

    def put(self, src, dst, to):
        k = self.used
        self.used += 1
        copy = pltpu.make_async_remote_copy(
            src_ref=src,
            dst_ref=dst,
            send_sem=self.send.at[k],
            recv_sem=self.recv.at[k],
            device_id=to,
            device_id_type=MESH,
        )
        copy.start()
        self.sent.append(copy)
        return (k, to)

    def got(self, ticket, landed):
        self.idle(self.pace)
        k, to = ticket
        pltpu.make_async_remote_copy(
            src_ref=landed,
            dst_ref=landed,
            send_sem=self.send.at[k],
            recv_sem=self.recv.at[k],
            device_id=to,
            device_id_type=MESH,
        ).wait_recv()

    def drain(self):
        for copy in self.sent:
            copy.wait_send()


def meet(peers):
    barrier = pltpu.get_barrier_semaphore()
    for to in peers:
        pl.semaphore_signal(barrier, inc=1, device_id=to, device_id_type=MESH)
    pl.semaphore_wait(barrier, len(peers))


def near(axis):
    at = lax.axis_index(axis)
    return at, lax.rem(at + 1, 4), lax.rem(at + 3, 4), lax.rem(at + 2, 4)


def seq_peers():
    y, yp, ym, y2 = near("y")
    return [
        {"xh": 1 - lax.axis_index("xh")},
        {"y": yp},
        {"y": ym},
        {"core": 1 - lax.axis_index("core")},
    ]


def head_peers():
    z, zp, zm, z2 = near("z")
    return [{"xl": 1 - lax.axis_index("xl")}, {"z": zp}, {"z": zm}]


def by_rows(ref, rows, parts=2):
    step = rows // parts

    def at(slot, first, count):
        return ref.at[pl.ds(pl.multiple_of(slot * rows + first, step), count)]

    return at


def by_columns(ref, width):
    def at(slot, first, count):
        return ref.at[pl.ds(first, count), pl.ds(pl.multiple_of(slot * width, 128), width)]

    return at


def add_to(total, part):
    total[...] = (total[...].astype(F32) + part[...].astype(F32)).astype(total.dtype)


def together(*runs):
    runs = list(runs)
    while runs:
        for run in list(runs):
            try:
                next(run)
            except StopIteration:
                runs.remove(run)
        yield


def finish(run):
    for _ in run:
        pass


def gather_seq(wire, at, rows):
    xh, c = lax.axis_index("xh"), lax.axis_index("core")
    y, yp, ym, y2 = near("y")
    xo, co = 1 - xh, 1 - c
    half = rows // 2
    whole, low, high = (0, rows), (0, half), (half, half)
    across, up, down, beside = {"xh": xo}, {"y": yp}, {"y": ym}, {"core": co}

    def slot(a, b, d):
        return a * 8 + b * 2 + d

    def pass_on(s, part, to):
        return wire.put(at(s, *part), at(s, *part), to)

    side = []
    own, far = slot(xh, y, c), slot(xo, y, c)
    t_x = pass_on(own, whole, across)
    ups, downs = [pass_on(own, whole, up)], [pass_on(own, whole, down)]
    side.append((pass_on(own, whole, beside), slot(xh, y, co)))
    yield
    wire.got(t_x, at(far, *whole))
    ups.append(pass_on(far, whole, up))
    downs.append(pass_on(far, whole, down))
    side.append((pass_on(far, whole, beside), slot(xo, y, co)))
    yield
    last = []
    for k, q in enumerate((xh, xo)):
        wire.got(ups[k], at(slot(q, ym, c), *whole))
        a = pass_on(slot(q, ym, c), low, up)
        side.append((pass_on(slot(q, ym, c), whole, beside), slot(q, ym, co)))
        wire.got(downs[k], at(slot(q, yp, c), *whole))
        b = pass_on(slot(q, yp, c), high, down)
        side.append((pass_on(slot(q, yp, c), whole, beside), slot(q, yp, co)))
        last.append((a, b))
        yield
    for k, q in enumerate((xh, xo)):
        wire.got(last[k][0], at(slot(q, y2, c), *low))
        wire.got(last[k][1], at(slot(q, y2, c), *high))
        side.append((pass_on(slot(q, y2, c), whole, beside), slot(q, y2, co)))
        yield
    for ticket, s in side:
        wire.got(ticket, at(s, *whole))


def ring_scatter(wire, at, slot, axis, first, count, land, before=None):
    r, rp, rm, r2 = near(axis)
    up, down = {axis: rp}, {axis: rm}
    half = count // 2
    wait = before or (lambda j: None)
    low, high = land.at[pl.ds(0, half)], land.at[pl.ds(half, half)]
    from_up, from_down = land.at[pl.ds(count, count)], land.at[pl.ds(2 * count, count)]
    wait(2)
    a = wire.put(at(slot(r2), first, half), low, up)
    b = wire.put(at(slot(r2), first + half, half), high, down)
    yield
    wait(1)
    wire.got(a, low)
    add_to(at(slot(rp), first, half), low)
    u = wire.put(at(slot(rp), first, count), from_down, up)
    wait(3)
    wire.got(b, high)
    add_to(at(slot(rm), first + half, half), high)
    d = wire.put(at(slot(rm), first, count), from_up, down)
    yield
    wait(0)
    wire.got(u, from_down)
    add_to(at(slot(r), first, count), from_down)
    wire.got(d, from_up)
    add_to(at(slot(r), first, count), from_up)


def scatter_seq(wire, at, rows, land):
    xh, c = lax.axis_index("xh"), lax.axis_index("core")
    y, yp, ym, y2 = near("y")
    xo, co = 1 - xh, 1 - c

    def slot(a, b, d):
        return a * 8 + b * 2 + d

    def block(k, count=1):
        return land.at[pl.ds(k * rows, count * rows)]

    places = {0: y, 1: yp, 2: y2, 3: ym}
    side = {}
    for n, q in enumerate((xo, xh)):
        for m, j in enumerate((2, 1, 3, 0)):
            dst = block(4 * n + m)
            side[n, j] = (wire.put(at(slot(q, places[j], co), 0, rows), dst, {"core": co}), dst)

    def before(n, q):
        def wait(j):
            ticket, dst = side[n, j]
            wire.got(ticket, dst)
            add_to(at(slot(q, places[j], c), 0, rows), dst)

        return wait

    def ring(n, q):
        return ring_scatter(
            wire, at, lambda j: slot(q, j, c), "y", 0, rows, block(8 + 3 * n, 3), before(n, q)
        )

    sent = []

    def far():
        yield from ring(0, xo)
        sent.append(wire.put(at(slot(xo, y, c), 0, rows), block(14), {"xh": xo}))

    yield from together(far(), ring(1, xh))
    wire.got(sent[0], block(14))
    return block(14)


def scatter_head(wire, at, rows, land):
    xl = lax.axis_index("xl")
    z, zp, zm, z2 = near("z")
    xo = 1 - xl
    half = rows // 2

    def slot(j, q):
        return j * 2 + q

    def block(k, count=1):
        return land.at[pl.ds(k * half, count * half)]

    places = {0: z, 1: zp, 2: z2, 3: zm}
    side = {}
    for m, j in enumerate((2, 1, 3, 0)):
        side[j] = (wire.put(at(slot(places[j], xo), 0, half), block(m), {"xl": xo}), block(m))

    def wait(j):
        ticket, dst = side[j]
        wire.got(ticket, dst)
        add_to(at(slot(places[j], xl), 0, half), dst)

    sent = []

    def far():
        yield from ring_scatter(
            wire, at, lambda j: slot(j, xo), "z", half, half, block(4, 3)
        )
        sent.append(wire.put(at(slot(z, xo), half, half), block(13), {"xl": xo}))

    yield from together(
        far(),
        ring_scatter(wire, at, lambda j: slot(j, xl), "z", half, half, block(7, 3)),
        ring_scatter(wire, at, lambda j: slot(j, xl), "z", 0, half, block(10, 3), wait),
    )
    wire.got(sent[0], block(13))
    add_to(at(slot(z, xl), half, half), block(13))


def gather_head(wire, at, rows):
    xl = lax.axis_index("xl")
    z, zp, zm, z2 = near("z")
    xo = 1 - xl
    half = rows // 2
    up, down, across = {"z": zp}, {"z": zm}, {"xl": xo}

    def slot(j, q):
        return j * 2 + q

    def pass_on(s, first, count, to):
        return wire.put(at(s, first, count), at(s, first, count), to)

    def ring(q, first, each=None):
        h = half // 2
        tell = each or (lambda j: None)
        a = pass_on(slot(z, q), first, half, up)
        b = pass_on(slot(z, q), first, half, down)
        tell(z)
        yield
        wire.got(a, at(slot(zm, q), first, half))
        c = pass_on(slot(zm, q), first, h, up)
        tell(zm)
        wire.got(b, at(slot(zp, q), first, half))
        d = pass_on(slot(zp, q), first + h, h, down)
        tell(zp)
        yield
        wire.got(c, at(slot(z2, q), first, h))
        wire.got(d, at(slot(z2, q), first + h, h))
        tell(z2)

    side = []

    def tell(j):
        side.append((pass_on(slot(j, xl), 0, half, across), slot(j, xo)))

    t_x = pass_on(slot(z, xl), half, half, across)

    def far():
        wire.got(t_x, at(slot(z, xo), half, half))
        yield from ring(xo, half)

    yield from together(ring(xl, 0, tell), ring(xl, half), far())
    for ticket, s in side:
        wire.got(ticket, at(s, 0, half))


ANY = pl.BlockSpec(memory_space=pl.ANY)
VMEM = pl.BlockSpec(memory_space=pltpu.VMEM)


def wires(count):
    return [pltpu.SemaphoreType.DMA((count,)), pltpu.SemaphoreType.DMA((count,))]


def params(number):
    return pltpu.CompilerParams(collective_id=number, has_side_effects=True)


def bring(*pairs, sem):
    copies = [pltpu.make_async_copy(s, d, sem.at[k]) for k, (s, d) in enumerate(pairs)]
    for copy in copies:
        copy.start()
    return copies


def seq_index():
    return lax.axis_index("xh") * 8 + lax.axis_index("y") * 2 + lax.axis_index("core")


def head_index():
    return lax.axis_index("z") * 2 + lax.axis_index("xl")


def total_into(out_at, acc_at, residual, rows, width):
    me = head_index()
    own = acc_at(me, 0, rows)
    kept = residual.at[pl.ds(0, rows), pl.ds(pl.multiple_of(me * width, 128), width)]
    out_at(me, 0, rows)[...] = (kept[...].astype(F32) + own[...].astype(F32)).astype(BF16)


def head_run(wire, acc, land, residual, out):
    rows, columns = acc.shape
    width = columns // 8
    yield from scatter_head(wire, by_columns(acc, width), rows, land)
    total_into(by_columns(out, width), by_columns(acc, width), residual, rows, width)
    yield from gather_head(wire, by_columns(out, width), rows)


def dot_last(a, b):
    return lax.dot_general(a, b, (((1,), (1,)), ((), ())), preferred_element_type=F32)


def dot(a, b):
    return jnp.dot(a, b, preferred_element_type=F32)


def folded(value, op):
    parts = [value[:, k : k + 128] for k in range(0, value.shape[1], 128)]
    while len(parts) > 1:
        parts = [op(a, b) for a, b in zip(parts[::2], parts[1::2])]
    return parts[0]


CHUNK = 512


def fill_bias(bias, firsts, position, rows, length):
    row = lax.broadcasted_iota(jnp.int32, (rows, CHUNK), 0)
    low = jnp.where(row < BLK, firsts[0], firsts[1])
    high = row + position
    for k in range(0, length, CHUNK):
        column = lax.broadcasted_iota(jnp.int32, (rows, CHUNK), 1) + k
        seen = (column >= low) & (column <= high)
        bias[:, k : k + CHUNK] = jnp.where(seen, 0.0, -jnp.inf)


def flipped(value):
    return value.astype(F32).T


def log_decays(logs):
    t = lax.broadcasted_iota(jnp.int32, (RC, RC), 0)
    s = lax.broadcasted_iota(jnp.int32, (RC, RC), 1)
    upto = jnp.where(t <= s, 1.0, 0.0)
    rows, columns = [], []
    for c in range(logs.shape[1] // RC):
        part = jnp.dot(
            logs[:, c * RC : (c + 1) * RC],
            upto,
            precision=lax.Precision.HIGHEST,
            preferred_element_type=F32,
        )
        rows.append(part)
        tall = jnp.concatenate((part, jnp.zeros((RC - part.shape[0], RC), F32)), axis=0)
        columns.append(tall.T)
    return rows, columns


def spread(peers):
    z, xl = lax.axis_index("z"), lax.axis_index("xl")
    places = []
    for k in range(1, 8):
        to = (lax.rem(z + k // 2, 4), lax.rem(xl + k, 2))
        came = (lax.rem(z + 4 - k // 2, 4), lax.rem(xl + k, 2))
        places.append((to, came))
    return places


def open_kernel(
    mid_in, second_in, cot_in, wk_in, wv_in, wq_in, wo_in, ret_key, ret_value, gate, decay_exp,
    kv, q1, g1, q0, mid_t, slices, first_state, state, decay, logs,
    mid, second, cot, wkv, wq1, wo1, wq0, flip, kept, local, sent, send, recv,
):
    rows = mid.shape[0]
    share = wkv.shape[0] // 8
    me = head_index()
    copies = bring(
        (mid_in, mid),
        (wk_in, wkv.at[:, pl.ds(0, E)]),
        (wv_in, wkv.at[:, pl.ds(E, E)]),
        sem=local,
    )
    places = spread(7)
    meet(seq_peers() + [{"z": a, "xl": b} for (a, b), _ in places])
    for copy in copies:
        copy.wait()
    copies += bring(
        (second_in, second),
        (wq_in.at[1], wq1),
        (cot_in, cot),
        (wo_in.at[1], wo1),
        (wq_in.at[0], wq0),
        sem=local.at[pl.ds(3, 5)],
    )
    wire = Wire(send, recv)
    at = by_rows(kv, rows)
    at(seq_index(), 0, rows)[...] = dot(mid[...], wkv[...]).astype(BF16)
    own = pltpu.make_async_copy(
        wkv.at[pl.ds(pl.multiple_of(me * share, share), share)], kept.at[me], sent.at[0]
    )
    own.start()

    def exchange():
        tickets = []
        for (a, b), (ca, cb) in places:
            src = wkv.at[pl.ds(pl.multiple_of((a * 2 + b) * share, share), share)]
            tickets.append((wire.put(src, kept.at[me], {"z": a, "xl": b}), ca * 2 + cb))
        yield
        yield
        yield
        yield
        yield
        for ticket, slot in tickets:
            wire.got(ticket, kept.at[slot])

    work = []

    def product(out, left, right, how, number):
        def part(k):
            def go():
                if k == 0:
                    copies[number].wait()
                    if number != 7:
                        copies[number - 1].wait()
                out[:, k : k + E] = how(left, right, k, E).astype(BF16)

            return go

        work.extend(part(k) for k in range(0, out.shape[1], E))

    def straight(left, right, at, count):
        return dot(left[...], right[:, at : at + count])

    def across(left, right, at, count):
        return dot_last(left[...], right[at : at + count])

    def rates():
        row = lax.broadcasted_iota(jnp.int32, (8, 128), 0)
        rate = jnp.zeros((8, 128), F32)
        for r in range(gate.shape[0]):
            power = jnp.full((8, 128), decay_exp[r], jnp.int32).astype(F32)
            rate = jnp.where(row == r, jnp.exp2(power * (-1.0 / 64.0)), rate)
        empty = jnp.zeros((8 - gate.shape[0], gate.shape[1]), F32)
        tall = jnp.concatenate((gate[...], empty), axis=0)
        logs[...] = -rate[:, :1] * tall

    def states():
        arow, acol = log_decays(logs[...])
        total = arow[0][:, RC - 1 :] + arow[1][:, RC - 1 :]
        decay[:8] = jnp.broadcast_to(total, (8, 128))
        decay[8:] = jnp.zeros((8, 128), F32)
        for r in range(ret_key.shape[1] // E):
            cols = slice(r * E, (r + 1) * E)
            made = []
            for c in range(2):
                span = slice(c * RC, (c + 1) * RC)
                shrink = jnp.exp(arow[c][r : r + 1, RC - 1 :] - acol[c][:, r : r + 1])
                scaled = (shrink * ret_key[span, cols].astype(F32)).astype(BF16)
                made.append(dot(flipped(scaled).astype(BF16), ret_value[span, cols]))
            first_state[cols] = made[0]
            last = jnp.exp(arow[1][r : r + 1, RC - 1 :])
            state[cols] = (last * made[0] + made[1]).astype(BF16)

    def turn(k):
        def go():
            for j in range(k, k + 512, 128):
                flip[j : j + 128] = flipped(mid[:, j : j + 128]).astype(BF16)

        return go

    product(q1, second, wq1, straight, 4)
    product(g1, cot, wo1, across, 6)
    product(q0, mid, wq0, straight, 7)
    turns = [turn(k) for k in range(0, mid.shape[1], 512)]
    wire.work = [rates, states, turns[0]] + work + turns[1:]
    finish(together(gather_seq(wire, at, rows), exchange()))
    wire.idle(len(wire.work))
    own.wait()
    outs = [
        pltpu.make_async_copy(flip, mid_t, sent.at[1]),
        pltpu.make_async_copy(kept, slices, sent.at[2]),
    ]
    for copy in outs:
        copy.start()
    wire.drain()
    for copy in outs:
        copy.wait()


def open_stage(number, *operands):
    mid, w_query = operands[0], operands[5]
    rows, depth = mid.shape
    wide = w_query.shape[2]
    shape = jax.ShapeDtypeStruct
    return pl.pallas_call(
        open_kernel,
        out_shape=(
            shape((16 * rows, 2 * E), BF16),
            shape((rows, wide), BF16),
            shape((rows, wide), BF16),
            shape((rows, wide), BF16),
            shape((depth, rows), BF16),
            shape((8, depth // 8, 2 * E), BF16),
            shape((wide, E), F32),
            shape((wide, E), BF16),
            shape((16, 128), F32),
            shape((8, rows), F32),
        ),
        in_specs=[ANY] * 7 + [VMEM] * 3 + [pl.BlockSpec(memory_space=pltpu.SMEM)],
        out_specs=(VMEM, VMEM, VMEM, VMEM, ANY, ANY, VMEM, VMEM, VMEM, VMEM),
        scratch_shapes=[
            pltpu.VMEM((rows, depth), BF16),
            pltpu.VMEM((rows, depth), BF16),
            pltpu.VMEM((rows, depth), BF16),
            pltpu.VMEM((depth, 2 * E), BF16),
            pltpu.VMEM((depth, wide), BF16),
            pltpu.VMEM((wide, depth), BF16),
            pltpu.VMEM((depth, wide), BF16),
            pltpu.VMEM((depth, rows), BF16),
            pltpu.VMEM((8, depth // 8, 2 * E), BF16),
            pltpu.SemaphoreType.DMA((8,)),
            pltpu.SemaphoreType.DMA((3,)),
            *wires(30),
        ],
        compiler_params=params(number),
    )(*operands)


def close_kernel(
    part_in, dkv_in, slices_in, mid_t_in, w_ret_in, states_in,
    own_res, rq, rk, rv, logs, decays, first_state,
    mid_out, gq, gk, gv, w_sum,
    grad_mid, acc_m, land_m, acc_k, land_k, kv_all, w_acc, w_land, grads,
    slices, mid_t, w_ret, states, local, send, recv,
):
    rows, depth = acc_m.shape
    share = depth // 8
    heads = rq.shape[1] // E
    me, here = head_index(), seq_index()
    copies = bring(
        (dkv_in, acc_k),
        (part_in, acc_m),
        (mid_t_in, mid_t),
        (slices_in, slices),
        (w_ret_in, w_ret),
        (states_in, states),
        sem=local,
    )
    meet(seq_peers() + head_peers())
    copies[0].wait()
    copies[1].wait()
    wire = Wire(send, recv)
    kv_at = by_rows(kv_all, rows, 4)
    w_rows = depth // 16
    w_at = by_rows(w_sum, w_rows)
    s_rows = heads * E
    s_at = by_rows(grads, s_rows)
    arow, acol = log_decays(logs[...])
    t = lax.broadcasted_iota(jnp.int32, (RC, RC), 0)
    s = lax.broadcasted_iota(jnp.int32, (RC, RC), 1)
    pieces = [(r, c) for r in range(heads) for c in range(2)]
    where = {(r, c): (slice(c * RC, (c + 1) * RC), slice(r * E, (r + 1) * E)) for r, c in pieces}
    weights, second, turned, entering, after = {}, {}, {}, {}, {}

    def end(r, c):
        return arow[c][r : r + 1, RC - 1 :]

    def prepare(r, c):
        a_t, a_s = acol[c][:, r : r + 1], arow[c][r : r + 1]
        lower = t >= s
        weights[r, c] = jnp.where(lower, jnp.exp(jnp.where(lower, a_t - a_s, 0.0)), 0.0)
        q, k = rq[where[r, c]], rk[where[r, c]]
        both = (weights[r, c] * dot_last(q, k)).astype(BF16)
        second[r, c] = flipped(both).astype(BF16)
        grown = (jnp.exp(a_t) * q.astype(F32)).astype(BF16)
        turned[r, c] = flipped(grown).astype(BF16)

    def arriving(r):
        cols = where[r, 0][1]
        now = jnp.zeros((E, E), F32)
        for k in range(15):
            mine = states[k * s_rows + r * E : k * s_rows + (r + 1) * E].astype(F32)
            new = jnp.exp(decays[k * 16 + r : k * 16 + r + 1]) * now + mine
            now = jnp.where(k < here, new, now)
        entering[r, 0] = now.astype(BF16)
        entering[r, 1] = (jnp.exp(end(r, 0)) * now + first_state[cols]).astype(BF16)

    def early():
        copies[5].wait()

    work = [early]
    for r in range(heads):
        work.append(lambda r=r: arriving(r))
    for r, c in pieces:
        work.append(lambda r=r, c=c: prepare(r, c))

    def keys():
        at = by_columns(acc_k, rows)
        rest = yield from scatter_seq(wire, at, rows, land_k)
        own = at(here, 0, rows)
        total = own[...].astype(F32) + rest[...].astype(F32)
        kv_at(me, 0, rows)[...] = total.T.astype(BF16)

    m_at = by_columns(acc_m, share)
    wire.work = work
    finish(together(keys(), scatter_head(wire, m_at, rows, land_m)))
    wire.idle(len(wire.work))
    own_kv = kv_at(me, 0, rows)
    gather_kv = gather_head(wire, kv_at, rows)
    next(gather_kv)
    copies[2].wait()
    w_acc[...] = dot(mid_t[...], own_kv[...]).astype(BF16)

    def sums():
        at = by_rows(w_acc, w_rows)
        rest = yield from scatter_seq(wire, at, w_rows, w_land)
        w_at(here, 0, w_rows)[...] = (
            at(here, 0, w_rows)[...].astype(F32) + rest[...].astype(F32)
        ).astype(BF16)
        yield
        yield from gather_seq(wire, w_at, w_rows)

    shared = sums()
    next(shared)
    finish(gather_kv)
    copies[3].wait()
    total = m_at(me, 0, rows)[...].astype(F32) + own_res[...].astype(F32)
    for h in range(8):
        total = total + dot_last(kv_at(h, 0, rows)[...], slices[h])
    out_at = by_columns(grad_mid, share)
    out_at(me, 0, rows)[...] = total.astype(BF16)

    def beside(run):
        for _ in run:
            next(shared, None)

    beside(gather_head(wire, out_at, rows))
    shown = pltpu.make_async_copy(grad_mid, mid_out, local.at[6])
    shown.start()
    copies[4].wait()
    grad_o = dot_last(grad_mid[...], w_ret[...]).astype(BF16)
    own_grad = {}
    for r, c in pieces:
        span, cols = where[r, c]
        own_grad[r, c] = dot(turned[r, c], grad_o[span, cols]) * (1.0 / E)
    for r in range(heads):
        made = own_grad[r, 0] + jnp.exp(end(r, 0)) * own_grad[r, 1]
        grads[pl.ds(pl.multiple_of(here * s_rows + r * E, E), E)] = made.astype(BF16)
    back = gather_seq(wire, s_at, s_rows)
    next(back)
    inner = {}

    def inside(r, c):
        span, cols = where[r, c]
        g, q, k, v = grad_o[span, cols], rq[span, cols], rk[span, cols], rv[span, cols]
        first = (weights[r, c] * dot_last(g, v)).astype(BF16)
        grow = jnp.exp(acol[c][:, r : r + 1])
        carried = grow * dot_last(g, entering[r, c])
        gq[span, cols] = ((dot(first, k) + carried) * (1.0 / E)).astype(BF16)
        inner[r, c] = (
            dot(flipped(first).astype(BF16), q) * (1.0 / E),
            dot(second[r, c], g) * (1.0 / E),
        )

    wire.work = [lambda r=r, c=c: inside(r, c) for r, c in pieces]
    beside(back)
    wire.idle(len(wire.work))
    for r in range(heads):
        now = jnp.zeros((E, E), F32)
        for k in range(15, 0, -1):
            mine = grads[k * s_rows + r * E : k * s_rows + (r + 1) * E].astype(F32)
            new = mine + jnp.exp(decays[k * 16 + r : k * 16 + r + 1]) * now
            now = jnp.where(k > here, new, now)
        after[r, 1] = now.astype(BF16)
        after[r, 0] = (own_grad[r, 1] + jnp.exp(end(r, 1)) * now).astype(BF16)
    for r, c in pieces:
        span, cols = where[r, c]
        shrink = jnp.exp(end(r, c) - acol[c][:, r : r + 1])
        gk[span, cols] = (
            inner[r, c][0] + shrink * dot_last(rv[span, cols], after[r, c])
        ).astype(BF16)
        gv[span, cols] = (inner[r, c][1] + shrink * dot(rk[span, cols], after[r, c])).astype(BF16)
    finish(shared)
    shown.wait()
    wire.drain()


def close_stage(number, *operands):
    part, dkv, slices, mid_t, w_ret, states = operands[:6]
    rows, depth = part.shape
    width = operands[7].shape[1]
    shape = jax.ShapeDtypeStruct
    return pl.pallas_call(
        close_kernel,
        out_shape=(
            shape((rows, depth), BF16),
            shape((rows, width), BF16),
            shape((rows, width), BF16),
            shape((rows, width), BF16),
            shape((depth, 2 * E), BF16),
        ),
        in_specs=[ANY] * 6 + [VMEM] * 7,
        out_specs=(ANY, VMEM, VMEM, VMEM, VMEM),
        scratch_shapes=[
            pltpu.VMEM(part.shape, BF16),
            pltpu.VMEM(part.shape, BF16),
            pltpu.VMEM((7 * rows, depth // 8), BF16),
            pltpu.VMEM(dkv.shape, BF16),
            pltpu.VMEM((15 * rows, dkv.shape[1] // 16), BF16),
            pltpu.VMEM((8 * rows, 2 * E), BF16),
            pltpu.VMEM((depth, 2 * E), BF16),
            pltpu.VMEM((15 * depth // 16, 2 * E), BF16),
            pltpu.VMEM(states.shape, BF16),
            pltpu.VMEM(slices.shape, BF16),
            pltpu.VMEM(mid_t.shape, BF16),
            pltpu.VMEM(w_ret.shape, BF16),
            pltpu.VMEM(states.shape, BF16),
            pltpu.SemaphoreType.DMA((7,)),
            *wires(180),
        ],
        compiler_params=params(number),
    )(*operands)


def hand_out_kernel(*refs):
    ins, outs, held, (wide, sem_in, sem_out) = refs[:5], refs[5:11], refs[11:16], refs[16:]
    copies = bring(*zip(ins, held), sem=sem_in)
    sends = []
    for k in range(4):
        copies[k].wait()
        sends.append(pltpu.make_async_copy(held[k], outs[k], sem_out.at[k]))
        sends[-1].start()
    copies[4].wait()
    for k in range(2):
        wide[k] = held[4][:, k * E : (k + 1) * E].astype(F32)
        sends.append(pltpu.make_async_copy(wide.at[k], outs[4 + k], sem_out.at[4 + k]))
        sends[-1].start()
    for send in sends:
        send.wait()


def hand_out(*arrays):
    shape = jax.ShapeDtypeStruct
    depth = arrays[4].shape[0]
    return pl.pallas_call(
        hand_out_kernel,
        out_shape=tuple(shape(a.shape, a.dtype) for a in arrays[:4])
        + (shape((depth, E), F32), shape((depth, E), F32)),
        in_specs=[ANY] * 5,
        out_specs=(ANY,) * 6,
        scratch_shapes=[pltpu.VMEM(a.shape, a.dtype) for a in arrays]
        + [
            pltpu.VMEM((2, depth, E), F32),
            pltpu.SemaphoreType.DMA((5,)),
            pltpu.SemaphoreType.DMA((6,)),
        ],
    )(*arrays)


def scores_pass(q, kv, bias, raised, stats):
    def part(k):
        def go():
            for at in (slice(k, k + CHUNK), slice(k + CHUNK, k + 2 * CHUNK)):
                scores = dot_last(q(), kv[at, :E]) + bias[:, at]
                raised[:, at] = scores
                most = folded(scores, jnp.maximum)
                top = stats.get("top")
                stats["top"] = most if top is None else jnp.maximum(top, most)

        return go

    return [part(k) for k in range(0, kv.shape[0], 2 * CHUNK)]


def power_pass(raised, stats):
    def part(k):
        def go():
            if k == 0:
                stats["top"] = jnp.max(stats["top"], axis=1, keepdims=True)
            for at in (slice(k, k + CHUNK), slice(k + CHUNK, k + 2 * CHUNK)):
                shifted = raised[:, at] - stats["top"]
                power = jnp.exp2(shifted * (math.log2(math.e) / math.sqrt(E)))
                raised[:, at] = power
                more = folded(power, jnp.add)
                stats["sum"] = stats["sum"] + more if "sum" in stats else more

        return go

    return [part(k) for k in range(0, raised.shape[1], 2 * CHUNK)]


def output_pass(kv, raised, rounded, inverse, outputs, stats):
    def part(k):
        def go():
            if k == 0:
                whole = jnp.sum(stats["sum"], axis=1, keepdims=True)
                stats["inverse"] = 1.0 / whole
                inverse[...] = jnp.broadcast_to(stats["inverse"], inverse.shape)
            for at in (slice(k, k + CHUNK), slice(k + CHUNK, k + 2 * CHUNK)):
                probs = (raised[:, at] * stats["inverse"]).astype(BF16)
                rounded[:, at] = probs
                made = dot(probs, kv[at, E:])
                stats["out"] = stats["out"] + made if "out" in stats else made
            if k + 2 * CHUNK == kv.shape[0]:
                outputs(stats["out"].astype(BF16))

        return go

    return [part(k) for k in range(0, kv.shape[0], 2 * CHUNK)]


def forward_parts(q, kv, bias, raised, rounded, inverse, outputs):
    stats = {}
    return (
        scores_pass(q, kv, bias, raised, stats)
        + power_pass(raised, stats)
        + output_pass(kv, raised, rounded, inverse, outputs, stats)
    )


def backward(q, g, kv, raised, rounded, inverse, outputs, total):
    length = kv.shape[0]
    delta = jnp.sum(g.astype(F32) * outputs.astype(F32), axis=1, keepdims=True)
    scaled = inverse[:, :1] * (1.0 / math.sqrt(E))
    q_t = flipped(q).astype(BF16)
    g_t = flipped(g).astype(BF16)
    query_grad = jnp.zeros(q.shape, F32)
    for k in range(0, length, CHUNK):
        at = slice(k, k + CHUNK)
        dprobs = dot_last(g, kv[at, E:])
        dscores = ((raised[:, at] * scaled) * (dprobs - delta)).astype(BF16)
        query_grad = query_grad + dot(dscores, kv[at, :E])
        total[:E, at] = total[:E, at] + dot(q_t, dscores)
        total[E:, at] = total[E:, at] + dot(g_t, rounded[:, at])
    return query_grad.astype(BF16)


def middle_kernel(
    wq_in, wo_in, cot_in, state, decay, firsts, q1, g1, q0, kv,
    part, dkv, own_up, states, decays,
    bias, total, raised, rounded, inverse, outputs, q_grad, g0,
    wq1, wq0, wo0, residual, upstream, acc, land, local, send, recv,
):
    rows, depth = acc.shape
    length = kv.shape[0]
    share = depth // 8
    heads = q1.shape[1] // E
    s_rows, d_rows = state.shape[0], decay.shape[0]
    s_at, d_at = by_rows(states, s_rows), by_rows(decays, d_rows)
    me, here = head_index(), seq_index()
    copies = bring(
        (wq_in.at[1], wq1),
        (cot_in, residual),
        (state, s_at(here, 0, s_rows)),
        (decay, d_at(here, 0, d_rows)),
        (wo_in.at[0], wo0),
        (wq_in.at[0], wq0),
        sem=local,
    )
    fill_bias(bias, firsts, here * rows, rows, length)
    total[...] = jnp.zeros_like(total)

    def keep(cols):
        def put(value):
            outputs[:, cols] = value

        return put

    def back(h, g):
        cols = pl.ds(pl.multiple_of(h * E, E), E)
        return cols, lambda q: backward(
            q[:, cols], g[:, cols], kv, raised.at[h], rounded.at[h], inverse.at[h],
            outputs[:, cols], total,
        )

    def upper(h, _):
        cols, run = back(h, g1)
        for item in forward_parts(
            lambda: q1[:, cols], kv, bias, raised.at[h], rounded.at[h], inverse.at[h], keep(cols)
        ):
            item()
        q_grad[:, cols] = run(q1)
        return 0

    lax.fori_loop(0, heads, upper, 0)
    copies[0].wait()
    for k in range(0, depth, share):
        acc[:, k : k + share] = dot_last(q_grad[...], wq1[k : k + share]).astype(BF16)
    meet(seq_peers() + head_peers())
    for copy in copies[1:4]:
        copy.wait()
    wire = Wire(send, recv)
    for h in range(heads):
        cols = slice(h * E, (h + 1) * E)
        wire.work += forward_parts(
            lambda cols=cols: q0[:, cols],
            kv, bias, raised.at[h], rounded.at[h], inverse.at[h], keep(cols),
        )
    finish(
        together(
            head_run(wire, acc, land, residual, upstream),
            gather_seq(wire, s_at, s_rows),
            gather_seq(wire, d_at, d_rows),
        )
    )
    wire.idle(len(wire.work))
    copies[4].wait()
    g0[...] = dot_last(upstream[...], wo0[...]).astype(BF16)

    def lower(h, _):
        cols, run = back(h, g0)
        q_grad[:, cols] = run(q0)
        return 0

    lax.fori_loop(0, heads, lower, 0)
    dkv[...] = total[...].astype(BF16)
    copies[5].wait()
    for k in range(0, depth, share):
        part[:, k : k + share] = dot_last(q_grad[...], wq0[k : k + share]).astype(BF16)
    own_up[...] = by_columns(upstream, share)(me, 0, rows)[...]
    wire.drain()


def middle_stage(number, *operands):
    w_query, w_out, cot, state, decay = operands[:5]
    q1, kv = operands[6], operands[9]
    rows, depth = cot.shape
    wide, length = q1.shape[1], kv.shape[0]
    heads = wide // E
    shape = jax.ShapeDtypeStruct
    return pl.pallas_call(
        middle_kernel,
        out_shape=(
            shape((rows, depth), BF16),
            shape((2 * E, length), BF16),
            shape((rows, depth // 8), BF16),
            shape((16 * state.shape[0], E), BF16),
            shape((16 * decay.shape[0], 128), F32),
        ),
        in_specs=[ANY] * 5 + [pl.BlockSpec(memory_space=pltpu.SMEM)] + [VMEM] * 4,
        out_specs=(VMEM,) * 5,
        scratch_shapes=[
            pltpu.VMEM((rows, length), F32),
            pltpu.VMEM((2 * E, length), F32),
            pltpu.VMEM((heads, rows, length), F32),
            pltpu.VMEM((heads, rows, length), BF16),
            pltpu.VMEM((heads, rows, 128), F32),
            pltpu.VMEM((rows, wide), BF16),
            pltpu.VMEM((rows, wide), BF16),
            pltpu.VMEM((rows, wide), BF16),
            pltpu.VMEM((depth, wide), BF16),
            pltpu.VMEM((depth, wide), BF16),
            pltpu.VMEM((wide, depth), BF16),
            pltpu.VMEM((rows, depth), BF16),
            pltpu.VMEM((rows, depth), BF16),
            pltpu.VMEM((rows, depth), BF16),
            pltpu.VMEM((7 * rows, depth // 8), BF16),
            pltpu.SemaphoreType.DMA((6,)),
            *wires(90),
        ],
        compiler_params=pltpu.CompilerParams(
            collective_id=number, has_side_effects=True, vmem_limit_bytes=67043328
        ),
    )(*operands)


def local(
    mid,
    second_in,
    cotangent,
    w_key,
    w_value,
    w_query,
    w_out,
    w_ret_out,
    ret_query,
    ret_key,
    ret_value,
    gate,
    decay_exp,
    mask_start,
):
    kv, q1, g1, q0, mid_t, slices, first_state, state, decay, logs = open_stage(
        0, mid, second_in, cotangent, w_key, w_value, w_query, w_out, ret_key, ret_value, gate,
        decay_exp,
    )
    part, dkv, own_up, states, decays = middle_stage(
        1, w_query, w_out, cotangent, state, decay, mask_start, q1, g1, q0, kv
    )
    made = close_stage(
        2, part, dkv, slices, mid_t, w_ret_out, states, own_up, ret_query, ret_key, ret_value,
        logs, decays, first_state,
    )
    return hand_out(*made)


def solution(mesh):
    torus = Mesh(mesh.devices.reshape(2, 4, 2, 4, 2), ("xh", "y", "core", "z", "xl"))
    in_specs = (
        P(SEQ, None),
        P(SEQ, None),
        P(SEQ, None),
        P(None, HEAD),
        P(None, HEAD),
        P(None, None, HEAD),
        P(None, HEAD, None),
        P(HEAD, None),
        P(SEQ, HEAD),
        P(SEQ, HEAD),
        P(SEQ, HEAD),
        P(HEAD, SEQ),
        P(HEAD),
        P(SEQ),
    )
    out_specs = (
        P(SEQ, None),
        P(SEQ, HEAD),
        P(SEQ, HEAD),
        P(SEQ, HEAD),
        P(None, HEAD),
        P(None, HEAD),
    )
    return jax.shard_map(local, mesh=torus, in_specs=in_specs, out_specs=out_specs, check_vma=False)
```

```python
import functools
import math

import jax
import jax.numpy as jnp
from jax import lax
from jax.experimental import pallas as pl
from jax.experimental.pallas import tpu as pltpu
from jax.sharding import Mesh
from jax.sharding import PartitionSpec as P

E = 128
BLK = 128
RC = 128
SEQ = ("xh", "y", "core")
HEAD = ("z", "xl")

MESH = pl.DeviceIdType.MESH
BF16 = jnp.bfloat16
F32 = jnp.float32


class Wire:
    def __init__(self, send, recv):
        self.send, self.recv, self.sent, self.used = send, recv, [], 0
        self.work, self.pace = [], 1

    def idle(self, count):
        for item in self.work[:count]:
            item()
        self.work = self.work[count:]

    def put(self, src, dst, to):
        k = self.used
        self.used += 1
        copy = pltpu.make_async_remote_copy(
            src_ref=src,
            dst_ref=dst,
            send_sem=self.send.at[k],
            recv_sem=self.recv.at[k],
            device_id=to,
            device_id_type=MESH,
        )
        copy.start()
        self.sent.append(copy)
        return (k, to)

    def got(self, ticket, landed):
        self.idle(self.pace)
        k, to = ticket
        pltpu.make_async_remote_copy(
            src_ref=landed,
            dst_ref=landed,
            send_sem=self.send.at[k],
            recv_sem=self.recv.at[k],
            device_id=to,
            device_id_type=MESH,
        ).wait_recv()

    def drain(self):
        for copy in self.sent:
            copy.wait_send()
        self.sent = []


def greet(peers):
    barrier = pltpu.get_barrier_semaphore()
    for to in peers:
        pl.semaphore_signal(barrier, inc=1, device_id=to, device_id_type=MESH)


def answered(peers):
    pl.semaphore_wait(pltpu.get_barrier_semaphore(), len(peers))


def near(axis):
    at = lax.axis_index(axis)
    return at, lax.rem(at + 1, 4), lax.rem(at + 3, 4), lax.rem(at + 2, 4)


def seq_peers():
    y, yp, ym, y2 = near("y")
    return [
        {"xh": 1 - lax.axis_index("xh")},
        {"y": yp},
        {"y": ym},
        {"core": 1 - lax.axis_index("core")},
    ]


def head_peers():
    z, zp, zm, z2 = near("z")
    return [{"xl": 1 - lax.axis_index("xl")}, {"z": zp}, {"z": zm}]


def by_rows(ref, rows, parts=2):
    step = rows // parts

    def at(slot, first, count):
        return ref.at[pl.ds(pl.multiple_of(slot * rows + first, step), count)]

    return at


def by_columns(ref, width):
    def at(slot, first, count):
        return ref.at[pl.ds(first, count), pl.ds(pl.multiple_of(slot * width, 128), width)]

    return at


def add_to(total, part):
    total[...] = (total[...].astype(F32) + part[...].astype(F32)).astype(total.dtype)


def together(*runs):
    runs = list(runs)
    while runs:
        for run in list(runs):
            try:
                next(run)
            except StopIteration:
                runs.remove(run)
        yield


def finish(run):
    for _ in run:
        pass


def gather_seq(wire, at, rows):
    xh, c = lax.axis_index("xh"), lax.axis_index("core")
    y, yp, ym, y2 = near("y")
    xo, co = 1 - xh, 1 - c
    half = rows // 2
    whole, low, high = (0, rows), (0, half), (half, half)
    across, up, down, beside = {"xh": xo}, {"y": yp}, {"y": ym}, {"core": co}

    def slot(a, b, d):
        return a * 8 + b * 2 + d

    def pass_on(s, part, to):
        return wire.put(at(s, *part), at(s, *part), to)

    side = []
    own, far = slot(xh, y, c), slot(xo, y, c)
    t_x = pass_on(own, whole, across)
    ups, downs = [pass_on(own, whole, up)], [pass_on(own, whole, down)]
    side.append((pass_on(own, whole, beside), slot(xh, y, co)))
    yield
    wire.got(t_x, at(far, *whole))
    ups.append(pass_on(far, whole, up))
    downs.append(pass_on(far, whole, down))
    side.append((pass_on(far, whole, beside), slot(xo, y, co)))
    yield
    last = []
    for k, q in enumerate((xh, xo)):
        wire.got(ups[k], at(slot(q, ym, c), *whole))
        a = pass_on(slot(q, ym, c), low, up)
        side.append((pass_on(slot(q, ym, c), whole, beside), slot(q, ym, co)))
        wire.got(downs[k], at(slot(q, yp, c), *whole))
        b = pass_on(slot(q, yp, c), high, down)
        side.append((pass_on(slot(q, yp, c), whole, beside), slot(q, yp, co)))
        last.append((a, b))
        yield
    for k, q in enumerate((xh, xo)):
        wire.got(last[k][0], at(slot(q, y2, c), *low))
        wire.got(last[k][1], at(slot(q, y2, c), *high))
        side.append((pass_on(slot(q, y2, c), whole, beside), slot(q, y2, co)))
        yield
    for ticket, s in side:
        wire.got(ticket, at(s, *whole))


def ring_scatter(wire, at, slot, axis, first, count, land, before=None):
    r, rp, rm, r2 = near(axis)
    up, down = {axis: rp}, {axis: rm}
    half = count // 2
    wait = before or (lambda j: None)
    low, high = land.at[pl.ds(0, half)], land.at[pl.ds(half, half)]
    from_up, from_down = land.at[pl.ds(count, count)], land.at[pl.ds(2 * count, count)]
    wait(2)
    a = wire.put(at(slot(r2), first, half), low, up)
    b = wire.put(at(slot(r2), first + half, half), high, down)
    yield
    wait(1)
    wire.got(a, low)
    add_to(at(slot(rp), first, half), low)
    u = wire.put(at(slot(rp), first, count), from_down, up)
    wait(3)
    wire.got(b, high)
    add_to(at(slot(rm), first + half, half), high)
    d = wire.put(at(slot(rm), first, count), from_up, down)
    yield
    wait(0)
    wire.got(u, from_down)
    add_to(at(slot(r), first, count), from_down)
    wire.got(d, from_up)
    add_to(at(slot(r), first, count), from_up)


def scatter_seq(wire, at, rows, land):
    xh, c = lax.axis_index("xh"), lax.axis_index("core")
    y, yp, ym, y2 = near("y")
    xo, co = 1 - xh, 1 - c

    def slot(a, b, d):
        return a * 8 + b * 2 + d

    def block(k, count=1):
        return land.at[pl.ds(k * rows, count * rows)]

    places = {0: y, 1: yp, 2: y2, 3: ym}
    side = {}
    for n, q in enumerate((xo, xh)):
        for m, j in enumerate((2, 1, 3, 0)):
            dst = block(4 * n + m)
            side[n, j] = (wire.put(at(slot(q, places[j], co), 0, rows), dst, {"core": co}), dst)

    def before(n, q):
        def wait(j):
            ticket, dst = side[n, j]
            wire.got(ticket, dst)
            add_to(at(slot(q, places[j], c), 0, rows), dst)

        return wait

    def ring(n, q):
        return ring_scatter(
            wire, at, lambda j: slot(q, j, c), "y", 0, rows, block(8 + 3 * n, 3), before(n, q)
        )

    sent = []

    def far():
        yield from ring(0, xo)
        sent.append(wire.put(at(slot(xo, y, c), 0, rows), block(14), {"xh": xo}))

    yield from together(far(), ring(1, xh))
    wire.got(sent[0], block(14))
    return block(14)


def scatter_head(wire, at, rows, land):
    xl = lax.axis_index("xl")
    z, zp, zm, z2 = near("z")
    xo = 1 - xl
    half = rows // 2

    def slot(j, q):
        return j * 2 + q

    def block(k, count=1):
        return land.at[pl.ds(k * half, count * half)]

    places = {0: z, 1: zp, 2: z2, 3: zm}
    side = {}
    for m, j in enumerate((2, 1, 3, 0)):
        side[j] = (wire.put(at(slot(places[j], xo), 0, half), block(m), {"xl": xo}), block(m))

    def wait(j):
        ticket, dst = side[j]
        wire.got(ticket, dst)
        add_to(at(slot(places[j], xl), 0, half), dst)

    sent = []

    def far():
        yield from ring_scatter(
            wire, at, lambda j: slot(j, xo), "z", half, half, block(4, 3)
        )
        sent.append(wire.put(at(slot(z, xo), half, half), block(13), {"xl": xo}))

    yield from together(
        far(),
        ring_scatter(wire, at, lambda j: slot(j, xl), "z", half, half, block(7, 3)),
        ring_scatter(wire, at, lambda j: slot(j, xl), "z", 0, half, block(10, 3), wait),
    )
    wire.got(sent[0], block(13))
    add_to(at(slot(z, xl), half, half), block(13))


def gather_head(wire, at, rows):
    xl = lax.axis_index("xl")
    z, zp, zm, z2 = near("z")
    xo = 1 - xl
    half = rows // 2
    up, down, across = {"z": zp}, {"z": zm}, {"xl": xo}

    def slot(j, q):
        return j * 2 + q

    def pass_on(s, first, count, to):
        return wire.put(at(s, first, count), at(s, first, count), to)

    def ring(q, first, each=None):
        h = half // 2
        tell = each or (lambda j: None)
        a = pass_on(slot(z, q), first, half, up)
        b = pass_on(slot(z, q), first, half, down)
        tell(z)
        yield
        wire.got(a, at(slot(zm, q), first, half))
        c = pass_on(slot(zm, q), first, h, up)
        tell(zm)
        wire.got(b, at(slot(zp, q), first, half))
        d = pass_on(slot(zp, q), first + h, h, down)
        tell(zp)
        yield
        wire.got(c, at(slot(z2, q), first, h))
        wire.got(d, at(slot(z2, q), first + h, h))
        tell(z2)

    side = []

    def tell(j):
        side.append((pass_on(slot(j, xl), 0, half, across), slot(j, xo)))

    t_x = pass_on(slot(z, xl), half, half, across)

    def far():
        wire.got(t_x, at(slot(z, xo), half, half))
        yield from ring(xo, half)

    yield from together(ring(xl, 0, tell), ring(xl, half), far())
    for ticket, s in side:
        wire.got(ticket, at(s, 0, half))


ANY = pl.BlockSpec(memory_space=pl.ANY)
VMEM = pl.BlockSpec(memory_space=pltpu.VMEM)


def bring(*pairs, sem):
    copies = [pltpu.make_async_copy(s, d, sem.at[k]) for k, (s, d) in enumerate(pairs)]
    for copy in copies:
        copy.start()
    return copies


def seq_index():
    return lax.axis_index("xh") * 8 + lax.axis_index("y") * 2 + lax.axis_index("core")


def head_index():
    return lax.axis_index("z") * 2 + lax.axis_index("xl")


def total_into(out_at, acc_at, residual, rows, width):
    me = head_index()
    own = acc_at(me, 0, rows)
    kept = residual.at[pl.ds(0, rows), pl.ds(pl.multiple_of(me * width, 128), width)]
    out_at(me, 0, rows)[...] = (kept[...].astype(F32) + own[...].astype(F32)).astype(BF16)


def head_run(wire, acc, land, residual, out):
    rows, columns = acc.shape
    width = columns // 8
    yield from scatter_head(wire, by_columns(acc, width), rows, land)
    total_into(by_columns(out, width), by_columns(acc, width), residual, rows, width)
    yield from gather_head(wire, by_columns(out, width), rows)


def dot_last(a, b):
    return lax.dot_general(a, b, (((1,), (1,)), ((), ())), preferred_element_type=F32)


def dot(a, b):
    return jnp.dot(a, b, preferred_element_type=F32)


def folded(value, op):
    parts = [value[:, k : k + 128] for k in range(0, value.shape[1], 128)]
    while len(parts) > 1:
        parts = [op(a, b) for a, b in zip(parts[::2], parts[1::2])]
    return parts[0]


CHUNK = 512


def fill_bias(bias, firsts, position, rows, length):
    row = lax.broadcasted_iota(jnp.int32, (rows, CHUNK), 0)
    low = jnp.where(row < BLK, firsts[0], firsts[1])
    high = row + position
    for k in range(0, length, CHUNK):
        column = lax.broadcasted_iota(jnp.int32, (rows, CHUNK), 1) + k
        seen = (column >= low) & (column <= high)
        bias[:, k : k + CHUNK] = jnp.where(seen, 0.0, -jnp.inf)


def flipped(value):
    return value.astype(F32).T


def log_decays(logs):
    t = lax.broadcasted_iota(jnp.int32, (RC, RC), 0)
    s = lax.broadcasted_iota(jnp.int32, (RC, RC), 1)
    upto = jnp.where(t <= s, 1.0, 0.0)
    rows, columns = [], []
    for c in range(logs.shape[1] // RC):
        part = jnp.dot(
            logs[:, c * RC : (c + 1) * RC],
            upto,
            precision=lax.Precision.HIGHEST,
            preferred_element_type=F32,
        )
        rows.append(part)
        tall = jnp.concatenate((part, jnp.zeros((RC - part.shape[0], RC), F32)), axis=0)
        columns.append(tall.T)
    return rows, columns


def spread(peers):
    z, xl = lax.axis_index("z"), lax.axis_index("xl")
    places = []
    for k in range(1, 8):
        to = (lax.rem(z + k // 2, 4), lax.rem(xl + k, 2))
        came = (lax.rem(z + 4 - k // 2, 4), lax.rem(xl + k, 2))
        places.append((to, came))
    return places


def hand_out_kernel(*refs):
    ins, outs, held, (wide, sem_in, sem_out) = refs[:5], refs[5:11], refs[11:16], refs[16:]
    copies = bring(*zip(ins, held), sem=sem_in)
    sends = []
    for k in range(4):
        copies[k].wait()
        sends.append(pltpu.make_async_copy(held[k], outs[k], sem_out.at[k]))
        sends[-1].start()
    copies[4].wait()
    for k in range(2):
        wide[k] = held[4][:, k * E : (k + 1) * E].astype(F32)
        sends.append(pltpu.make_async_copy(wide.at[k], outs[4 + k], sem_out.at[4 + k]))
        sends[-1].start()
    for send in sends:
        send.wait()


def hand_out(*arrays):
    shape = jax.ShapeDtypeStruct
    depth = arrays[4].shape[0]
    return pl.pallas_call(
        hand_out_kernel,
        out_shape=tuple(shape(a.shape, a.dtype) for a in arrays[:4])
        + (shape((depth, E), F32), shape((depth, E), F32)),
        in_specs=[ANY] * 5,
        out_specs=(ANY,) * 6,
        scratch_shapes=[pltpu.VMEM(a.shape, a.dtype) for a in arrays]
        + [
            pltpu.VMEM((2, depth, E), F32),
            pltpu.SemaphoreType.DMA((5,)),
            pltpu.SemaphoreType.DMA((6,)),
        ],
    )(*arrays)


def scores_pass(q, kv, bias, raised, stats):
    def part(k):
        def go():
            for at in (slice(k, k + CHUNK), slice(k + CHUNK, k + 2 * CHUNK)):
                scores = dot_last(q(), kv[at, :E]) + bias[:, at]
                raised[:, at] = scores
                most = folded(scores, jnp.maximum)
                top = stats.get("top")
                stats["top"] = most if top is None else jnp.maximum(top, most)

        return go

    return [part(k) for k in range(0, kv.shape[0], 2 * CHUNK)]


def power_pass(raised, stats):
    def part(k):
        def go():
            if k == 0:
                stats["top"] = jnp.max(stats["top"], axis=1, keepdims=True)
            for at in (slice(k, k + CHUNK), slice(k + CHUNK, k + 2 * CHUNK)):
                shifted = raised[:, at] - stats["top"]
                power = jnp.exp2(shifted * (math.log2(math.e) / math.sqrt(E)))
                raised[:, at] = power
                more = folded(power, jnp.add)
                stats["sum"] = stats["sum"] + more if "sum" in stats else more

        return go

    return [part(k) for k in range(0, raised.shape[1], 2 * CHUNK)]


def output_pass(kv, raised, rounded, inverse, outputs, stats):
    def part(k):
        def go():
            if k == 0:
                whole = jnp.sum(stats["sum"], axis=1, keepdims=True)
                stats["inverse"] = 1.0 / whole
                inverse[...] = jnp.broadcast_to(stats["inverse"], inverse.shape)
            for at in (slice(k, k + CHUNK), slice(k + CHUNK, k + 2 * CHUNK)):
                probs = (raised[:, at] * stats["inverse"]).astype(BF16)
                rounded[:, at] = probs
                made = dot(probs, kv[at, E:])
                stats["out"] = stats["out"] + made if "out" in stats else made
            if k + 2 * CHUNK == kv.shape[0]:
                outputs(stats["out"].astype(BF16))

        return go

    return [part(k) for k in range(0, kv.shape[0], 2 * CHUNK)]


def forward_parts(q, kv, bias, raised, rounded, inverse, outputs):
    stats = {}
    return (
        scores_pass(q, kv, bias, raised, stats)
        + power_pass(raised, stats)
        + output_pass(kv, raised, rounded, inverse, outputs, stats)
    )


def backward(q, g, kv, raised, rounded, inverse, outputs, total):
    length = kv.shape[0]
    delta = jnp.sum(g.astype(F32) * outputs.astype(F32), axis=1, keepdims=True)
    scaled = inverse[:, :1] * (1.0 / math.sqrt(E))
    q_t = flipped(q).astype(BF16)
    g_t = flipped(g).astype(BF16)
    query_grad = jnp.zeros(q.shape, F32)
    for k in range(0, length, CHUNK):
        at = slice(k, k + CHUNK)
        dprobs = dot_last(g, kv[at, E:])
        dscores = ((raised[:, at] * scaled) * (dprobs - delta)).astype(BF16)
        query_grad = query_grad + dot(dscores, kv[at, :E])
        total[:E, at] = total[:E, at] + dot(q_t, dscores)
        total[E:, at] = total[E:, at] + dot(g_t, rounded[:, at])
    return query_grad.astype(BF16)


def opening(r, wire, copies, work):
    rows, depth = r.mid.shape

    def product(out, left, right, how, *numbers):
        def part(k):
            def go():
                if k == 0:
                    for number in numbers:
                        copies[number].wait()
                out[:, k : k + E] = how(left, right, k, E).astype(BF16)

            return go

        work.extend(part(k) for k in range(0, out.shape[1], E))

    def straight(left, right, at, count):
        return dot(left[...], right[:, at : at + count])

    def across(left, right, at, count):
        return dot_last(left[...], right[at : at + count])

    def rates():
        row = lax.broadcasted_iota(jnp.int32, (8, 128), 0)
        rate = jnp.zeros((8, 128), F32)
        for k in range(r.gate.shape[0]):
            power = jnp.full((8, 128), r.decay_exp[k], jnp.int32).astype(F32)
            rate = jnp.where(row == k, jnp.exp2(power * (-1.0 / 64.0)), rate)
        empty = jnp.zeros((8 - r.gate.shape[0], r.gate.shape[1]), F32)
        tall = jnp.concatenate((r.gate[...], empty), axis=0)
        r.logs[...] = -rate[:, :1] * tall

    def states():
        arow, acol = log_decays(r.logs[...])
        total = arow[0][:, RC - 1 :] + arow[1][:, RC - 1 :]
        here = seq_index()
        mine = r.decays.at[pl.ds(pl.multiple_of(here * 16, 16), 16)]
        mine[...] = jnp.concatenate(
            (jnp.broadcast_to(total, (8, 128)), jnp.zeros((8, 128), F32)), axis=0
        )
        count = r.ret_key.shape[1]
        for h in range(count // E):
            cols = slice(h * E, (h + 1) * E)
            made = []
            for c in range(2):
                span = slice(c * RC, (c + 1) * RC)
                shrink = jnp.exp(arow[c][h : h + 1, RC - 1 :] - acol[c][:, h : h + 1])
                scaled = (shrink * r.ret_key[span, cols].astype(F32)).astype(BF16)
                made.append(dot(flipped(scaled).astype(BF16), r.ret_value[span, cols]))
            r.first_state[cols] = made[0]
            last = jnp.exp(arow[1][h : h + 1, RC - 1 :])
            to = r.states.at[pl.ds(pl.multiple_of(here * count + h * E, E), E)]
            to[...] = (last * made[0] + made[1]).astype(BF16)

    def turn(k):
        def go():
            for j in range(k, k + 512, 128):
                r.mid_t[j : j + 128] = flipped(r.mid[:, j : j + 128]).astype(BF16)

        return go

    turns = [turn(k) for k in range(0, depth, 512)]
    work.extend([rates, states, turns[0]])
    product(r.q1, r.second, r.wq1, straight, 3, 4)
    product(r.g1, r.residual, r.wo, across, 5, 6)
    product(r.q0, r.mid, r.wq0, straight, 7)
    work.extend(turns[1:])


def exchange(r, wire, places):
    me, c = head_index(), lax.axis_index("core")
    share = r.wkv.shape[0] // 8
    tickets, side = [], []

    def mine(slot, half):
        return r.slices.at[slot, :, pl.ds(pl.multiple_of(half * E, E), E)]

    for (a, b), (ca, cb) in places:
        rows = pl.ds(pl.multiple_of((a * 2 + b) * share, share), share)
        src = r.wkv.at[rows, pl.ds(pl.multiple_of(c * E, E), E)]
        tickets.append((wire.put(src, mine(me, c), {"z": a, "xl": b}), ca * 2 + cb))
    yield
    for ticket, slot in tickets:
        wire.got(ticket, mine(slot, c))
        side.append((wire.put(mine(slot, c), mine(slot, c), {"core": 1 - c}), slot))
        yield
    for ticket, slot in side:
        wire.got(ticket, mine(slot, 1 - c))


def closing(r, wire, run_states):
    rows, depth = r.acc.shape
    share = depth // 8
    heads = r.ret_query.shape[1] // E
    me, here = head_index(), seq_index()
    kv_at = by_rows(r.kv_all, rows, 4)
    w_rows = depth // 16
    w_at = by_rows(r.w_sum, w_rows)
    s_rows = heads * E
    s_at = by_rows(r.grads, s_rows)
    arow, acol = log_decays(r.logs[...])
    t = lax.broadcasted_iota(jnp.int32, (RC, RC), 0)
    s = lax.broadcasted_iota(jnp.int32, (RC, RC), 1)
    pieces = [(h, c) for h in range(heads) for c in range(2)]
    where = {(h, c): (slice(c * RC, (c + 1) * RC), slice(h * E, (h + 1) * E)) for h, c in pieces}
    weights, second, turned, entering, after = {}, {}, {}, {}, {}
    rq, rk, rv = r.ret_query, r.ret_key, r.ret_value

    def end(h, c):
        return arow[c][h : h + 1, RC - 1 :]

    def prepare(h, c):
        a_t, a_s = acol[c][:, h : h + 1], arow[c][h : h + 1]
        lower = t >= s
        weights[h, c] = jnp.where(lower, jnp.exp(jnp.where(lower, a_t - a_s, 0.0)), 0.0)
        q, k = rq[where[h, c]], rk[where[h, c]]
        both = (weights[h, c] * dot_last(q, k)).astype(BF16)
        second[h, c] = flipped(both).astype(BF16)
        grown = (jnp.exp(a_t) * q.astype(F32)).astype(BF16)
        turned[h, c] = flipped(grown).astype(BF16)

    def arriving(h):
        cols = where[h, 0][1]
        now = jnp.zeros((E, E), F32)
        for k in range(15):
            mine = r.states[k * s_rows + h * E : k * s_rows + (h + 1) * E].astype(F32)
            new = jnp.exp(r.decays[k * 16 + h : k * 16 + h + 1]) * now + mine
            now = jnp.where(k < here, new, now)
        entering[h, 0] = now.astype(BF16)
        entering[h, 1] = (jnp.exp(end(h, 0)) * now + r.first_state[cols]).astype(BF16)

    def keys():
        at = by_columns(r.acc_k, rows)
        rest = yield from scatter_seq(wire, at, rows, r.land_k)
        own = at(here, 0, rows)
        total = own[...].astype(F32) + rest[...].astype(F32)
        kv_at(me, 0, rows)[...] = total.T.astype(BF16)

    run_keys = keys()
    next(run_keys)
    for k in range(0, depth, share):
        r.acc[:, k : k + share] = dot_last(r.q_grad[...], r.wq0[k : k + share]).astype(BF16)
    wire.work = [lambda h=h: arriving(h) for h in range(heads)]
    wire.work += [lambda h=h, c=c: prepare(h, c) for h, c in pieces]
    m_at = by_columns(r.acc, share)
    finish(together(scatter_head(wire, m_at, rows, r.land), run_keys))
    wire.idle(len(wire.work))
    own_kv = kv_at(me, 0, rows)
    gather_kv = gather_head(wire, kv_at, rows)
    next(gather_kv)
    r.wkv[...] = dot(r.mid_t[...], own_kv[...]).astype(BF16)

    def sums():
        at = by_rows(r.wkv, w_rows)
        rest = yield from scatter_seq(wire, at, w_rows, r.w_land)
        w_at(here, 0, w_rows)[...] = (
            at(here, 0, w_rows)[...].astype(F32) + rest[...].astype(F32)
        ).astype(BF16)
        yield
        yield from gather_seq(wire, w_at, w_rows)

    shared = sums()
    next(shared)

    def beside(run):
        for _ in run:
            next(shared, None)

    beside(gather_kv)
    total = m_at(me, 0, rows)[...].astype(F32)
    total = total + by_columns(r.upstream, share)(me, 0, rows)[...].astype(F32)
    for h in range(8):
        total = total + dot_last(kv_at(h, 0, rows)[...], r.slices[h])
    out_at = by_columns(r.mid, share)
    out_at(me, 0, rows)[...] = total.astype(BF16)
    beside(gather_head(wire, out_at, rows))
    shown = [pltpu.make_async_copy(r.mid, r.grad_mid, r.local.at[0])]
    shown[0].start()
    grad_o = dot_last(r.mid[...], r.wo[...]).astype(BF16)
    own_grad = {}
    for h, c in pieces:
        span, cols = where[h, c]
        own_grad[h, c] = dot(turned[h, c], grad_o[span, cols]) * (1.0 / E)
    for h in range(heads):
        made = own_grad[h, 0] + jnp.exp(end(h, 0)) * own_grad[h, 1]
        r.grads[pl.ds(pl.multiple_of(here * s_rows + h * E, E), E)] = made.astype(BF16)
    back = gather_seq(wire, s_at, s_rows)
    next(back)
    inner = {}

    def inside(h, c):
        span, cols = where[h, c]
        g, q, k, v = grad_o[span, cols], rq[span, cols], rk[span, cols], rv[span, cols]
        first = (weights[h, c] * dot_last(g, v)).astype(BF16)
        grow = jnp.exp(acol[c][:, h : h + 1])
        carried = grow * dot_last(g, entering[h, c])
        r.gq[span, cols] = ((dot(first, k) + carried) * (1.0 / E)).astype(BF16)
        inner[h, c] = (
            dot(flipped(first).astype(BF16), q) * (1.0 / E),
            dot(second[h, c], g) * (1.0 / E),
        )

    wire.work = [lambda h=h, c=c: inside(h, c) for h, c in pieces]
    beside(back)
    wire.idle(len(wire.work))
    for h in range(heads):
        now = jnp.zeros((E, E), F32)
        for k in range(15, 0, -1):
            mine = r.grads[k * s_rows + h * E : k * s_rows + (h + 1) * E].astype(F32)
            new = mine + jnp.exp(r.decays[k * 16 + h : k * 16 + h + 1]) * now
            now = jnp.where(k > here, new, now)
        after[h, 1] = now.astype(BF16)
        after[h, 0] = (own_grad[h, 1] + jnp.exp(end(h, 1)) * now).astype(BF16)
    for h, c in pieces:
        span, cols = where[h, c]
        shrink = jnp.exp(end(h, c) - acol[c][:, h : h + 1])
        r.gk[span, cols] = (
            inner[h, c][0] + shrink * dot_last(rv[span, cols], after[h, c])
        ).astype(BF16)
        r.gv[span, cols] = (inner[h, c][1] + shrink * dot(rk[span, cols], after[h, c])).astype(BF16)
    finish(shared)
    for copy in shown:
        copy.wait()
    wire.drain()


class Refs:
    def __init__(self, names, refs):
        for name, ref in zip(names, refs, strict=True):
            setattr(self, name, ref)


IN_NAMES = (
    "mid_in", "second_in", "cot_in", "wk_in", "wv_in", "wq_in", "wo_in", "wr_in",
    "ret_query", "ret_key", "ret_value", "gate", "decay_exp", "firsts",
)
OUT_NAMES = ("grad_mid", "gq", "gk", "gv", "w_sum")


def whole_kernel(names, *refs):
    r = Refs(names, refs)
    rows, depth = r.mid.shape
    length = r.kv.shape[0]
    share = depth // 8
    heads = r.q1.shape[1] // E
    here = seq_index()
    copies = bring(
        (r.mid_in, r.mid),
        (r.wk_in, r.wkv.at[:, pl.ds(0, E)]),
        (r.wv_in, r.wkv.at[:, pl.ds(E, E)]),
        sem=r.local,
    )
    places = spread(7)
    peers = seq_peers() + [{"z": a, "xl": b} for (a, b), _ in places]
    greet(peers)
    for copy in copies:
        copy.wait()
    copies += bring(
        (r.second_in, r.second),
        (r.wq_in.at[1], r.wq1),
        (r.cot_in, r.residual),
        (r.wo_in.at[1], r.wo),
        (r.wq_in.at[0], r.wq0),
        sem=r.local.at[pl.ds(3, 5)],
    )
    wire = Wire(r.send, r.recv)
    at = by_rows(r.kv, rows)
    at(here, 0, rows)[...] = dot(r.mid[...], r.wkv[...]).astype(BF16)
    answered(peers)
    opening(r, wire, copies, wire.work)
    wire.work.append(lambda: fill_bias(r.bias, r.firsts, here * rows, rows, length))

    def clear():
        r.total[...] = jnp.zeros_like(r.total)

    wire.work.append(clear)
    run_kv = gather_seq(wire, at, rows)
    next(run_kv)
    next(run_kv)
    run_slices = exchange(r, wire, places)
    next(run_slices)
    me = head_index()
    own = pltpu.make_async_copy(
        r.wkv.at[pl.ds(pl.multiple_of(me * share, share), share)], r.slices.at[me], r.local.at[8]
    )
    own.start()
    finish(run_kv)
    wire.idle(len(wire.work))
    s_rows = heads * E
    run_states = together(
        gather_seq(wire, by_rows(r.states, s_rows), s_rows),
        gather_seq(wire, by_rows(r.decays, 16), 16),
        run_slices,
    )
    next(run_states)
    late = bring((r.wo_in.at[0], r.wo), sem=r.local.at[pl.ds(9, 1)])

    def keep(cols):
        def put(value):
            r.outputs[:, cols] = value

        return put

    def ahead(h, q, cols):
        return forward_parts(
            lambda: q[:, cols],
            r.kv, r.bias, r.raised.at[h], r.rounded.at[h], r.inverse.at[h], keep(cols),
        )

    def wide(h):
        return pl.ds(pl.multiple_of(h * E, E), E)

    def upper(h, _):
        for item in ahead(h, r.q1, wide(h)):
            item()
        return 0

    def back(q, g):
        def go(h, _):
            cols = wide(h)
            r.q_grad[:, cols] = backward(
                q[:, cols], g[:, cols], r.kv, r.raised.at[h], r.rounded.at[h], r.inverse.at[h],
                r.outputs[:, cols], r.total,
            )
            return 0

        return go

    lax.fori_loop(0, heads, upper, 0)
    next(run_states)
    lax.fori_loop(0, heads, back(r.q1, r.g1), 0)
    next(run_states)
    for k in range(0, depth, share):
        r.acc[:, k : k + share] = dot_last(r.q_grad[...], r.wq1[k : k + share]).astype(BF16)
    for h in range(heads):
        wire.work += ahead(h, r.q0, slice(h * E, (h + 1) * E))
    finish(
        together(
            head_run(wire, r.acc, r.land, r.residual, r.upstream),
            run_states,
        )
    )
    wire.idle(len(wire.work))
    own.wait()
    late[0].wait()
    r.g0[...] = dot_last(r.upstream[...], r.wo[...]).astype(BF16)
    last = bring((r.wr_in, r.wo), sem=r.local.at[pl.ds(10, 1)])
    lax.fori_loop(0, heads, back(r.q0, r.g0), 0)
    r.acc_k[...] = r.total[...].astype(BF16)
    last[0].wait()
    wire.drain()
    closing(r, wire, run_states)


def whole(number, *operands):
    rows, depth = operands[0].shape
    wide = operands[8].shape[1]
    heads = wide // E
    length = 16 * rows
    shape = jax.ShapeDtypeStruct
    scratch = {
        "mid": pltpu.VMEM((rows, depth), BF16),
        "second": pltpu.VMEM((rows, depth), BF16),
        "residual": pltpu.VMEM((rows, depth), BF16),
        "wkv": pltpu.VMEM((depth, 2 * E), BF16),
        "wq1": pltpu.VMEM((depth, wide), BF16),
        "wq0": pltpu.VMEM((depth, wide), BF16),
        "wo": pltpu.VMEM((wide, depth), BF16),
        "mid_t": pltpu.VMEM((depth, rows), BF16),
        "slices": pltpu.VMEM((8, depth // 8, 2 * E), BF16),
        "kv": pltpu.VMEM((length, 2 * E), BF16),
        "q1": pltpu.VMEM((rows, wide), BF16),
        "g1": pltpu.VMEM((rows, wide), BF16),
        "q0": pltpu.VMEM((rows, wide), BF16),
        "outputs": pltpu.VMEM((rows, wide), BF16),
        "logs": pltpu.VMEM((8, rows), F32),
        "first_state": pltpu.VMEM((wide, E), F32),
        "states": pltpu.VMEM((16 * wide, E), BF16),
        "decays": pltpu.VMEM((256, 128), F32),
        "bias": pltpu.VMEM((rows, length), F32),
        "total": pltpu.VMEM((2 * E, length), F32),
        "raised": pltpu.VMEM((heads, rows, length), F32),
        "rounded": pltpu.VMEM((heads, rows, length), BF16),
        "inverse": pltpu.VMEM((heads, rows, 128), F32),
        "upstream": pltpu.VMEM((rows, depth), BF16),
        "land": pltpu.VMEM((7 * rows, depth // 8), BF16),
        "acc_k": pltpu.VMEM((2 * E, length), BF16),
        "land_k": pltpu.VMEM((15 * rows, rows), BF16),
        "kv_all": pltpu.VMEM((8 * rows, 2 * E), BF16),
        "w_land": pltpu.VMEM((15 * depth // 16, 2 * E), BF16),
        "grads": pltpu.VMEM((16 * wide, E), BF16),
        "local": pltpu.SemaphoreType.DMA((11,)),
        "send": pltpu.SemaphoreType.DMA((320,)),
        "recv": pltpu.SemaphoreType.DMA((320,)),
    }
    names = IN_NAMES + OUT_NAMES + tuple(scratch)
    shared = {"acc": "second", "g0": "g1", "q_grad": "gq"}

    def kernel(*refs):
        again = [refs[names.index(name)] for name in shared.values()]
        whole_kernel(names + tuple(shared), *refs, *again)

    smem = pl.BlockSpec(memory_space=pltpu.SMEM)
    return pl.pallas_call(
        kernel,
        out_shape=(
            shape((rows, depth), BF16),
            shape((rows, wide), BF16),
            shape((rows, wide), BF16),
            shape((rows, wide), BF16),
            shape((depth, 2 * E), BF16),
        ),
        in_specs=[ANY] * 8 + [VMEM] * 4 + [smem] * 2,
        out_specs=(ANY, VMEM, VMEM, VMEM, VMEM),
        scratch_shapes=list(scratch.values()),
        compiler_params=pltpu.CompilerParams(
            collective_id=number, has_side_effects=True, vmem_limit_bytes=67043328
        ),
    )(*operands)


def local(
    mid,
    second_in,
    cotangent,
    w_key,
    w_value,
    w_query,
    w_out,
    w_ret_out,
    ret_query,
    ret_key,
    ret_value,
    gate,
    decay_exp,
    mask_start,
):
    made = whole(
        0, mid, second_in, cotangent, w_key, w_value, w_query, w_out, w_ret_out,
        ret_query, ret_key, ret_value, gate, decay_exp, mask_start,
    )
    return hand_out(*made)


def solution(mesh):
    torus = Mesh(mesh.devices.reshape(2, 4, 2, 4, 2), ("xh", "y", "core", "z", "xl"))
    in_specs = (
        P(SEQ, None),
        P(SEQ, None),
        P(SEQ, None),
        P(None, HEAD),
        P(None, HEAD),
        P(None, None, HEAD),
        P(None, HEAD, None),
        P(HEAD, None),
        P(SEQ, HEAD),
        P(SEQ, HEAD),
        P(SEQ, HEAD),
        P(HEAD, SEQ),
        P(HEAD),
        P(SEQ),
    )
    out_specs = (
        P(SEQ, None),
        P(SEQ, HEAD),
        P(SEQ, HEAD),
        P(SEQ, HEAD),
        P(None, HEAD),
        P(None, HEAD),
    )
    return jax.shard_map(local, mesh=torus, in_specs=in_specs, out_specs=out_specs, check_vma=False)
```

```python
import functools
import math

import jax
import jax.numpy as jnp
from jax import lax
from jax.experimental import pallas as pl
from jax.experimental.pallas import tpu as pltpu
from jax.sharding import Mesh
from jax.sharding import PartitionSpec as P

E = 128
BLK = 128
RC = 128
SEQ = ("xh", "y", "core")
HEAD = ("z", "xl")

MESH = pl.DeviceIdType.MESH
BF16 = jnp.bfloat16
F32 = jnp.float32


class Wire:
    def __init__(self, send, recv):
        self.send, self.recv, self.sent, self.used = send, recv, [], 0
        self.work, self.pace, self.plan, self.waits = [], 1, {}, 0

    def planned(self, work, plan):
        self.work, self.pace, self.plan, self.waits = work, 0, plan, 0

    def idle(self, count):
        for item in self.work[:count]:
            item()
        self.work = self.work[count:]

    def put(self, src, dst, to):
        k = self.used
        self.used += 1
        copy = pltpu.make_async_remote_copy(
            src_ref=src,
            dst_ref=dst,
            send_sem=self.send.at[k],
            recv_sem=self.recv.at[k],
            device_id=to,
            device_id_type=MESH,
        )
        copy.start()
        self.sent.append(copy)
        return (k, to)

    def got(self, ticket, landed):
        self.idle(self.plan.get(self.waits, self.pace))
        self.waits += 1
        k, to = ticket
        pltpu.make_async_remote_copy(
            src_ref=landed,
            dst_ref=landed,
            send_sem=self.send.at[k],
            recv_sem=self.recv.at[k],
            device_id=to,
            device_id_type=MESH,
        ).wait_recv()

    def drain(self):
        for copy in self.sent:
            copy.wait_send()
        self.sent = []


def greet(peers):
    barrier = pltpu.get_barrier_semaphore()
    for to in peers:
        pl.semaphore_signal(barrier, inc=1, device_id=to, device_id_type=MESH)


def answered(peers):
    pl.semaphore_wait(pltpu.get_barrier_semaphore(), len(peers))


def near(axis):
    at = lax.axis_index(axis)
    return at, lax.rem(at + 1, 4), lax.rem(at + 3, 4), lax.rem(at + 2, 4)


def seq_peers():
    y, yp, ym, y2 = near("y")
    return [
        {"xh": 1 - lax.axis_index("xh")},
        {"y": yp},
        {"y": ym},
        {"core": 1 - lax.axis_index("core")},
    ]


def head_peers():
    z, zp, zm, z2 = near("z")
    return [{"xl": 1 - lax.axis_index("xl")}, {"z": zp}, {"z": zm}]


def by_rows(ref, rows, parts=2):
    step = rows // parts

    def at(slot, first, count):
        return ref.at[pl.ds(pl.multiple_of(slot * rows + first, step), count)]

    return at


def by_columns(ref, width):
    def at(slot, first, count):
        return ref.at[pl.ds(first, count), pl.ds(pl.multiple_of(slot * width, 128), width)]

    return at


def add_to(total, part):
    total[...] = (total[...].astype(F32) + part[...].astype(F32)).astype(total.dtype)


def together(*runs):
    runs = list(runs)
    while runs:
        for run in list(runs):
            try:
                next(run)
            except StopIteration:
                runs.remove(run)
        yield


def finish(run):
    for _ in run:
        pass


def gather_seq(wire, at, rows):
    xh, c = lax.axis_index("xh"), lax.axis_index("core")
    y, yp, ym, y2 = near("y")
    xo, co = 1 - xh, 1 - c
    half = rows // 2
    whole, low, high = (0, rows), (0, half), (half, half)
    across, up, down, beside = {"xh": xo}, {"y": yp}, {"y": ym}, {"core": co}

    def slot(a, b, d):
        return a * 8 + b * 2 + d

    def pass_on(s, part, to):
        return wire.put(at(s, *part), at(s, *part), to)

    side = []
    own, far = slot(xh, y, c), slot(xo, y, c)
    t_x = pass_on(own, whole, across)
    ups, downs = [pass_on(own, whole, up)], [pass_on(own, whole, down)]
    side.append((pass_on(own, whole, beside), slot(xh, y, co)))
    yield
    wire.got(t_x, at(far, *whole))
    ups.append(pass_on(far, whole, up))
    downs.append(pass_on(far, whole, down))
    side.append((pass_on(far, whole, beside), slot(xo, y, co)))
    yield
    last = []
    for k, q in enumerate((xh, xo)):
        wire.got(ups[k], at(slot(q, ym, c), *whole))
        a = pass_on(slot(q, ym, c), low, up)
        side.append((pass_on(slot(q, ym, c), whole, beside), slot(q, ym, co)))
        wire.got(downs[k], at(slot(q, yp, c), *whole))
        b = pass_on(slot(q, yp, c), high, down)
        side.append((pass_on(slot(q, yp, c), whole, beside), slot(q, yp, co)))
        last.append((a, b))
        yield
    for k, q in enumerate((xh, xo)):
        wire.got(last[k][0], at(slot(q, y2, c), *low))
        wire.got(last[k][1], at(slot(q, y2, c), *high))
        side.append((pass_on(slot(q, y2, c), whole, beside), slot(q, y2, co)))
        yield
    for ticket, s in side:
        wire.got(ticket, at(s, *whole))


def ring_scatter(wire, at, slot, axis, first, count, land, before=None):
    r, rp, rm, r2 = near(axis)
    up, down = {axis: rp}, {axis: rm}
    half = count // 2
    wait = before or (lambda j: None)
    low, high = land.at[pl.ds(0, half)], land.at[pl.ds(half, half)]
    from_up, from_down = land.at[pl.ds(count, count)], land.at[pl.ds(2 * count, count)]
    wait(2)
    a = wire.put(at(slot(r2), first, half), low, up)
    b = wire.put(at(slot(r2), first + half, half), high, down)
    yield
    wait(1)
    wire.got(a, low)
    add_to(at(slot(rp), first, half), low)
    u = wire.put(at(slot(rp), first, count), from_down, up)
    wait(3)
    wire.got(b, high)
    add_to(at(slot(rm), first + half, half), high)
    d = wire.put(at(slot(rm), first, count), from_up, down)
    yield
    wait(0)
    wire.got(u, from_down)
    add_to(at(slot(r), first, count), from_down)
    wire.got(d, from_up)
    add_to(at(slot(r), first, count), from_up)


def scatter_seq(wire, at, rows, land):
    xh, c = lax.axis_index("xh"), lax.axis_index("core")
    y, yp, ym, y2 = near("y")
    xo, co = 1 - xh, 1 - c

    def slot(a, b, d):
        return a * 8 + b * 2 + d

    def block(k, count=1):
        return land.at[pl.ds(k * rows, count * rows)]

    places = {0: y, 1: yp, 2: y2, 3: ym}
    side = {}
    for n, q in enumerate((xo, xh)):
        for m, j in enumerate((2, 1, 3, 0)):
            dst = block(4 * n + m)
            side[n, j] = (wire.put(at(slot(q, places[j], co), 0, rows), dst, {"core": co}), dst)

    yield

    def before(n, q):
        def wait(j):
            ticket, dst = side[n, j]
            wire.got(ticket, dst)
            add_to(at(slot(q, places[j], c), 0, rows), dst)

        return wait

    def ring(n, q):
        return ring_scatter(
            wire, at, lambda j: slot(q, j, c), "y", 0, rows, block(8 + 3 * n, 3), before(n, q)
        )

    sent = []

    def far():
        yield from ring(0, xo)
        sent.append(wire.put(at(slot(xo, y, c), 0, rows), block(14), {"xh": xo}))

    yield from together(far(), ring(1, xh))
    wire.got(sent[0], block(14))
    return block(14)


def scatter_head(wire, at, rows, land):
    xl = lax.axis_index("xl")
    z, zp, zm, z2 = near("z")
    xo = 1 - xl
    cut = rows * 3 // 8
    left = rows - cut

    def slot(j, q):
        return j * 2 + q

    def block(k, count=1):
        return land.at[pl.ds(k * cut, count * cut)]

    def lower(k, count=1):
        return land.at[pl.ds(7 * cut + k * left, count * left)]

    places = {0: z, 1: zp, 2: z2, 3: zm}
    side = {}
    for m, j in enumerate((2, 1, 3, 0)):
        side[j] = (wire.put(at(slot(places[j], xo), 0, cut), block(m), {"xl": xo}), block(m))

    def wait(j):
        ticket, dst = side[j]
        wire.got(ticket, dst)
        add_to(at(slot(places[j], xl), 0, cut), dst)

    sent = []

    def far():
        yield from ring_scatter(
            wire, at, lambda j: slot(j, xo), "z", cut, left, lower(0, 3)
        )
        sent.append(wire.put(at(slot(z, xo), cut, left), lower(6), {"xl": xo}))

    yield from together(
        far(),
        ring_scatter(wire, at, lambda j: slot(j, xl), "z", cut, left, lower(3, 3)),
        ring_scatter(wire, at, lambda j: slot(j, xl), "z", 0, cut, block(4, 3), wait),
    )
    wire.got(sent[0], lower(6))
    add_to(at(slot(z, xl), cut, left), lower(6))


def gather_head(wire, at, rows):
    xl = lax.axis_index("xl")
    z, zp, zm, z2 = near("z")
    xo = 1 - xl
    cut = rows * 3 // 8
    left = rows - cut
    up, down, across = {"z": zp}, {"z": zm}, {"xl": xo}

    def slot(j, q):
        return j * 2 + q

    def pass_on(s, first, count, to):
        return wire.put(at(s, first, count), at(s, first, count), to)

    def ring(q, first, half, each=None):
        h = half // 2
        tell = each or (lambda j: None)
        a = pass_on(slot(z, q), first, half, up)
        b = pass_on(slot(z, q), first, half, down)
        tell(z)
        yield
        wire.got(a, at(slot(zm, q), first, half))
        c = pass_on(slot(zm, q), first, h, up)
        tell(zm)
        wire.got(b, at(slot(zp, q), first, half))
        d = pass_on(slot(zp, q), first + h, h, down)
        tell(zp)
        yield
        wire.got(c, at(slot(z2, q), first, h))
        wire.got(d, at(slot(z2, q), first + h, h))
        tell(z2)

    side = []

    def tell(j):
        side.append((pass_on(slot(j, xl), 0, cut, across), slot(j, xo)))

    t_x = pass_on(slot(z, xl), cut, left, across)

    def far():
        wire.got(t_x, at(slot(z, xo), cut, left))
        yield from ring(xo, cut, left)

    yield from together(ring(xl, 0, cut, tell), ring(xl, cut, left), far())
    for ticket, s in side:
        wire.got(ticket, at(s, 0, cut))


ANY = pl.BlockSpec(memory_space=pl.ANY)
VMEM = pl.BlockSpec(memory_space=pltpu.VMEM)


def bring(*pairs, sem):
    copies = [pltpu.make_async_copy(s, d, sem.at[k]) for k, (s, d) in enumerate(pairs)]
    for copy in copies:
        copy.start()
    return copies


def seq_index():
    return lax.axis_index("xh") * 8 + lax.axis_index("y") * 2 + lax.axis_index("core")


def head_index():
    return lax.axis_index("z") * 2 + lax.axis_index("xl")


def total_into(out_at, acc_at, residual, rows, width):
    me = head_index()
    own = acc_at(me, 0, rows)
    kept = residual.at[pl.ds(0, rows), pl.ds(pl.multiple_of(me * width, 128), width)]
    out_at(me, 0, rows)[...] = (kept[...].astype(F32) + own[...].astype(F32)).astype(BF16)


def head_run(wire, acc, land, residual, out):
    rows, columns = acc.shape
    width = columns // 8
    yield from scatter_head(wire, by_columns(acc, width), rows, land)
    total_into(by_columns(out, width), by_columns(acc, width), residual, rows, width)
    yield from gather_head(wire, by_columns(out, width), rows)


def dot_last(a, b):
    return lax.dot_general(a, b, (((1,), (1,)), ((), ())), preferred_element_type=F32)


def dot(a, b):
    return jnp.dot(a, b, preferred_element_type=F32)


def folded(value, op):
    parts = [value[:, k : k + 128] for k in range(0, value.shape[1], 128)]
    while len(parts) > 1:
        parts = [op(a, b) for a, b in zip(parts[::2], parts[1::2])]
    return parts[0]


CHUNK = 512


def fill_bias(bias, firsts, position, rows, length):
    row = lax.broadcasted_iota(jnp.int32, (rows, CHUNK), 0)
    low = jnp.where(row < BLK, firsts[0], firsts[1])
    high = row + position
    for k in range(0, length, CHUNK):
        column = lax.broadcasted_iota(jnp.int32, (rows, CHUNK), 1) + k
        seen = (column >= low) & (column <= high)
        bias[:, k : k + CHUNK] = jnp.where(seen, 0.0, -jnp.inf)


def flipped(value):
    return value.astype(F32).T


def log_decays(logs):
    t = lax.broadcasted_iota(jnp.int32, (RC, RC), 0)
    s = lax.broadcasted_iota(jnp.int32, (RC, RC), 1)
    upto = jnp.where(t <= s, 1.0, 0.0)
    rows, columns = [], []
    for c in range(logs.shape[1] // RC):
        part = jnp.dot(
            logs[:, c * RC : (c + 1) * RC],
            upto,
            precision=lax.Precision.HIGHEST,
            preferred_element_type=F32,
        )
        rows.append(part)
        tall = jnp.concatenate((part, jnp.zeros((RC - part.shape[0], RC), F32)), axis=0)
        columns.append(tall.T)
    return rows, columns


def spread(peers):
    z, xl = lax.axis_index("z"), lax.axis_index("xl")
    places = []
    for k in range(1, 8):
        to = (lax.rem(z + k // 2, 4), lax.rem(xl + k, 2))
        came = (lax.rem(z + 4 - k // 2, 4), lax.rem(xl + k, 2))
        places.append((to, came))
    return places


def hand_out_kernel(*refs):
    ins, outs, held, (wide, sem_in, sem_out) = refs[:5], refs[5:11], refs[11:16], refs[16:]
    copies = bring(*zip(ins, held), sem=sem_in)
    sends = []
    for k in range(4):
        copies[k].wait()
        sends.append(pltpu.make_async_copy(held[k], outs[k], sem_out.at[k]))
        sends[-1].start()
    copies[4].wait()
    for k in range(2):
        wide[k] = held[4][:, k * E : (k + 1) * E].astype(F32)
        sends.append(pltpu.make_async_copy(wide.at[k], outs[4 + k], sem_out.at[4 + k]))
        sends[-1].start()
    for send in sends:
        send.wait()


def hand_out(*arrays):
    shape = jax.ShapeDtypeStruct
    depth = arrays[4].shape[0]
    return pl.pallas_call(
        hand_out_kernel,
        out_shape=tuple(shape(a.shape, a.dtype) for a in arrays[:4])
        + (shape((depth, E), F32), shape((depth, E), F32)),
        in_specs=[ANY] * 5,
        out_specs=(ANY,) * 6,
        scratch_shapes=[pltpu.VMEM(a.shape, a.dtype) for a in arrays]
        + [
            pltpu.VMEM((2, depth, E), F32),
            pltpu.SemaphoreType.DMA((5,)),
            pltpu.SemaphoreType.DMA((6,)),
        ],
    )(*arrays)


def scores_pass(q, kv, bias, raised, stats):
    def part(k):
        def go():
            for at in (slice(k, k + CHUNK), slice(k + CHUNK, k + 2 * CHUNK)):
                scores = dot_last(q(), kv[at, :E]) + bias[:, at]
                raised[:, at] = scores
                most = folded(scores, jnp.maximum)
                top = stats.get("top")
                stats["top"] = most if top is None else jnp.maximum(top, most)

        return go

    return [part(k) for k in range(0, kv.shape[0], 2 * CHUNK)]


def power_pass(raised, stats):
    def part(k):
        def go():
            if k == 0:
                stats["top"] = jnp.max(stats["top"], axis=1, keepdims=True)
            for at in (slice(k, k + CHUNK), slice(k + CHUNK, k + 2 * CHUNK)):
                shifted = raised[:, at] - stats["top"]
                power = jnp.exp2(shifted * (math.log2(math.e) / math.sqrt(E)))
                raised[:, at] = power
                more = folded(power, jnp.add)
                stats["sum"] = stats["sum"] + more if "sum" in stats else more

        return go

    return [part(k) for k in range(0, raised.shape[1], 2 * CHUNK)]


def output_pass(kv, raised, rounded, inverse, outputs, stats):
    def part(k):
        def go():
            if k == 0:
                whole = jnp.sum(stats["sum"], axis=1, keepdims=True)
                stats["inverse"] = 1.0 / whole
                inverse[...] = jnp.broadcast_to(stats["inverse"], inverse.shape)
            for at in (slice(k, k + CHUNK), slice(k + CHUNK, k + 2 * CHUNK)):
                probs = (raised[:, at] * stats["inverse"]).astype(BF16)
                rounded[:, at] = probs
                made = dot(probs, kv[at, E:])
                stats["out"] = stats["out"] + made if "out" in stats else made
            if k + 2 * CHUNK == kv.shape[0]:
                outputs(stats["out"].astype(BF16))

        return go

    return [part(k) for k in range(0, kv.shape[0], 2 * CHUNK)]


def forward_parts(q, kv, bias, raised, rounded, inverse, outputs):
    stats = {}
    return (
        scores_pass(q, kv, bias, raised, stats)
        + power_pass(raised, stats)
        + output_pass(kv, raised, rounded, inverse, outputs, stats)
    )


def backward(q, g, kv, raised, rounded, inverse, outputs, total):
    length = kv.shape[0]
    delta = jnp.sum(g.astype(F32) * outputs.astype(F32), axis=1, keepdims=True)
    scaled = inverse[:, :1] * (1.0 / math.sqrt(E))
    q_t = flipped(q).astype(BF16)
    g_t = flipped(g).astype(BF16)
    query_grad = jnp.zeros(q.shape, F32)
    for k in range(0, length, CHUNK):
        at = slice(k, k + CHUNK)
        dprobs = dot_last(g, kv[at, E:])
        dscores = ((raised[:, at] * scaled) * (dprobs - delta)).astype(BF16)
        query_grad = query_grad + dot(dscores, kv[at, :E])
        total[:E, at] = total[:E, at] + dot(q_t, dscores)
        total[E:, at] = total[E:, at] + dot(g_t, rounded[:, at])
    return query_grad.astype(BF16)


WIRES = 120


def opening(r, wire, copies, rest, work):
    rows, depth = r.mid.shape

    def product(out, left, right, how, *numbers):
        def part(k):
            def go():
                if k == 0:
                    for number in numbers:
                        copies[number].wait()
                out[:, k : k + E] = how(left, right, k, E).astype(BF16)

            return go

        work.extend(part(k) for k in range(0, out.shape[1], E))

    def straight(left, right, at, count):
        return dot(left[...], right[:, at : at + count])

    def across(left, right, at, count):
        return dot_last(left[...], right[at : at + count])

    def rates():
        row = lax.broadcasted_iota(jnp.int32, (8, 128), 0)
        rate = jnp.zeros((8, 128), F32)
        for k in range(r.gate.shape[0]):
            power = jnp.full((8, 128), r.decay_exp[k], jnp.int32).astype(F32)
            rate = jnp.where(row == k, jnp.exp2(power * (-1.0 / 64.0)), rate)
        empty = jnp.zeros((8 - r.gate.shape[0], r.gate.shape[1]), F32)
        tall = jnp.concatenate((r.gate[...], empty), axis=0)
        r.logs[...] = -rate[:, :1] * tall

    def states():
        for copy in rest:
            copy.wait()
        arow, acol = log_decays(r.logs[...])
        total = arow[0][:, RC - 1 :] + arow[1][:, RC - 1 :]
        here = seq_index()
        mine = r.decays.at[pl.ds(pl.multiple_of(here * 16, 16), 16)]
        mine[...] = jnp.concatenate(
            (jnp.broadcast_to(total, (8, 128)), jnp.zeros((8, 128), F32)), axis=0
        )
        count = r.ret_key.shape[1]
        for h in range(count // E):
            cols = slice(h * E, (h + 1) * E)
            made = []
            for c in range(2):
                span = slice(c * RC, (c + 1) * RC)
                shrink = jnp.exp(arow[c][h : h + 1, RC - 1 :] - acol[c][:, h : h + 1])
                scaled = (shrink * r.ret_key[span, cols].astype(F32)).astype(BF16)
                made.append(dot(flipped(scaled).astype(BF16), r.ret_value[span, cols]))
            r.first_state[cols] = made[0]
            last = jnp.exp(arow[1][h : h + 1, RC - 1 :])
            to = r.states.at[pl.ds(pl.multiple_of(here * count + h * E, E), E)]
            to[...] = (last * made[0] + made[1]).astype(BF16)

    def turn(k):
        def go():
            for j in range(k, k + 512, 128):
                r.mid_t[j : j + 128] = flipped(r.mid[:, j : j + 128]).astype(BF16)

        return go

    turns = [turn(k) for k in range(0, depth, 512)]
    work.extend([rates, states, turns[0]])
    product(r.q1, r.second, r.wq1, straight, 3, 4)
    product(r.g1, r.residual, r.wo, across, 5, 6)
    product(r.q0, r.mid, r.wq0, straight, 7)
    work.extend(turns[1:])


def exchange(r, wire, places):
    me, c = head_index(), lax.axis_index("core")
    share = r.wkv.shape[0] // 8
    tickets, side = [], []

    def mine(slot, half):
        return r.slices.at[slot, :, pl.ds(pl.multiple_of(half * E, E), E)]

    for (a, b), (ca, cb) in places:
        rows = pl.ds(pl.multiple_of((a * 2 + b) * share, share), share)
        src = r.wkv.at[rows, pl.ds(pl.multiple_of(c * E, E), E)]
        tickets.append((wire.put(src, mine(me, c), {"z": a, "xl": b}), ca * 2 + cb))
    yield
    yield
    for ticket, slot in tickets:
        wire.got(ticket, mine(slot, c))
        side.append((wire.put(mine(slot, c), mine(slot, c), {"core": 1 - c}), slot))
    yield
    yield
    yield
    yield
    yield
    for ticket, slot in side:
        wire.got(ticket, mine(slot, 1 - c))


def closing(r, wire):
    rows, depth = r.acc.shape
    share = depth // 8
    heads = r.ret_query.shape[1] // E
    me, here = head_index(), seq_index()
    kv_at = by_rows(r.kv_all, rows, 16)
    w_rows = depth // 16
    w_at = by_rows(r.w_sum, w_rows)
    s_rows = heads * E
    c_half = s_rows // 2
    arow, acol = log_decays(r.logs[...])
    t = lax.broadcasted_iota(jnp.int32, (RC, RC), 0)
    s = lax.broadcasted_iota(jnp.int32, (RC, RC), 1)
    pieces = [(h, c) for h in range(heads) for c in range(2)]
    where = {(h, c): (slice(c * RC, (c + 1) * RC), slice(h * E, (h + 1) * E)) for h, c in pieces}
    weights, second, turned, entering, after = {}, {}, {}, {}, {}
    rq, rk, rv = r.ret_query, r.ret_key, r.ret_value

    def end(h, c):
        return arow[c][h : h + 1, RC - 1 :]

    def prepare(h, c):
        a_t, a_s = acol[c][:, h : h + 1], arow[c][h : h + 1]
        lower = t >= s
        weights[h, c] = jnp.where(lower, jnp.exp(jnp.where(lower, a_t - a_s, 0.0)), 0.0)
        q, k = rq[where[h, c]], rk[where[h, c]]
        both = (weights[h, c] * dot_last(q, k)).astype(BF16)
        second[h, c] = flipped(both).astype(BF16)
        grown = (jnp.exp(a_t) * q.astype(F32)).astype(BF16)
        turned[h, c] = flipped(grown).astype(BF16)

    def arriving(h):
        cols = where[h, 0][1]
        now = jnp.zeros((E, E), F32)
        for k in range(15):
            mine = r.states[k * s_rows + h * E : k * s_rows + (h + 1) * E].astype(F32)
            new = jnp.exp(r.decays[k * 16 + h : k * 16 + h + 1]) * now + mine
            now = jnp.where(k < here, new, now)
        entering[h, 0] = now.astype(BF16)
        entering[h, 1] = (jnp.exp(end(h, 0)) * now + r.first_state[cols]).astype(BF16)

    def keys():
        at = by_columns(r.acc_k, rows)
        rest = yield from scatter_seq(wire, at, rows, r.land_k)
        own = at(here, 0, rows)
        total = own[...].astype(F32) + rest[...].astype(F32)
        kv_at(me, 0, rows)[...] = total.T.astype(BF16)

    run_keys = keys()
    next(run_keys)
    for k in range(0, depth, share):
        r.acc[:, k : k + share] = dot_last(r.q_grad[...], r.wq0[k : k + share]).astype(BF16)
    work = [lambda h=h: arriving(h) for h in range(heads)]
    work += [lambda h=h, c=c: prepare(h, c) for h, c in pieces]
    wire.planned(work, {2: 9})
    m_at = by_columns(r.acc, share)
    finish(together(run_keys, scatter_head(wire, m_at, rows, r.land)))
    wire.idle(len(wire.work))
    own_kv = kv_at(me, 0, rows)
    gather_kv = gather_head(wire, kv_at, rows)
    next(gather_kv)
    r.wkv[...] = dot(r.mid_t[...], own_kv[...]).astype(BF16)

    def sums():
        at = by_rows(r.wkv, w_rows)
        rest = yield from scatter_seq(wire, at, w_rows, r.w_land)
        w_at(here, 0, w_rows)[...] = (
            at(here, 0, w_rows)[...].astype(F32) + rest[...].astype(F32)
        ).astype(BF16)
        yield from gather_seq(wire, w_at, w_rows)

    shared = sums()
    next(shared)
    next(shared)

    def beside(run):
        for _ in run:
            next(shared, None)

    beside(gather_kv)
    total = m_at(me, 0, rows)[...].astype(F32)
    total = total + by_columns(r.upstream, share)(me, 0, rows)[...].astype(F32)
    for h in range(8):
        total = total + dot_last(kv_at(h, 0, rows)[...], r.slices[h])
    out_at = by_columns(r.mid, share)
    out_at(me, 0, rows)[...] = total.astype(BF16)
    beside(gather_head(wire, out_at, rows))
    shown = [pltpu.make_async_copy(r.mid, r.grad_mid, r.local.at[0])]
    shown[0].start()
    grad_o = dot_last(r.mid[...], r.wo[...]).astype(BF16)
    own_grad = {}
    for h, c in pieces:
        span, cols = where[h, c]
        own_grad[h, c] = dot(turned[h, c], grad_o[span, cols]) * (1.0 / E)
    for h in range(heads):
        made = own_grad[h, 0] + jnp.exp(end(h, 0)) * own_grad[h, 1]
        r.own_state[h * E : (h + 1) * E] = made.astype(BF16)
    core = lax.axis_index("core")
    chip = here - core
    ticket = wire.put(r.own_state, r.side_state, {"core": 1 - core})
    inner = {}

    def inside(h, c):
        span, cols = where[h, c]
        g, q, k, v = grad_o[span, cols], rq[span, cols], rk[span, cols], rv[span, cols]
        first = (weights[h, c] * dot_last(g, v)).astype(BF16)
        grow = jnp.exp(acol[c][:, h : h + 1])
        carried = grow * dot_last(g, entering[h, c])
        r.gq[span, cols] = ((dot(first, k) + carried) * (1.0 / E)).astype(BF16)
        inner[h, c] = (
            dot(flipped(first).astype(BF16), q) * (1.0 / E),
            dot(second[h, c], g) * (1.0 / E),
        )

    wire.planned([lambda h=h, c=c: inside(h, c) for h, c in pieces], {0: 2, 1: 4})
    wire.got(ticket, r.side_state)
    for h in range(heads):
        cols = slice(h * E, (h + 1) * E)
        mine, other = r.own_state[cols].astype(F32), r.side_state[cols].astype(F32)
        lead = r.decays[pl.ds(chip * 16 + h, 1)]
        made = jnp.where(core == 0, mine, other) + jnp.exp(lead) * jnp.where(core == 0, other, mine)
        r.chip_state[cols] = made.astype(BF16)
    s_at = by_rows(r.grads, c_half)
    s_at(here, 0, c_half)[...] = r.chip_state[pl.ds(pl.multiple_of(core * c_half, c_half), c_half)]
    beside(gather_seq(wire, s_at, c_half))
    wire.idle(len(wire.work))
    for h in range(heads):
        now = jnp.zeros((E, E), F32)
        for k in range(7, 0, -1):
            mine = r.grads[k * s_rows + h * E : k * s_rows + (h + 1) * E].astype(F32)
            both = r.decays[k * 32 + h : k * 32 + h + 1] + r.decays[k * 32 + 16 + h : k * 32 + 17 + h]
            new = mine + jnp.exp(both) * now
            now = jnp.where(2 * k > chip, new, now)
        beyond = r.decays[pl.ds((chip + 1) * 16 + h, 1)]
        new = r.side_state[h * E : (h + 1) * E].astype(F32) + jnp.exp(beyond) * now
        now = jnp.where(core == 0, new, now)
        after[h, 1] = now.astype(BF16)
        after[h, 0] = (own_grad[h, 1] + jnp.exp(end(h, 1)) * now).astype(BF16)
    for h, c in pieces:
        span, cols = where[h, c]
        shrink = jnp.exp(end(h, c) - acol[c][:, h : h + 1])
        r.gk[span, cols] = (
            inner[h, c][0] + shrink * dot_last(rv[span, cols], after[h, c])
        ).astype(BF16)
        r.gv[span, cols] = (inner[h, c][1] + shrink * dot(rk[span, cols], after[h, c])).astype(BF16)
    finish(shared)
    for copy in shown:
        copy.wait()
    wire.drain()


class Refs:
    def __init__(self, names, refs):
        for name, ref in zip(names, refs, strict=True):
            setattr(self, name, ref)


IN_NAMES = (
    "mid_in", "second_in", "cot_in", "wk_in", "wv_in", "wq_in", "wo_in", "wr_in",
    "rq_in", "rk_in", "rv_in", "gate", "decay_exp", "firsts",
)
OUT_NAMES = ("grad_mid", "gq", "gk", "gv", "w_sum")


def whole_kernel(names, *refs):
    r = Refs(names, refs)
    rows, depth = r.mid.shape
    length = r.kv.shape[0]
    share = depth // 8
    heads = r.q1.shape[1] // E
    here = seq_index()
    copies = bring(
        (r.mid_in, r.mid),
        (r.wk_in, r.wkv.at[:, pl.ds(0, E)]),
        (r.wv_in, r.wkv.at[:, pl.ds(E, E)]),
        sem=r.local,
    )
    places = spread(7)
    peers = seq_peers() + [{"z": a, "xl": b} for (a, b), _ in places]
    greet(peers)
    for copy in copies:
        copy.wait()
    copies += bring(
        (r.second_in, r.second),
        (r.wq_in.at[1], r.wq1),
        (r.cot_in, r.residual),
        (r.wo_in.at[1], r.wo),
        (r.wq_in.at[0], r.wq0),
        sem=r.local.at[pl.ds(3, 5)],
    )
    rest = bring(
        (r.rk_in, r.ret_key),
        (r.rv_in, r.ret_value),
        (r.rq_in, r.ret_query),
        sem=r.local.at[pl.ds(11, 3)],
    )
    wire = Wire(r.send, r.recv)
    at = by_rows(r.kv, rows)
    at(here, 0, rows)[...] = dot(r.mid[...], r.wkv[...]).astype(BF16)
    answered(peers)
    opening(r, wire, copies, rest, wire.work)
    wire.work.append(lambda: fill_bias(r.bias, r.firsts, here * rows, rows, length))

    def clear():
        r.total[...] = jnp.zeros_like(r.total)

    wire.work.append(clear)
    run_kv = gather_seq(wire, at, rows)
    next(run_kv)
    next(run_kv)
    run_slices = exchange(r, wire, places)
    next(run_slices)
    me = head_index()
    own = pltpu.make_async_copy(
        r.wkv.at[pl.ds(pl.multiple_of(me * share, share), share)], r.slices.at[me], r.local.at[8]
    )
    own.start()
    finish(run_kv)
    wire.idle(len(wire.work))
    s_rows = heads * E
    run_states = together(
        gather_seq(wire, by_rows(r.states, s_rows), s_rows),
        gather_seq(wire, by_rows(r.decays, 16), 16),
        run_slices,
    )
    next(run_states)
    late = bring((r.wo_in.at[0], r.wo), sem=r.local.at[pl.ds(9, 1)])

    def keep(cols):
        def put(value):
            r.outputs[:, cols] = value

        return put

    def ahead(h, q, cols):
        return forward_parts(
            lambda: q[:, cols],
            r.kv, r.bias, r.raised.at[h], r.rounded.at[h], r.inverse.at[h], keep(cols),
        )

    def wide(h):
        return pl.ds(pl.multiple_of(h * E, E), E)

    def upper(h, _):
        for item in ahead(h, r.q1, wide(h)):
            item()
        return 0

    def back(q, g):
        def go(h, _):
            cols = wide(h)
            r.q_grad[:, cols] = backward(
                q[:, cols], g[:, cols], r.kv, r.raised.at[h], r.rounded.at[h], r.inverse.at[h],
                r.outputs[:, cols], r.total,
            )
            return 0

        return go

    lax.fori_loop(0, heads, upper, 0)
    next(run_states)
    lax.fori_loop(0, heads, back(r.q1, r.g1), 0)
    next(run_states)
    next(run_states)
    for k in range(0, depth, share):
        r.acc[:, k : k + share] = dot_last(r.q_grad[...], r.wq1[k : k + share]).astype(BF16)
    work = []
    for h in range(heads):
        work += ahead(h, r.q0, slice(h * E, (h + 1) * E))
    wire.planned(work, {0: 10, 16: 3, 17: 14, 34: 9})
    for step, _ in enumerate(head_run(wire, r.acc, r.land, r.residual, r.upstream)):
        if step in (3, 4):
            next(run_states)
    wire.idle(len(wire.work))
    own.wait()
    late[0].wait()
    r.g0[...] = dot_last(r.upstream[...], r.wo[...]).astype(BF16)
    last = bring((r.wr_in, r.wo), sem=r.local.at[pl.ds(10, 1)])
    finish(run_states)
    wire.drain()
    greet(peers)
    lax.fori_loop(0, heads, back(r.q0, r.g0), 0)
    r.acc_k[...] = r.total[...].astype(BF16)
    last[0].wait()
    answered(peers)
    wire.used = 0
    closing(r, wire)


def whole(number, *operands):
    rows, depth = operands[0].shape
    wide = operands[8].shape[1]
    heads = wide // E
    length = 16 * rows
    shape = jax.ShapeDtypeStruct
    scratch = {
        "ret_query": pltpu.VMEM((rows, wide), BF16),
        "ret_key": pltpu.VMEM((rows, wide), BF16),
        "ret_value": pltpu.VMEM((rows, wide), BF16),
        "mid": pltpu.VMEM((rows, depth), BF16),
        "second": pltpu.VMEM((rows, depth), BF16),
        "residual": pltpu.VMEM((rows, depth), BF16),
        "wkv": pltpu.VMEM((depth, 2 * E), BF16),
        "wq1": pltpu.VMEM((depth, wide), BF16),
        "wq0": pltpu.VMEM((depth, wide), BF16),
        "wo": pltpu.VMEM((wide, depth), BF16),
        "mid_t": pltpu.VMEM((depth, rows), BF16),
        "slices": pltpu.VMEM((8, depth // 8, 2 * E), BF16),
        "kv": pltpu.VMEM((length, 2 * E), BF16),
        "q1": pltpu.VMEM((rows, wide), BF16),
        "g1": pltpu.VMEM((rows, wide), BF16),
        "q0": pltpu.VMEM((rows, wide), BF16),
        "outputs": pltpu.VMEM((rows, wide), BF16),
        "logs": pltpu.VMEM((8, rows), F32),
        "first_state": pltpu.VMEM((wide, E), F32),
        "states": pltpu.VMEM((16 * wide, E), BF16),
        "decays": pltpu.VMEM((256, 128), F32),
        "bias": pltpu.VMEM((rows, length), F32),
        "total": pltpu.VMEM((2 * E, length), F32),
        "raised": pltpu.VMEM((heads, rows, length), F32),
        "rounded": pltpu.VMEM((heads, rows, length), BF16),
        "inverse": pltpu.VMEM((heads, rows, 128), F32),
        "upstream": pltpu.VMEM((rows, depth), BF16),
        "land": pltpu.VMEM((7 * rows, depth // 8), BF16),
        "acc_k": pltpu.VMEM((2 * E, length), BF16),
        "land_k": pltpu.VMEM((15 * rows, rows), BF16),
        "kv_all": pltpu.VMEM((8 * rows, 2 * E), BF16),
        "w_land": pltpu.VMEM((15 * depth // 16, 2 * E), BF16),
        "grads": pltpu.VMEM((8 * wide, E), BF16),
        "own_state": pltpu.VMEM((wide, E), BF16),
        "side_state": pltpu.VMEM((wide, E), BF16),
        "chip_state": pltpu.VMEM((wide, E), BF16),
        "local": pltpu.SemaphoreType.DMA((14,)),
        "send": pltpu.SemaphoreType.DMA((WIRES,)),
        "recv": pltpu.SemaphoreType.DMA((WIRES,)),
    }
    names = IN_NAMES + OUT_NAMES + tuple(scratch)
    shared = {"acc": "second", "g0": "g1", "q_grad": "gq"}

    def kernel(*refs):
        again = [refs[names.index(name)] for name in shared.values()]
        whole_kernel(names + tuple(shared), *refs, *again)

    smem = pl.BlockSpec(memory_space=pltpu.SMEM)
    return pl.pallas_call(
        kernel,
        out_shape=(
            shape((rows, depth), BF16),
            shape((rows, wide), BF16),
            shape((rows, wide), BF16),
            shape((rows, wide), BF16),
            shape((depth, 2 * E), BF16),
        ),
        in_specs=[ANY] * 11 + [VMEM] + [smem] * 2,
        out_specs=(ANY, VMEM, VMEM, VMEM, VMEM),
        scratch_shapes=list(scratch.values()),
        compiler_params=pltpu.CompilerParams(
            collective_id=number, has_side_effects=True, vmem_limit_bytes=67043328
        ),
    )(*operands)


def local(
    mid,
    second_in,
    cotangent,
    w_key,
    w_value,
    w_query,
    w_out,
    w_ret_out,
    ret_query,
    ret_key,
    ret_value,
    gate,
    decay_exp,
    mask_start,
):
    made = whole(
        0, mid, second_in, cotangent, w_key, w_value, w_query, w_out, w_ret_out,
        ret_query, ret_key, ret_value, gate, decay_exp, mask_start,
    )
    return hand_out(*made)


def solution(mesh):
    torus = Mesh(mesh.devices.reshape(2, 4, 2, 4, 2), ("xh", "y", "core", "z", "xl"))
    in_specs = (
        P(SEQ, None),
        P(SEQ, None),
        P(SEQ, None),
        P(None, HEAD),
        P(None, HEAD),
        P(None, None, HEAD),
        P(None, HEAD, None),
        P(HEAD, None),
        P(SEQ, HEAD),
        P(SEQ, HEAD),
        P(SEQ, HEAD),
        P(HEAD, SEQ),
        P(HEAD),
        P(SEQ),
    )
    out_specs = (
        P(SEQ, None),
        P(SEQ, HEAD),
        P(SEQ, HEAD),
        P(SEQ, HEAD),
        P(None, HEAD),
        P(None, HEAD),
    )
    return jax.shard_map(local, mesh=torus, in_specs=in_specs, out_specs=out_specs, check_vma=False)
```

```python
import functools
import math

import jax
import jax.numpy as jnp
from jax import lax
from jax.experimental import pallas as pl
from jax.experimental.pallas import tpu as pltpu
from jax.sharding import Mesh
from jax.sharding import PartitionSpec as P

E = 128
BLK = 128
RC = 128
SEQ = ("xh", "y", "core")
HEAD = ("z", "xl")

MESH = pl.DeviceIdType.MESH
BF16 = jnp.bfloat16
F32 = jnp.float32


class Wire:
    def __init__(self, send, recv):
        self.send, self.recv, self.sent, self.used = send, recv, [], 0
        self.work, self.pace, self.plan, self.waits = [], 1, {}, 0

    def planned(self, work, plan):
        self.work, self.pace, self.plan, self.waits = work, 0, plan, 0

    def idle(self, count):
        for item in self.work[:count]:
            item()
        self.work = self.work[count:]

    def put(self, src, dst, to):
        k = self.used
        self.used += 1
        copy = pltpu.make_async_remote_copy(
            src_ref=src,
            dst_ref=dst,
            send_sem=self.send.at[k],
            recv_sem=self.recv.at[k],
            device_id=to,
            device_id_type=MESH,
        )
        copy.start()
        self.sent.append(copy)
        return (k, to)

    def got(self, ticket, landed):
        self.idle(self.plan.get(self.waits, self.pace))
        self.waits += 1
        k, to = ticket
        pltpu.make_async_remote_copy(
            src_ref=landed,
            dst_ref=landed,
            send_sem=self.send.at[k],
            recv_sem=self.recv.at[k],
            device_id=to,
            device_id_type=MESH,
        ).wait_recv()

    def drain(self):
        for copy in self.sent:
            copy.wait_send()
        self.sent = []


def greet(peers):
    barrier = pltpu.get_barrier_semaphore()
    for to in peers:
        pl.semaphore_signal(barrier, inc=1, device_id=to, device_id_type=MESH)


def answered(peers):
    pl.semaphore_wait(pltpu.get_barrier_semaphore(), len(peers))


def near(axis):
    at = lax.axis_index(axis)
    return at, lax.rem(at + 1, 4), lax.rem(at + 3, 4), lax.rem(at + 2, 4)


def seq_peers():
    y, yp, ym, y2 = near("y")
    return [
        {"xh": 1 - lax.axis_index("xh")},
        {"y": yp},
        {"y": ym},
        {"core": 1 - lax.axis_index("core")},
    ]


def head_peers():
    z, zp, zm, z2 = near("z")
    return [{"xl": 1 - lax.axis_index("xl")}, {"z": zp}, {"z": zm}]


def by_rows(ref, rows, parts=2):
    step = rows // parts

    def at(slot, first, count):
        return ref.at[pl.ds(pl.multiple_of(slot * rows + first, step), count)]

    return at


def by_columns(ref, width):
    def at(slot, first, count):
        return ref.at[pl.ds(first, count), pl.ds(pl.multiple_of(slot * width, 128), width)]

    return at


def add_to(total, part):
    total[...] = (total[...].astype(F32) + part[...].astype(F32)).astype(total.dtype)


def together(*runs):
    runs = list(runs)
    while runs:
        for run in list(runs):
            try:
                next(run)
            except StopIteration:
                runs.remove(run)
        yield


def finish(run):
    for _ in run:
        pass


def gather_seq(wire, at, rows):
    xh, c = lax.axis_index("xh"), lax.axis_index("core")
    y, yp, ym, y2 = near("y")
    xo, co = 1 - xh, 1 - c
    half = rows // 2
    whole, low, high = (0, rows), (0, half), (half, half)
    across, up, down, beside = {"xh": xo}, {"y": yp}, {"y": ym}, {"core": co}

    def slot(a, b, d):
        return a * 8 + b * 2 + d

    def pass_on(s, part, to):
        return wire.put(at(s, *part), at(s, *part), to)

    side = []
    own, far = slot(xh, y, c), slot(xo, y, c)
    t_x = pass_on(own, whole, across)
    ups, downs = [pass_on(own, whole, up)], [pass_on(own, whole, down)]
    side.append((pass_on(own, whole, beside), slot(xh, y, co)))
    yield
    wire.got(t_x, at(far, *whole))
    ups.append(pass_on(far, whole, up))
    downs.append(pass_on(far, whole, down))
    side.append((pass_on(far, whole, beside), slot(xo, y, co)))
    yield
    last = []
    for k, q in enumerate((xh, xo)):
        wire.got(ups[k], at(slot(q, ym, c), *whole))
        a = pass_on(slot(q, ym, c), low, up)
        side.append((pass_on(slot(q, ym, c), whole, beside), slot(q, ym, co)))
        wire.got(downs[k], at(slot(q, yp, c), *whole))
        b = pass_on(slot(q, yp, c), high, down)
        side.append((pass_on(slot(q, yp, c), whole, beside), slot(q, yp, co)))
        last.append((a, b))
        yield
    for k, q in enumerate((xh, xo)):
        wire.got(last[k][0], at(slot(q, y2, c), *low))
        wire.got(last[k][1], at(slot(q, y2, c), *high))
        side.append((pass_on(slot(q, y2, c), whole, beside), slot(q, y2, co)))
        yield
    for ticket, s in side:
        wire.got(ticket, at(s, *whole))


def ring_scatter(wire, at, slot, axis, first, count, land, before=None):
    r, rp, rm, r2 = near(axis)
    up, down = {axis: rp}, {axis: rm}
    half = count // 2
    wait = before or (lambda j: None)
    low, high = land.at[pl.ds(0, half)], land.at[pl.ds(half, half)]
    from_up, from_down = land.at[pl.ds(count, count)], land.at[pl.ds(2 * count, count)]
    wait(2)
    a = wire.put(at(slot(r2), first, half), low, up)
    b = wire.put(at(slot(r2), first + half, half), high, down)
    yield
    wait(1)
    wire.got(a, low)
    add_to(at(slot(rp), first, half), low)
    u = wire.put(at(slot(rp), first, count), from_down, up)
    wait(3)
    wire.got(b, high)
    add_to(at(slot(rm), first + half, half), high)
    d = wire.put(at(slot(rm), first, count), from_up, down)
    yield
    wait(0)
    wire.got(u, from_down)
    add_to(at(slot(r), first, count), from_down)
    wire.got(d, from_up)
    add_to(at(slot(r), first, count), from_up)


def scatter_seq(wire, at, rows, land):
    xh, c = lax.axis_index("xh"), lax.axis_index("core")
    y, yp, ym, y2 = near("y")
    xo, co = 1 - xh, 1 - c

    def slot(a, b, d):
        return a * 8 + b * 2 + d

    def block(k, count=1):
        return land.at[pl.ds(k * rows, count * rows)]

    places = {0: y, 1: yp, 2: y2, 3: ym}
    side = {}
    for n, q in enumerate((xo, xh)):
        for m, j in enumerate((2, 1, 3, 0)):
            dst = block(4 * n + m)
            side[n, j] = (wire.put(at(slot(q, places[j], co), 0, rows), dst, {"core": co}), dst)

    yield

    def before(n, q):
        def wait(j):
            ticket, dst = side[n, j]
            wire.got(ticket, dst)
            add_to(at(slot(q, places[j], c), 0, rows), dst)

        return wait

    def ring(n, q):
        return ring_scatter(
            wire, at, lambda j: slot(q, j, c), "y", 0, rows, block(8 + 3 * n, 3), before(n, q)
        )

    sent = []

    def far():
        yield from ring(0, xo)
        sent.append(wire.put(at(slot(xo, y, c), 0, rows), block(14), {"xh": xo}))

    yield from together(far(), ring(1, xh))
    wire.got(sent[0], block(14))
    return block(14)


def scatter_head(wire, at, rows, land):
    xl = lax.axis_index("xl")
    z, zp, zm, z2 = near("z")
    xo = 1 - xl
    cut = rows * 3 // 8
    left = rows - cut

    def slot(j, q):
        return j * 2 + q

    def block(k, count=1):
        return land.at[pl.ds(k * cut, count * cut)]

    def lower(k, count=1):
        return land.at[pl.ds(7 * cut + k * left, count * left)]

    places = {0: z, 1: zp, 2: z2, 3: zm}
    side = {}
    for m, j in enumerate((2, 1, 3, 0)):
        side[j] = (wire.put(at(slot(places[j], xo), 0, cut), block(m), {"xl": xo}), block(m))

    def wait(j):
        ticket, dst = side[j]
        wire.got(ticket, dst)
        add_to(at(slot(places[j], xl), 0, cut), dst)

    sent = []

    def far():
        yield from ring_scatter(
            wire, at, lambda j: slot(j, xo), "z", cut, left, lower(0, 3)
        )
        sent.append(wire.put(at(slot(z, xo), cut, left), lower(6), {"xl": xo}))

    yield from together(
        far(),
        ring_scatter(wire, at, lambda j: slot(j, xl), "z", cut, left, lower(3, 3)),
        ring_scatter(wire, at, lambda j: slot(j, xl), "z", 0, cut, block(4, 3), wait),
    )
    wire.got(sent[0], lower(6))
    add_to(at(slot(z, xl), cut, left), lower(6))


def gather_head(wire, at, rows):
    xl = lax.axis_index("xl")
    z, zp, zm, z2 = near("z")
    xo = 1 - xl
    cut = rows * 3 // 8
    left = rows - cut
    up, down, across = {"z": zp}, {"z": zm}, {"xl": xo}

    def slot(j, q):
        return j * 2 + q

    def pass_on(s, first, count, to):
        return wire.put(at(s, first, count), at(s, first, count), to)

    def ring(q, first, half, each=None):
        h = half // 2
        tell = each or (lambda j: None)
        a = pass_on(slot(z, q), first, half, up)
        b = pass_on(slot(z, q), first, half, down)
        tell(z)
        yield
        wire.got(a, at(slot(zm, q), first, half))
        c = pass_on(slot(zm, q), first, h, up)
        tell(zm)
        wire.got(b, at(slot(zp, q), first, half))
        d = pass_on(slot(zp, q), first + h, h, down)
        tell(zp)
        yield
        wire.got(c, at(slot(z2, q), first, h))
        wire.got(d, at(slot(z2, q), first + h, h))
        tell(z2)

    side = []

    def tell(j):
        side.append((pass_on(slot(j, xl), 0, cut, across), slot(j, xo)))

    t_x = pass_on(slot(z, xl), cut, left, across)

    def far():
        wire.got(t_x, at(slot(z, xo), cut, left))
        yield from ring(xo, cut, left)

    yield from together(ring(xl, 0, cut, tell), ring(xl, cut, left), far())
    for ticket, s in side:
        wire.got(ticket, at(s, 0, cut))


ANY = pl.BlockSpec(memory_space=pl.ANY)
VMEM = pl.BlockSpec(memory_space=pltpu.VMEM)


def bring(*pairs, sem):
    copies = [pltpu.make_async_copy(s, d, sem.at[k]) for k, (s, d) in enumerate(pairs)]
    for copy in copies:
        copy.start()
    return copies


def seq_index():
    return lax.axis_index("xh") * 8 + lax.axis_index("y") * 2 + lax.axis_index("core")


def head_index():
    return lax.axis_index("z") * 2 + lax.axis_index("xl")


def total_into(out_at, acc_at, residual, rows, width):
    me = head_index()
    own = acc_at(me, 0, rows)
    kept = residual.at[pl.ds(0, rows), pl.ds(pl.multiple_of(me * width, 128), width)]
    out_at(me, 0, rows)[...] = (kept[...].astype(F32) + own[...].astype(F32)).astype(BF16)


def head_run(wire, acc, land, residual, out):
    rows, columns = acc.shape
    width = columns // 8
    yield from scatter_head(wire, by_columns(acc, width), rows, land)
    total_into(by_columns(out, width), by_columns(acc, width), residual, rows, width)
    yield from gather_head(wire, by_columns(out, width), rows)


def dot_last(a, b):
    return lax.dot_general(a, b, (((1,), (1,)), ((), ())), preferred_element_type=F32)


def dot(a, b):
    return jnp.dot(a, b, preferred_element_type=F32)


def folded(value, op):
    parts = [value[:, k : k + 128] for k in range(0, value.shape[1], 128)]
    while len(parts) > 1:
        parts = [op(a, b) for a, b in zip(parts[::2], parts[1::2])]
    return parts[0]


CHUNK = 512


def fill_bias(bias, firsts, position, rows, length):
    row = lax.broadcasted_iota(jnp.int32, (rows, CHUNK), 0)
    low = jnp.where(row < BLK, firsts[0], firsts[1])
    high = row + position
    for k in range(0, length, CHUNK):
        column = lax.broadcasted_iota(jnp.int32, (rows, CHUNK), 1) + k
        seen = (column >= low) & (column <= high)
        bias[:, k : k + CHUNK] = jnp.where(seen, 0.0, -jnp.inf)


def flipped(value):
    return value.astype(F32).T


def log_decays(logs):
    t = lax.broadcasted_iota(jnp.int32, (RC, RC), 0)
    s = lax.broadcasted_iota(jnp.int32, (RC, RC), 1)
    upto = jnp.where(t <= s, 1.0, 0.0)
    rows, columns = [], []
    for c in range(logs.shape[1] // RC):
        part = jnp.dot(
            logs[:, c * RC : (c + 1) * RC],
            upto,
            precision=lax.Precision.HIGHEST,
            preferred_element_type=F32,
        )
        rows.append(part)
        tall = jnp.concatenate((part, jnp.zeros((RC - part.shape[0], RC), F32)), axis=0)
        columns.append(tall.T)
    return rows, columns


def spread(peers):
    z, xl = lax.axis_index("z"), lax.axis_index("xl")
    places = []
    for k in range(1, 8):
        to = (lax.rem(z + k // 2, 4), lax.rem(xl + k, 2))
        came = (lax.rem(z + 4 - k // 2, 4), lax.rem(xl + k, 2))
        places.append((to, came))
    return places


def hand_out_kernel(*refs):
    ins, outs, held, (wide, sem_in, sem_out) = refs[:5], refs[5:11], refs[11:16], refs[16:]
    copies = bring(*zip(ins, held), sem=sem_in)
    sends = []
    for k in range(4):
        copies[k].wait()
        sends.append(pltpu.make_async_copy(held[k], outs[k], sem_out.at[k]))
        sends[-1].start()
    copies[4].wait()
    for k in range(2):
        wide[k] = held[4][:, k * E : (k + 1) * E].astype(F32)
        sends.append(pltpu.make_async_copy(wide.at[k], outs[4 + k], sem_out.at[4 + k]))
        sends[-1].start()
    for send in sends:
        send.wait()


def hand_out(*arrays):
    shape = jax.ShapeDtypeStruct
    depth = arrays[4].shape[0]
    return pl.pallas_call(
        hand_out_kernel,
        out_shape=tuple(shape(a.shape, a.dtype) for a in arrays[:4])
        + (shape((depth, E), F32), shape((depth, E), F32)),
        in_specs=[ANY] * 5,
        out_specs=(ANY,) * 6,
        scratch_shapes=[pltpu.VMEM(a.shape, a.dtype) for a in arrays]
        + [
            pltpu.VMEM((2, depth, E), F32),
            pltpu.SemaphoreType.DMA((5,)),
            pltpu.SemaphoreType.DMA((6,)),
        ],
    )(*arrays)


def scores_pass(q, kv, bias, raised, stats):
    def part(k):
        def go():
            for at in (slice(k, k + CHUNK), slice(k + CHUNK, k + 2 * CHUNK)):
                scores = dot_last(q(), kv[at, :E]) + bias[:, at]
                raised[:, at] = scores
                most = folded(scores, jnp.maximum)
                top = stats.get("top")
                stats["top"] = most if top is None else jnp.maximum(top, most)

        return go

    return [part(k) for k in range(0, kv.shape[0], 2 * CHUNK)]


def power_pass(raised, stats):
    def part(k):
        def go():
            if k == 0:
                stats["top"] = jnp.max(stats["top"], axis=1, keepdims=True)
            for at in (slice(k, k + CHUNK), slice(k + CHUNK, k + 2 * CHUNK)):
                shifted = raised[:, at] - stats["top"]
                power = jnp.exp2(shifted * (math.log2(math.e) / math.sqrt(E)))
                raised[:, at] = power
                more = folded(power, jnp.add)
                stats["sum"] = stats["sum"] + more if "sum" in stats else more

        return go

    return [part(k) for k in range(0, raised.shape[1], 2 * CHUNK)]


def output_pass(kv, raised, rounded, inverse, outputs, stats):
    def part(k):
        def go():
            if k == 0:
                whole = jnp.sum(stats["sum"], axis=1, keepdims=True)
                stats["inverse"] = 1.0 / whole
                inverse[...] = jnp.broadcast_to(stats["inverse"], inverse.shape)
            for at in (slice(k, k + CHUNK), slice(k + CHUNK, k + 2 * CHUNK)):
                probs = (raised[:, at] * stats["inverse"]).astype(BF16)
                rounded[:, at] = probs
                made = dot(probs, kv[at, E:])
                stats["out"] = stats["out"] + made if "out" in stats else made
            if k + 2 * CHUNK == kv.shape[0]:
                outputs(stats["out"].astype(BF16))

        return go

    return [part(k) for k in range(0, kv.shape[0], 2 * CHUNK)]


def forward_parts(q, kv, bias, raised, rounded, inverse, outputs):
    stats = {}
    return (
        scores_pass(q, kv, bias, raised, stats)
        + power_pass(raised, stats)
        + output_pass(kv, raised, rounded, inverse, outputs, stats)
    )


def backward(q, g, kv, raised, rounded, inverse, outputs, total):
    length = kv.shape[0]
    now = total is not None
    delta = jnp.sum(g.astype(F32) * outputs.astype(F32), axis=1, keepdims=True)
    scaled = inverse[:, :1] * (1.0 / math.sqrt(E))
    if now:
        q_t = flipped(q).astype(BF16)
        g_t = flipped(g).astype(BF16)
    query_grad = jnp.zeros(q.shape, F32)
    for k in range(0, length, CHUNK):
        at = slice(k, k + CHUNK)
        dprobs = dot_last(g, kv[at, E:])
        dscores = ((raised[:, at] * scaled) * (dprobs - delta)).astype(BF16)
        query_grad = query_grad + dot(dscores, kv[at, :E])
        if now:
            total[:E, at] = total[:E, at] + dot(q_t, dscores)
            total[E:, at] = total[E:, at] + dot(g_t, rounded[:, at])
        else:
            raised[:, at] = dscores.astype(F32)
    return query_grad.astype(BF16)


def later_parts(q, g, raised, rounded, total):
    held = {}

    def part(k):
        def go():
            if k == 0:
                held["q"], held["g"] = flipped(q()).astype(BF16), flipped(g()).astype(BF16)
            for at in (slice(k, k + CHUNK), slice(k + CHUNK, k + 2 * CHUNK)):
                total[:E, at] = total[:E, at] + dot(held["q"], raised[:, at].astype(BF16))
                total[E:, at] = total[E:, at] + dot(held["g"], rounded[:, at])

        return go

    return [part(k) for k in range(0, raised.shape[1], 2 * CHUNK)]


WIRES = 120


def opening(r, wire, copies, rest, work):
    rows, depth = r.mid.shape

    def product(out, left, right, how, *numbers):
        def part(k):
            def go():
                if k == 0:
                    for number in numbers:
                        copies[number].wait()
                out[:, k : k + E] = how(left, right, k, E).astype(BF16)

            return go

        work.extend(part(k) for k in range(0, out.shape[1], E))

    def straight(left, right, at, count):
        return dot(left[...], right[:, at : at + count])

    def across(left, right, at, count):
        return dot_last(left[...], right[at : at + count])

    def rates():
        row = lax.broadcasted_iota(jnp.int32, (8, 128), 0)
        rate = jnp.zeros((8, 128), F32)
        for k in range(r.gate.shape[0]):
            power = jnp.full((8, 128), r.decay_exp[k], jnp.int32).astype(F32)
            rate = jnp.where(row == k, jnp.exp2(power * (-1.0 / 64.0)), rate)
        empty = jnp.zeros((8 - r.gate.shape[0], r.gate.shape[1]), F32)
        tall = jnp.concatenate((r.gate[...], empty), axis=0)
        r.logs[...] = -rate[:, :1] * tall

    def states():
        for copy in rest:
            copy.wait()
        arow, acol = log_decays(r.logs[...])
        total = arow[0][:, RC - 1 :] + arow[1][:, RC - 1 :]
        here = seq_index()
        mine = r.decays.at[pl.ds(pl.multiple_of(here * 16, 16), 16)]
        mine[...] = jnp.concatenate(
            (jnp.broadcast_to(total, (8, 128)), jnp.zeros((8, 128), F32)), axis=0
        )
        count = r.ret_key.shape[1]
        for h in range(count // E):
            cols = slice(h * E, (h + 1) * E)
            made = []
            for c in range(2):
                span = slice(c * RC, (c + 1) * RC)
                shrink = jnp.exp(arow[c][h : h + 1, RC - 1 :] - acol[c][:, h : h + 1])
                scaled = (shrink * r.ret_key[span, cols].astype(F32)).astype(BF16)
                made.append(dot(flipped(scaled).astype(BF16), r.ret_value[span, cols]))
            r.first_state[cols] = made[0]
            last = jnp.exp(arow[1][h : h + 1, RC - 1 :])
            to = r.states.at[pl.ds(pl.multiple_of(here * count + h * E, E), E)]
            to[...] = (last * made[0] + made[1]).astype(BF16)

    def turn(k):
        def go():
            for j in range(k, k + 512, 128):
                r.mid_t[j : j + 128] = flipped(r.mid[:, j : j + 128]).astype(BF16)

        return go

    turns = [turn(k) for k in range(0, depth, 512)]
    work.extend([rates, states, turns[0]])
    product(r.q1, r.second, r.wq1, straight, 3, 4)
    product(r.g1, r.residual, r.wo, across, 5, 6)
    product(r.q0, r.mid, r.wq0, straight, 7)
    work.extend(turns[1:])


def exchange(r, wire, places):
    me, c = head_index(), lax.axis_index("core")
    share = r.wkv.shape[0] // 8
    tickets, side = [], []

    def mine(slot, half):
        return r.slices.at[slot, :, pl.ds(pl.multiple_of(half * E, E), E)]

    for (a, b), (ca, cb) in places:
        rows = pl.ds(pl.multiple_of((a * 2 + b) * share, share), share)
        src = r.wkv.at[rows, pl.ds(pl.multiple_of(c * E, E), E)]
        tickets.append((wire.put(src, mine(me, c), {"z": a, "xl": b}), ca * 2 + cb))
    yield
    yield
    for ticket, slot in tickets:
        wire.got(ticket, mine(slot, c))
        side.append((wire.put(mine(slot, c), mine(slot, c), {"core": 1 - c}), slot))
    yield
    yield
    yield
    yield
    yield
    for ticket, slot in side:
        wire.got(ticket, mine(slot, 1 - c))


def closing(r, wire):
    rows, depth = r.acc.shape
    share = depth // 8
    heads = r.ret_query.shape[1] // E
    me, here = head_index(), seq_index()
    kv_at = by_rows(r.kv_all, rows, 16)
    w_rows = depth // 16
    w_at = by_rows(r.w_sum, w_rows)
    s_rows = heads * E
    c_half = s_rows // 2
    arow, acol = log_decays(r.logs[...])
    t = lax.broadcasted_iota(jnp.int32, (RC, RC), 0)
    s = lax.broadcasted_iota(jnp.int32, (RC, RC), 1)
    pieces = [(h, c) for h in range(heads) for c in range(2)]
    where = {(h, c): (slice(c * RC, (c + 1) * RC), slice(h * E, (h + 1) * E)) for h, c in pieces}
    weights, second, turned, entering, after = {}, {}, {}, {}, {}
    rq, rk, rv = r.ret_query, r.ret_key, r.ret_value

    def end(h, c):
        return arow[c][h : h + 1, RC - 1 :]

    def prepare(h, c):
        a_t, a_s = acol[c][:, h : h + 1], arow[c][h : h + 1]
        lower = t >= s
        weights[h, c] = jnp.where(lower, jnp.exp(jnp.where(lower, a_t - a_s, 0.0)), 0.0)
        q, k = rq[where[h, c]], rk[where[h, c]]
        both = (weights[h, c] * dot_last(q, k)).astype(BF16)
        second[h, c] = flipped(both).astype(BF16)
        grown = (jnp.exp(a_t) * q.astype(F32)).astype(BF16)
        turned[h, c] = flipped(grown).astype(BF16)

    def arriving(h):
        cols = where[h, 0][1]
        now = jnp.zeros((E, E), F32)
        for k in range(15):
            mine = r.states[k * s_rows + h * E : k * s_rows + (h + 1) * E].astype(F32)
            new = jnp.exp(r.decays[k * 16 + h : k * 16 + h + 1]) * now + mine
            now = jnp.where(k < here, new, now)
        entering[h, 0] = now.astype(BF16)
        entering[h, 1] = (jnp.exp(end(h, 0)) * now + r.first_state[cols]).astype(BF16)

    def keys():
        at = by_columns(r.acc_k, rows)
        rest = yield from scatter_seq(wire, at, rows, r.land_k)
        own = at(here, 0, rows)
        total = own[...].astype(F32) + rest[...].astype(F32)
        kv_at(me, 0, rows)[...] = total.T.astype(BF16)

    run_keys = keys()
    next(run_keys)
    for k in range(0, depth, share):
        r.acc[:, k : k + share] = dot_last(r.q_grad[...], r.wq0[k : k + share]).astype(BF16)
    work = [lambda h=h: arriving(h) for h in range(heads)]
    work += [lambda h=h, c=c: prepare(h, c) for h, c in pieces]
    wire.planned(work, {2: 9})
    m_at = by_columns(r.acc, share)
    finish(together(run_keys, scatter_head(wire, m_at, rows, r.land)))
    wire.idle(len(wire.work))
    own_kv = kv_at(me, 0, rows)
    gather_kv = gather_head(wire, kv_at, rows)
    next(gather_kv)
    r.wkv[...] = dot(r.mid_t[...], own_kv[...]).astype(BF16)

    def sums():
        at = by_rows(r.wkv, w_rows)
        rest = yield from scatter_seq(wire, at, w_rows, r.wq1.at[:, pl.ds(0, 2 * E)])
        w_at(here, 0, w_rows)[...] = (
            at(here, 0, w_rows)[...].astype(F32) + rest[...].astype(F32)
        ).astype(BF16)
        yield from gather_seq(wire, w_at, w_rows)

    shared = sums()
    next(shared)
    next(shared)

    def beside(run):
        for _ in run:
            next(shared, None)

    beside(gather_kv)
    total = m_at(me, 0, rows)[...].astype(F32)
    total = total + by_columns(r.upstream, share)(me, 0, rows)[...].astype(F32)
    for h in range(8):
        total = total + dot_last(kv_at(h, 0, rows)[...], r.slices[h])
    out_at = by_columns(r.mid, share)
    out_at(me, 0, rows)[...] = total.astype(BF16)
    beside(gather_head(wire, out_at, rows))
    shown = [pltpu.make_async_copy(r.mid, r.grad_mid, r.local.at[0])]
    shown[0].start()
    grad_o = dot_last(r.mid[...], r.wo[...]).astype(BF16)
    own_grad = {}
    for h, c in pieces:
        span, cols = where[h, c]
        own_grad[h, c] = dot(turned[h, c], grad_o[span, cols]) * (1.0 / E)
    for h in range(heads):
        made = own_grad[h, 0] + jnp.exp(end(h, 0)) * own_grad[h, 1]
        r.own_state[h * E : (h + 1) * E] = made.astype(BF16)
    core = lax.axis_index("core")
    chip = here - core
    ticket = wire.put(r.own_state, r.side_state, {"core": 1 - core})
    inner = {}

    def inside(h, c):
        span, cols = where[h, c]
        g, q, k, v = grad_o[span, cols], rq[span, cols], rk[span, cols], rv[span, cols]
        first = (weights[h, c] * dot_last(g, v)).astype(BF16)
        grow = jnp.exp(acol[c][:, h : h + 1])
        carried = grow * dot_last(g, entering[h, c])
        r.gq[span, cols] = ((dot(first, k) + carried) * (1.0 / E)).astype(BF16)
        inner[h, c] = (
            dot(flipped(first).astype(BF16), q) * (1.0 / E),
            dot(second[h, c], g) * (1.0 / E),
        )

    wire.planned([lambda h=h, c=c: inside(h, c) for h, c in pieces], {0: 2, 1: 4})
    wire.got(ticket, r.side_state)
    for h in range(heads):
        cols = slice(h * E, (h + 1) * E)
        mine, other = r.own_state[cols].astype(F32), r.side_state[cols].astype(F32)
        lead = r.decays[pl.ds(chip * 16 + h, 1)]
        made = jnp.where(core == 0, mine, other) + jnp.exp(lead) * jnp.where(core == 0, other, mine)
        r.chip_state[cols] = made.astype(BF16)
    s_at = by_rows(r.grads, c_half)
    s_at(here, 0, c_half)[...] = r.chip_state[pl.ds(pl.multiple_of(core * c_half, c_half), c_half)]
    beside(gather_seq(wire, s_at, c_half))
    wire.idle(len(wire.work))
    for h in range(heads):
        now = jnp.zeros((E, E), F32)
        for k in range(7, 0, -1):
            mine = r.grads[k * s_rows + h * E : k * s_rows + (h + 1) * E].astype(F32)
            both = r.decays[k * 32 + h : k * 32 + h + 1] + r.decays[k * 32 + 16 + h : k * 32 + 17 + h]
            new = mine + jnp.exp(both) * now
            now = jnp.where(2 * k > chip, new, now)
        beyond = r.decays[pl.ds((chip + 1) * 16 + h, 1)]
        new = r.side_state[h * E : (h + 1) * E].astype(F32) + jnp.exp(beyond) * now
        now = jnp.where(core == 0, new, now)
        after[h, 1] = now.astype(BF16)
        after[h, 0] = (own_grad[h, 1] + jnp.exp(end(h, 1)) * now).astype(BF16)
    for h, c in pieces:
        span, cols = where[h, c]
        shrink = jnp.exp(end(h, c) - acol[c][:, h : h + 1])
        r.gk[span, cols] = (
            inner[h, c][0] + shrink * dot_last(rv[span, cols], after[h, c])
        ).astype(BF16)
        r.gv[span, cols] = (inner[h, c][1] + shrink * dot(rk[span, cols], after[h, c])).astype(BF16)
    shown += bring((r.gq, r.gq_out), (r.gk, r.gk_out), (r.gv, r.gv_out), sem=r.local.at[pl.ds(1, 3)])
    finish(shared)
    for copy in shown:
        copy.wait()
    wire.drain()


class Refs:
    def __init__(self, names, refs):
        for name, ref in zip(names, refs, strict=True):
            setattr(self, name, ref)


IN_NAMES = (
    "mid_in", "second_in", "cot_in", "wk_in", "wv_in", "wq_in", "wo_in", "wr_in",
    "rq_in", "rk_in", "rv_in", "gate", "decay_exp", "firsts",
)
OUT_NAMES = ("grad_mid", "gq_out", "gk_out", "gv_out", "w_sum")


def whole_kernel(names, *refs):
    r = Refs(names, refs)
    rows, depth = r.mid.shape
    length = r.kv.shape[0]
    share = depth // 8
    heads = r.q1.shape[1] // E
    here = seq_index()
    copies = bring(
        (r.mid_in, r.mid),
        (r.wk_in, r.wkv.at[:, pl.ds(0, E)]),
        (r.wv_in, r.wkv.at[:, pl.ds(E, E)]),
        sem=r.local,
    )
    places = spread(7)
    peers = seq_peers() + [{"z": a, "xl": b} for (a, b), _ in places]
    greet(peers)
    for copy in copies:
        copy.wait()
    copies += bring(
        (r.second_in, r.second),
        (r.wq_in.at[1], r.wq1),
        (r.cot_in, r.residual),
        (r.wo_in.at[1], r.wo),
        (r.wq_in.at[0], r.wq0),
        sem=r.local.at[pl.ds(3, 5)],
    )
    rest = bring(
        (r.rk_in, r.ret_key),
        (r.rv_in, r.ret_value),
        (r.rq_in, r.ret_query),
        sem=r.local.at[pl.ds(11, 3)],
    )
    wire = Wire(r.send, r.recv)
    at = by_rows(r.kv, rows)
    at(here, 0, rows)[...] = dot(r.mid[...], r.wkv[...]).astype(BF16)
    answered(peers)
    opening(r, wire, copies, rest, wire.work)
    wire.work.append(lambda: fill_bias(r.bias, r.firsts, here * rows, rows, length))

    def clear():
        r.total[...] = jnp.zeros_like(r.total)

    wire.work.append(clear)
    run_kv = gather_seq(wire, at, rows)
    next(run_kv)
    next(run_kv)
    run_slices = exchange(r, wire, places)
    next(run_slices)
    me = head_index()
    own = pltpu.make_async_copy(
        r.wkv.at[pl.ds(pl.multiple_of(me * share, share), share)], r.slices.at[me], r.local.at[8]
    )
    own.start()
    finish(run_kv)
    wire.idle(len(wire.work))
    s_rows = heads * E
    run_states = together(
        gather_seq(wire, by_rows(r.states, s_rows), s_rows),
        gather_seq(wire, by_rows(r.decays, 16), 16),
        run_slices,
    )
    next(run_states)
    late = bring((r.wo_in.at[0], r.wo), sem=r.local.at[pl.ds(9, 1)])

    def keep(cols):
        def put(value):
            r.outputs[:, cols] = value

        return put

    def ahead(h, q, cols):
        return forward_parts(
            lambda: q[:, cols],
            r.kv, r.bias, r.raised.at[h], r.rounded.at[h], r.inverse.at[h], keep(cols),
        )

    def wide(h):
        return pl.ds(pl.multiple_of(h * E, E), E)

    def upper(h, _):
        for item in ahead(h, r.q1, wide(h)):
            item()
        return 0

    def back(q, g, total):
        def go(h, _):
            cols = wide(h)
            r.q_grad[:, cols] = backward(
                q[:, cols], g[:, cols], r.kv, r.raised.at[h], r.rounded.at[h], r.inverse.at[h],
                r.outputs[:, cols], total,
            )
            return 0

        return go

    lax.fori_loop(0, heads, upper, 0)
    next(run_states)
    lax.fori_loop(0, heads, back(r.q1, r.g1, None), 0)
    next(run_states)
    next(run_states)
    for k in range(0, depth, share):
        r.acc[:, k : k + share] = dot_last(r.q_grad[...], r.wq1[k : k + share]).astype(BF16)
    work = []
    for h in range(heads):
        cols = slice(h * E, (h + 1) * E)
        work += later_parts(
            lambda cols=cols: r.q1[:, cols],
            lambda cols=cols: r.g1[:, cols],
            r.raised.at[h], r.rounded.at[h], r.total,
        )
        work += ahead(h, r.q0, cols)
    wire.planned(
        work, {0: 12, 5: 2, 7: 2, 9: 2, 11: 2, 13: 2, 15: 2, 16: 4, 17: 14, 34: 6}
    )
    for step, _ in enumerate(head_run(wire, r.acc, r.land, r.residual, r.upstream)):
        if step in (3, 4):
            next(run_states)
    wire.idle(len(wire.work))
    own.wait()
    late[0].wait()
    r.g0[...] = dot_last(r.upstream[...], r.wo[...]).astype(BF16)
    last = bring((r.wr_in, r.wo), sem=r.local.at[pl.ds(10, 1)])
    finish(run_states)
    wire.drain()
    greet(peers)
    lax.fori_loop(0, heads, back(r.q0, r.g0, r.total), 0)
    r.acc_k[...] = r.total[...].astype(BF16)
    last[0].wait()
    answered(peers)
    wire.used = 0
    closing(r, wire)


def whole(number, *operands):
    rows, depth = operands[0].shape
    wide = operands[8].shape[1]
    heads = wide // E
    length = 16 * rows
    shape = jax.ShapeDtypeStruct
    scratch = {
        "ret_query": pltpu.VMEM((rows, wide), BF16),
        "ret_key": pltpu.VMEM((rows, wide), BF16),
        "ret_value": pltpu.VMEM((rows, wide), BF16),
        "gq": pltpu.VMEM((rows, wide), BF16),
        "mid": pltpu.VMEM((rows, depth), BF16),
        "second": pltpu.VMEM((rows, depth), BF16),
        "residual": pltpu.VMEM((rows, depth), BF16),
        "wkv": pltpu.VMEM((depth, 2 * E), BF16),
        "wq1": pltpu.VMEM((depth, wide), BF16),
        "wq0": pltpu.VMEM((depth, wide), BF16),
        "wo": pltpu.VMEM((wide, depth), BF16),
        "mid_t": pltpu.VMEM((depth, rows), BF16),
        "slices": pltpu.VMEM((8, depth // 8, 2 * E), BF16),
        "kv": pltpu.VMEM((length, 2 * E), BF16),
        "q1": pltpu.VMEM((rows, wide), BF16),
        "g1": pltpu.VMEM((rows, wide), BF16),
        "q0": pltpu.VMEM((rows, wide), BF16),
        "outputs": pltpu.VMEM((rows, wide), BF16),
        "logs": pltpu.VMEM((8, rows), F32),
        "first_state": pltpu.VMEM((wide, E), F32),
        "states": pltpu.VMEM((16 * wide, E), BF16),
        "decays": pltpu.VMEM((256, 128), F32),
        "bias": pltpu.VMEM((rows, length), F32),
        "total": pltpu.VMEM((2 * E, length), F32),
        "raised": pltpu.VMEM((heads, rows, length), F32),
        "rounded": pltpu.VMEM((heads, rows, length), BF16),
        "inverse": pltpu.VMEM((heads, rows, 128), F32),
        "upstream": pltpu.VMEM((rows, depth), BF16),
        "land": pltpu.VMEM((7 * rows, depth // 8), BF16),
        "acc_k": pltpu.VMEM((2 * E, length), BF16),
        "land_k": pltpu.VMEM((15 * rows, rows), BF16),
        "kv_all": pltpu.VMEM((8 * rows, 2 * E), BF16),
        "grads": pltpu.VMEM((8 * wide, E), BF16),
        "own_state": pltpu.VMEM((wide, E), BF16),
        "side_state": pltpu.VMEM((wide, E), BF16),
        "chip_state": pltpu.VMEM((wide, E), BF16),
        "local": pltpu.SemaphoreType.DMA((14,)),
        "send": pltpu.SemaphoreType.DMA((WIRES,)),
        "recv": pltpu.SemaphoreType.DMA((WIRES,)),
    }
    names = IN_NAMES + OUT_NAMES + tuple(scratch)
    shared = {"acc": "second", "g0": "g1", "q_grad": "gq", "gk": "q1", "gv": "q0"}

    def kernel(*refs):
        again = [refs[names.index(name)] for name in shared.values()]
        whole_kernel(names + tuple(shared), *refs, *again)

    smem = pl.BlockSpec(memory_space=pltpu.SMEM)
    return pl.pallas_call(
        kernel,
        out_shape=(
            shape((rows, depth), BF16),
            shape((rows, wide), BF16),
            shape((rows, wide), BF16),
            shape((rows, wide), BF16),
            shape((depth, 2 * E), BF16),
        ),
        in_specs=[ANY] * 11 + [VMEM] + [smem] * 2,
        out_specs=(ANY, ANY, ANY, ANY, VMEM),
        scratch_shapes=list(scratch.values()),
        compiler_params=pltpu.CompilerParams(
            collective_id=number, has_side_effects=True, vmem_limit_bytes=67043328
        ),
    )(*operands)


def local(
    mid,
    second_in,
    cotangent,
    w_key,
    w_value,
    w_query,
    w_out,
    w_ret_out,
    ret_query,
    ret_key,
    ret_value,
    gate,
    decay_exp,
    mask_start,
):
    made = whole(
        0, mid, second_in, cotangent, w_key, w_value, w_query, w_out, w_ret_out,
        ret_query, ret_key, ret_value, gate, decay_exp, mask_start,
    )
    return hand_out(*made)


def solution(mesh):
    torus = Mesh(mesh.devices.reshape(2, 4, 2, 4, 2), ("xh", "y", "core", "z", "xl"))
    in_specs = (
        P(SEQ, None),
        P(SEQ, None),
        P(SEQ, None),
        P(None, HEAD),
        P(None, HEAD),
        P(None, None, HEAD),
        P(None, HEAD, None),
        P(HEAD, None),
        P(SEQ, HEAD),
        P(SEQ, HEAD),
        P(SEQ, HEAD),
        P(HEAD, SEQ),
        P(HEAD),
        P(SEQ),
    )
    out_specs = (
        P(SEQ, None),
        P(SEQ, HEAD),
        P(SEQ, HEAD),
        P(SEQ, HEAD),
        P(None, HEAD),
        P(None, HEAD),
    )
    return jax.shard_map(local, mesh=torus, in_specs=in_specs, out_specs=out_specs, check_vma=False)
```
